256 devices in a mesh: gx: 8 (over z), gy: 32 (over x, y, core).
Axes of the slice: x: 4, y: 4, z: 8, core: 2. Of those that a mesh axis runs over, the one named last changes fastest.
Arguments:
- velocity: float32 [3, 32, 128, 4096], P(None, None, 'gx', 'gy'), may hold values from -6 to 6
- old_tendency: float32 [3, 32, 128, 4096], P(None, None, 'gx', 'gy'), may hold values from -6 to 6
- obstacle: int32 [32, 128, 4096], P(None, 'gx', 'gy'), may hold values 0 or 1
Outputs:
- corrected: float32 [3, 32, 128, 4096], P(None, None, 'gx', 'gy')
- pressure: float32 [32, 128, 4096], P(None, 'gx', 'gy')
The draws below stay inside these ranges and needn't reach their ends.
Inputs may be any that keep to these rules, and one draw needn't show every extreme that they name: `obstacle`: 1 marks a building cell, 0 a fluid cell.
All inputs are finite; a program needn't handle non-finite values. No bound on the sum of `obstacle` on one device may be relied on, other than what follows from the above.
Results may differ from the reference program's by a relative error of at most 0.00002.
Values sent between devices are 32-bit elements; how exact they have to be, the bound alone decides.
No kernel may reach another device: no remote copies, remote signals or barrier semaphores. Data moves between devices by JAX's collectives and lax.ppermute only.
A program may use at most 128 MiB of HBM per device.

```python
import jax
import jax.numpy as jnp

NZ = 32
LEVELS = 3
SWEEPS = 2
COARSE_SWEEPS = 8
NX = 128
NY = 4096


def with_ends(entries, stream_key, least, largest):
    dims = entries.shape
    spot = [jax.random.randint(jax.random.fold_in(stream_key, axis), (), 0, dims[axis]) for axis in range(len(dims))]
    entries = entries.at[tuple(spot)].set(least)
    longest = dims.index(max(dims))
    spot[longest] = (spot[longest] + 1) % dims[longest]
    return entries.at[tuple(spot)].set(largest)


def level_of(own_key, shape, cuts, low, top_value):
    def one(dim, parts):
        heights = jax.random.uniform(jax.random.fold_in(jax.random.fold_in(own_key, 6), dim), (parts,), jnp.float32, low / len(cuts), top_value / len(cuts))
        return jnp.repeat(jnp.exp(heights), shape[dim] // parts).reshape((-1,) + (1,) * (len(shape) - dim - 1))

    gain = one(*cuts[0])
    for cut in cuts[1:]:
        gain = gain * one(*cut)
    return gain


def noise(rng, dims, spread, bound, cuts=(), held_as=jnp.bfloat16):
    values = jax.random.normal(rng, dims, jnp.float32) * spread
    if len(cuts) > 0:
        values = level_of(rng, dims, cuts, -0.22, 0.18) * values
    return jnp.clip(values, min=-bound, max=bound).astype(held_as)


def setup_inputs(seed: int = 0) -> dict:
    key_list = jax.random.split(jax.random.key(seed), 4)
    velocity = noise(key_list[0], (3, NZ, NX, NY), 1.0, 6.0, ((2, 8), (3, 32)), jnp.float32)
    old_tendency = noise(key_list[1], (3, NZ, NX, NY), 1.0, 6.0, ((2, 8), (3, 32)), jnp.float32)
    obstacle = with_ends((jax.random.randint(key_list[2], (NZ, NX, NY), 0, 6) < 1).astype(jnp.int32), jax.random.fold_in(key_list[2], 1), 0, 1)
    return {"velocity": velocity, "old_tendency": old_tendency, "obstacle": obstacle}


VISCOSITY = 0.1
TIME_STEP = 0.25
WEIGHT_NEW = 15.0 / 16.0
WEIGHT_OLD = -25.0 / 48.0
HELMHOLTZ = 1.0e-4


def vertical_pair(field):
    zeros_layer = jnp.zeros_like(field[..., :1, :, :])
    upper_cell = jnp.concatenate([field[..., 1:, :, :], zeros_layer], axis=-3)
    lower_cell = jnp.concatenate([zeros_layer, field[..., :-1, :, :]], axis=-3)
    return upper_cell, lower_cell


def vertical_count(size_z):
    layers = jnp.arange(size_z)
    above_ok = (layers < size_z - 1).astype(jnp.float32)
    below_ok = (layers > 0).astype(jnp.float32)
    return (above_ok + below_ok)[:, None, None]


def parity(size_z, size_x, size_y, start_x, start_y):
    layer_z = jnp.arange(size_z, dtype=jnp.int32)[:, None, None]
    row_x = (jnp.arange(size_x, dtype=jnp.int32) + start_x)[None, :, None]
    col_y = (jnp.arange(size_y, dtype=jnp.int32) + start_y)[None, None, :]
    return (layer_z + row_x + col_y) % 2


def gather_neighbours(extended):
    center = extended[:, 1:-1, 1:-1]
    upper_cell, lower_cell = vertical_pair(center)
    neighbours = extended[:, 2:, 1:-1] + extended[:, :-2, 1:-1] + extended[:, 1:-1, 2:] + extended[:, 1:-1, :-2] + upper_cell + lower_cell
    return center, neighbours


def relax_update(extended, source, spacing):
    center, neighbours = gather_neighbours(extended)
    diagonal = HELMHOLTZ + (4.0 + vertical_count(center.shape[0])) / spacing
    return (source + neighbours / spacing) / diagonal


def apply_operator(extended, spacing):
    center, neighbours = gather_neighbours(extended)
    diagonal = HELMHOLTZ + (4.0 + vertical_count(center.shape[0])) / spacing
    return diagonal * center - neighbours / spacing


def wrapped(field):
    return jnp.pad(field, ((0, 0), (1, 1), (1, 1)), mode="wrap")


def restrict(field):
    size_z, size_x, size_y = field.shape
    return field.reshape(size_z // 2, 2, size_x // 2, 2, size_y // 2, 2).mean(axis=(1, 3, 5))


def prolong(field):
    return jnp.repeat(jnp.repeat(jnp.repeat(field, 2, axis=0), 2, axis=1), 2, axis=2)


def global_sweep(field, source, spacing, colour):
    for shade in (0, 1):
        field = jnp.where(colour == shade, relax_update(wrapped(field), source, spacing), field)
    return field


def global_cycle(source, level):
    spacing = float(4 ** level)
    size_z, size_x, size_y = source.shape
    colour = parity(size_z, size_x, size_y, 0, 0)
    field = jnp.zeros_like(source)
    if level == LEVELS:
        for repeat_idx in range(COARSE_SWEEPS):
            field = global_sweep(field, source, spacing, colour)
        return field
    for repeat_idx in range(SWEEPS):
        field = global_sweep(field, source, spacing, colour)
    remain = source - apply_operator(wrapped(field), spacing)
    field = field + prolong(global_cycle(restrict(remain), level + 1))
    for repeat_idx in range(SWEEPS):
        field = global_sweep(field, source, spacing, colour)
    return field


def momentum(velocity, plus_x, minus_x, plus_y, minus_y, old_tendency, fluid):
    upper_cell, lower_cell = vertical_pair(velocity)
    advect = velocity[0] * (plus_x - minus_x) * 0.5 + velocity[1] * (plus_y - minus_y) * 0.5 + velocity[2] * (upper_cell - lower_cell) * 0.5
    diffuse = plus_x + minus_x + plus_y + minus_y + upper_cell + lower_cell - 6.0 * velocity
    tendency = VISCOSITY * diffuse - advect
    return fluid * (velocity + TIME_STEP * (WEIGHT_NEW * tendency + WEIGHT_OLD * old_tendency))


def divergence_of(east_u, west_u, north_v, south_v, predicted):
    upper_cell, lower_cell = vertical_pair(predicted[2])
    return 0.5 * ((east_u - west_u) + (north_v - south_v) + (upper_cell - lower_cell))


def correct(predicted, pressure_ext, pressure, fluid):
    upper_cell, lower_cell = vertical_pair(pressure)
    gradient = jnp.stack([
        0.5 * (pressure_ext[:, 2:, 1:-1] - pressure_ext[:, :-2, 1:-1]),
        0.5 * (pressure_ext[:, 1:-1, 2:] - pressure_ext[:, 1:-1, :-2]),
        0.5 * (upper_cell - lower_cell)])
    return fluid * (predicted - TIME_STEP * gradient)


def reference(velocity, old_tendency, obstacle):
    fluid = (1 - obstacle).astype(jnp.float32)
    predicted = momentum(velocity, jnp.roll(velocity, -1, axis=2), jnp.roll(velocity, 1, axis=2),
                         jnp.roll(velocity, -1, axis=3), jnp.roll(velocity, 1, axis=3), old_tendency, fluid)
    divergence = divergence_of(jnp.roll(predicted[0], -1, axis=1), jnp.roll(predicted[0], 1, axis=1),
                               jnp.roll(predicted[1], -1, axis=2), jnp.roll(predicted[1], 1, axis=2), predicted)
    source = -divergence / TIME_STEP
    pressure = global_cycle(source, 0)
    corrected = correct(predicted, wrapped(pressure), pressure, fluid)
    return corrected, pressure
```

```python
import functools

import jax
import jax.numpy as jnp
from jax import lax
from jax.experimental import pallas as pl
from jax.experimental.pallas import tpu as pltpu
from jax.sharding import PartitionSpec as P

TIME_STEP = 0.25
VISCOSITY = 0.1
WEIGHT_NEW = 15.0 / 16.0
WEIGHT_OLD = -25.0 / 48.0
HELMHOLTZ = 1.0e-4
INTERPRET = False
F32 = jnp.float32
NZ = 32
BX = 16
BY = 128


def vmem(*shape):
    return jax.ShapeDtypeStruct(shape, F32)


def call(kernel, outs, args, scratch=(), in_specs=None, name=None):
    return pl.pallas_call(
        kernel,
        out_shape=outs,
        in_specs=in_specs or [pl.BlockSpec(memory_space=pltpu.VMEM)] * len(args),
        scratch_shapes=[pltpu.VMEM(s, F32) for s in scratch],
        interpret=INTERPRET,
        name=name,
    )(*args)


def turn(a, shift, axis):
    return pltpu.roll(a, shift % a.shape[axis], axis)


def lanes(rows, cols=128):
    return lax.broadcasted_iota(jnp.int32, (rows, cols), 1)


def rows_of(rows, cols=128):
    return lax.broadcasted_iota(jnp.int32, (rows, cols), 0)


def odd_cells(rows, cols):
    return (rows_of(rows, cols) + lanes(rows, cols)) % 2 == 1


def diag(level, m):
    return HELMHOLTZ + (4.0 + m) / float(4**level)


def at_end(colour, k, count, odd, inner, end):
    if k == 0:
        return jnp.where(odd, inner, end) if colour == 0 else jnp.where(odd, end, inner)
    if k == count - 1:
        return jnp.where(odd, end, inner) if colour == 0 else jnp.where(odd, inner, end)
    return inner


def pack(low, high, odd):
    return jnp.where(odd, high, low), jnp.where(odd, low, high)


def scaled(value, level, colour, k, count, odd):
    return value * at_end(colour, k, count, odd, 1.0 / diag(level, 2), 1.0 / diag(level, 1))


def neighbours(src, colour, k, count, odd):
    b = src[k]
    zero = jnp.zeros_like(b)
    above = src[k + 1] if k < count - 1 else zero
    below = src[k - 1] if k > 0 else zero
    z = jnp.where(odd, above, below) if colour == 0 else jnp.where(odd, below, above)
    return turn(b, 1, 0) + turn(b, -1, 0) + turn(b, 1, 1) + turn(b, -1, 1) + (b + z)


def relaxed(src, fd, level, colour, k, count, odd):
    s = float(4**level)
    c = at_end(colour, k, count, odd, 1.0 / s / diag(level, 2), 1.0 / s / diag(level, 1))
    return fd[k] + c * neighbours(src, colour, k, count, odd)


def half_sweep(dst, src, fd, level, colour, count, odd):
    for k in range(count):
        dst[k] = relaxed(src, fd, level, colour, k, count, odd)


def residual(red, black, fd, level, k, count, odd):
    d = at_end(0, k, count, odd, diag(level, 2), diag(level, 1))
    return d * (relaxed(black, fd, level, 0, k, count, odd) - red[k])


def halving(n, m, target):
    i = lax.broadcasted_iota(jnp.int32, (n, m), 0)
    return (i // 2 == target).astype(F32)


def doubling(n, m, target):
    i = lax.broadcasted_iota(jnp.int32, (n, m), 0)
    return (i == target).astype(F32)


def matmul(a, b):
    return jnp.dot(a, b, precision=lax.Precision.HIGHEST, preferred_element_type=F32)


def edges_kernel(vel, row_first, row_last, cols):
    n = 3 * NZ
    row_first[...] = vel[pl.ds(0, n, stride=BX), :]
    row_last[...] = vel[pl.ds(BX - 1, n, stride=BX), :]
    lane = lanes(BX)
    for half in range(2):
        acc = jnp.zeros((BX, BY), F32)
        for j in range(64 * half, min(64 * half + 64, n)):
            v = vel[BX * j : BX * (j + 1), :]
            t = 2 * (j - 64 * half)
            acc = jnp.where(lane == t, turn(v, t, 1), acc)
            acc = jnp.where(lane == t + 1, turn(v, t + 2, 1), acc)
        cols[half] = acc


def momentum_kernel(vel, old, obst, x_low, x_high, c_left, c_right, pred, source, to_low, to_high, mixed):
    lane = lanes(BX)
    row = rows_of(BX)
    for half in range(2):
        mixed[half] = jnp.where(lane % 2 == 0, c_right[half], c_left[half])

    def cut(ref, j):
        return ref[BX * j : BX * (j + 1), :]

    for z in range(NZ):
        fluid = (1 - cut(obst, z)).astype(F32)
        now = [cut(vel, q * NZ + z) for q in range(3)]
        for q in range(3):
            j = q * NZ + z
            v = now[q]
            below_x = jnp.broadcast_to(x_low[j : j + 1, :], (BX, BY))
            above_x = jnp.broadcast_to(x_high[j : j + 1, :], (BX, BY))
            minus_x = jnp.where(row == 0, below_x, turn(v, 1, 0))
            plus_x = jnp.where(row == BX - 1, above_x, turn(v, -1, 0))
            edge = turn(mixed[j // 64], -(2 * (j % 64) + 1), 1)
            minus_y = jnp.where(lane == 0, edge, turn(v, 1, 1))
            plus_y = jnp.where(lane == BY - 1, edge, turn(v, -1, 1))
            zero = jnp.zeros_like(v)
            upper = cut(vel, j + 1) if z < NZ - 1 else zero
            lower = cut(vel, j - 1) if z > 0 else zero
            advect = (now[0] * (plus_x - minus_x) + now[1] * (plus_y - minus_y) + now[2] * (upper - lower)) * 0.5
            diffuse = plus_x + minus_x + plus_y + minus_y + upper + lower - 6.0 * v
            tendency = VISCOSITY * diffuse - advect
            pred[BX * j : BX * (j + 1), :] = fluid * (
                v + TIME_STEP * (WEIGHT_NEW * tendency + WEIGHT_OLD * cut(old, j))
            )
    scale = -0.5 / TIME_STEP
    columns = jnp.zeros((BX, BY), F32)
    for z in range(NZ):
        u = cut(pred, z)
        v = cut(pred, NZ + z)
        zero = jnp.zeros_like(u)
        upper = cut(pred, 2 * NZ + z + 1) if z < NZ - 1 else zero
        lower = cut(pred, 2 * NZ + z - 1) if z > 0 else zero
        east = jnp.where(row == BX - 1, 0.0, turn(u, -1, 0))
        west = jnp.where(row == 0, 0.0, turn(u, 1, 0))
        north = jnp.where(lane == BY - 1, 0.0, turn(v, -1, 1))
        south = jnp.where(lane == 0, 0.0, turn(v, 1, 1))
        s = scale * ((east - west) + (north - south) + (upper - lower))
        source[z] = s
        to_low[z] = s[:8]
        to_high[z] = s[8:]
        columns = jnp.where(lane == 2 * z, turn(v, 2 * z, 1), columns)
        columns = jnp.where(lane == 2 * z + 1, turn(v, 2 * z + 2, 1), columns)
    first = scale * pred[pl.ds(0, NZ, stride=BX), :]
    last = scale * pred[pl.ds(BX - 1, NZ, stride=BX), :]
    for g in range(4):
        to_low[NZ + g] = first[8 * g : 8 * g + 8]
        to_high[NZ + g] = last[8 * g : 8 * g + 8]
    columns = scale * columns
    to_low[NZ + 4] = columns[:8]
    to_high[NZ + 4] = columns[8:]


def widen_x_kernel(source, to_low, to_high, from_low, from_high, wide, to_left, to_right):
    lane = lanes(32)
    row8 = rows_of(8)
    row16 = rows_of(BX)

    def line(ref, z, n):
        g = NZ + z // 8
        r = z % 8
        return jnp.broadcast_to(ref[g, r : r + 1, :], (n, BY))

    for z in range(NZ):
        a = from_low[z] + jnp.where(row8 == 7, line(to_low, z, 8), 0.0)
        c = from_high[z] - jnp.where(row8 == 0, line(to_high, z, 8), 0.0)
        b = source[z]
        b = b - jnp.where(row16 == 0, line(from_low, z, BX), 0.0)
        b = b + jnp.where(row16 == BX - 1, line(from_high, z, BX), 0.0)
        wide[z, 0:8, :] = a
        wide[z, 8:24, :] = b
        wide[z, 24:32, :] = c
    wide[NZ, 0:8, :] = from_low[NZ + 4]
    wide[NZ, 8:16, :] = to_low[NZ + 4]
    wide[NZ, 16:24, :] = to_high[NZ + 4]
    wide[NZ, 24:32, :] = from_high[NZ + 4]
    half = NZ // 2
    for h in range(half):
        a = wide[h]
        b = turn(wide[h + half], 64, 1)
        to_left[h] = jnp.where(lane < 64, a, b)
        to_right[h] = jnp.where(lane < 64, b, a)
    to_left[half] = wide[NZ]
    to_right[half] = wide[NZ]


def fine_down_kernel(wide, from_left, from_right, fd_red, fd_black, black, sent, red, res, thin):
    lane = lanes(32)
    odd = odd_cells(32, 256)
    half = NZ // 2
    slots = NZ // 2
    own = wide[NZ]
    other = jnp.where(lane % 2 == 0, from_right[half], -from_left[half])
    own = jnp.where(lane % 2 == 0, own, -own)

    def layer(z):
        t0 = wide[z]
        h = z % half
        if z < half:
            t1 = jnp.where(lane < 64, from_right[h], from_left[h])
        else:
            t1 = turn(jnp.where(lane < 64, from_left[h], from_right[h]), 64, 1)
        shift = -(2 * z + 1)
        edge = (lane == 0) | (lane == BY - 1)
        t0 = t0 + jnp.where(edge, turn(other, shift, 1), 0.0)
        t1 = t1 + jnp.where(edge, turn(own, shift, 1), 0.0)
        return jnp.concatenate([t0, t1], axis=1)

    for k in range(slots):
        r, b = pack(layer(2 * k), layer(2 * k + 1), odd)
        r = scaled(r, 0, 0, k, slots, odd)
        fd_red[k] = r
        fd_black[k] = scaled(b, 0, 1, k, slots, odd)
    half_sweep(black, fd_red, fd_black, 0, 1, slots, odd)
    half_sweep(red, black, fd_red, 0, 0, slots, odd)
    half_sweep(black, red, fd_black, 0, 1, slots, odd)
    for k in range(slots):
        r = residual(red, black, fd_red, 0, k, slots, odd)
        res[BX * k : BX * (k + 1), :] = r[8:24]
    matrix = 0.125 * halving(256, 128, lax.broadcasted_iota(jnp.int32, (256, 128), 1))
    thin[...] = matmul(res[...], matrix)
    v = thin[pl.ds(0, 8 * slots, stride=2), :] + thin[pl.ds(1, 8 * slots, stride=2), :]
    for k in range(slots):
        for d in range(sent.shape[0]):
            sent[d, k] = v[8 * k : 8 * k + 8]


def middle_down_kernel(nx, index, gathered, fd_red, fd_black, black, coarse, red, res):
    ring = 8 * nx
    slots = 8
    odd8 = odd_cells(8, 128)
    odd = odd_cells(ring, 128)
    for j in range(nx):
        d = lax.rem(index[0] + j, nx)
        for k in range(slots):
            r, b = pack(gathered[d, 2 * k], gathered[d, 2 * k + 1], odd8)
            fd_red[k, 8 * j : 8 * j + 8, :] = scaled(r, 1, 0, k, slots, odd8)
            fd_black[k, 8 * j : 8 * j + 8, :] = scaled(b, 1, 1, k, slots, odd8)
    half_sweep(black, fd_red, fd_black, 1, 1, slots, odd)
    half_sweep(red, black, fd_red, 1, 0, slots, odd)
    half_sweep(black, red, fd_black, 1, 1, slots, odd)
    for k in range(slots):
        res[ring * k : ring * (k + 1), :] = residual(red, black, fd_red, 1, k, slots, odd)
    lane = lax.broadcasted_iota(jnp.int32, (128, 128), 1)
    column = jnp.where(lane < 32, lane, jnp.where(lane < 80, lane - 32, jnp.where(lane < 96, lane - 32, lane - 96)))
    res[...] = matmul(res[...], 0.125 * halving(128, 128, column))
    n = slots * ring // 2
    v = res[pl.ds(0, n, stride=2), :] + res[pl.ds(1, n, stride=2), :]
    for k in range(slots):
        coarse[k] = v[ring // 2 * k : ring // 2 * (k + 1)]


def up_kernel(
    nx, g_own, g_left, g_right, fd1_red, fd1_black, black1_in, fd0_red, fd0_black, black0_in, pred, obst,
    corrected, pressure, fd2_red, fd2_black, red2, black2, res2, fd3, red1, black1, big1, red0, black0, big0,
):
    x2 = 4 * nx
    lane = lanes(x2)
    odd2 = odd_cells(x2, 128)
    slots2 = 4

    def rhs2(z):
        return jnp.where(lane < 32, g_own[z], jnp.where(lane < 80, g_right[z], g_left[z]))

    for k in range(slots2):
        r, b = pack(rhs2(2 * k), rhs2(2 * k + 1), odd2)
        fd2_red[k] = scaled(r, 2, 0, k, slots2, odd2)
        fd2_black[k] = scaled(b, 2, 1, k, slots2, odd2)
    half_sweep(black2, fd2_red, fd2_black, 2, 1, slots2, odd2)
    half_sweep(red2, black2, fd2_red, 2, 0, slots2, odd2)
    half_sweep(black2, red2, fd2_black, 2, 1, slots2, odd2)
    for k in range(slots2):
        res2[x2 * k : x2 * (k + 1), :] = residual(red2, black2, fd2_red, 2, k, slots2, odd2)
    col = lax.broadcasted_iota(jnp.int32, (128, 128), 1)
    res2[...] = matmul(res2[...], 0.125 * halving(128, 128, col % 64))
    n = slots2 * x2 // 2
    x3 = x2 // 2
    fd3[...] = res2[pl.ds(0, n, stride=2), :] + res2[pl.ds(1, n, stride=2), :]

    odd3 = odd_cells(x3, 128)
    fr, fb = [], []
    for k in range(2):
        r, b = pack(fd3[x3 * 2 * k : x3 * (2 * k + 1), :], fd3[x3 * (2 * k + 1) : x3 * (2 * k + 2), :], odd3)
        fr.append(scaled(r, 3, 0, k, 2, odd3))
        fb.append(scaled(b, 3, 1, k, 2, odd3))
    r = fr
    for step in range(8):
        if step > 0:
            r = [relaxed(b, fr, 3, 0, k, 2, odd3) for k in range(2)]
        b = [relaxed(r, fb, 3, 1, k, 2, odd3) for k in range(2)]

    def layers(red, black, odd):
        return jnp.where(odd, black, red), jnp.where(odd, red, black)

    parts = []
    for k in range(2):
        parts += layers(r[k], b[k], odd3)
    e = matmul(jnp.concatenate(parts, axis=0), doubling(128, 128, col // 2))
    res2[pl.ds(0, n, stride=2), :] = e
    res2[pl.ds(1, n, stride=2), :] = e
    for k in range(slots2):
        black2[k] = black2[k] + res2[x2 * k : x2 * (k + 1), :]
    half_sweep(red2, black2, fd2_red, 2, 0, slots2, odd2)
    half_sweep(black2, red2, fd2_black, 2, 1, slots2, odd2)
    half_sweep(red2, black2, fd2_red, 2, 0, slots2, odd2)
    half_sweep(black2, red2, fd2_black, 2, 1, slots2, odd2)

    x1 = 8 * nx
    odd1 = odd_cells(x1, 128)
    slots1 = 8
    for k in range(slots2):
        low, high = layers(red2[k], black2[k], odd2)
        res2[x2 * k : x2 * (k + 1), :] = low
        fd3[0 : x2, :] = high
        big1[x1 * 2 * k : x1 * 2 * k + x2, :] = res2[x2 * k : x2 * (k + 1), :]
        big1[x1 * 2 * k + x2 : x1 * 2 * k + 2 * x2, :] = fd3[0 : x2, :]
    stacked = jnp.concatenate([big1[x1 * 2 * k : x1 * 2 * k + 2 * x2, :] for k in range(slots2)], axis=0)
    e = matmul(stacked, doubling(128, 128, jnp.where(col < 96, col // 2, col // 2 + 64)))
    m = 8 * x2
    big1[pl.ds(0, m, stride=2), :] = e
    big1[pl.ds(1, m, stride=2), :] = e
    for k in range(slots1):
        black1[k] = black1_in[k] + big1[x1 * k : x1 * (k + 1), :]
    half_sweep(red1, black1, fd1_red, 1, 0, slots1, odd1)
    half_sweep(black1, red1, fd1_black, 1, 1, slots1, odd1)
    half_sweep(red1, black1, fd1_red, 1, 0, slots1, odd1)
    half_sweep(black1, red1, fd1_black, 1, 1, slots1, odd1)

    slots0 = NZ // 2
    for k in range(slots1):
        low, high = layers(red1[k], black1[k], odd1)
        for i, v in enumerate((low, high)):
            at = 16 * (2 * k + i)
            big1[at : at + 16, :] = turn(v, 4, 0)[0:16]
    wide_col = lax.broadcasted_iota(jnp.int32, (128, 256), 1)
    e = matmul(big1[0 : 16 * slots0, :], doubling(128, 256, wide_col // 2))
    for t in range(2):
        part = e[:, 128 * t : 128 * t + 128]
        big0[t, pl.ds(0, 16 * slots0, stride=2), :] = part
        big0[t, pl.ds(1, 16 * slots0, stride=2), :] = part
    odd0 = odd_cells(32, 256)
    for k in range(slots0):
        add = jnp.concatenate([big0[t, 32 * k : 32 * (k + 1), :] for t in range(2)], axis=1)
        black0[k] = black0_in[k] + add
    half_sweep(red0, black0, fd0_red, 0, 0, slots0, odd0)
    half_sweep(black0, red0, fd0_black, 0, 1, slots0, odd0)
    half_sweep(red0, black0, fd0_red, 0, 0, slots0, odd0)
    half_sweep(black0, red0, fd0_black, 0, 1, slots0, odd0)
    for k in range(slots0):
        low, high = layers(red0[k], black0[k], odd0)
        red0[k] = low
        black0[k] = high

    def full(z):
        return (black0 if z % 2 else red0)[z // 2]

    for z in range(NZ):
        p = full(z)
        own = p[8:24, 0:128]
        pressure[BX * z : BX * (z + 1), :] = own
        zero = jnp.zeros_like(own)
        upper = full(z + 1)[8:24, 0:128] if z < NZ - 1 else zero
        lower = full(z - 1)[8:24, 0:128] if z > 0 else zero
        gx = turn(p, -1, 0)[8:24, 0:128] - turn(p, 1, 0)[8:24, 0:128]
        mid = p[8:24]
        gy = turn(mid, -1, 1)[:, 0:128] - turn(mid, 1, 1)[:, 0:128]
        fluid = (1 - obst[BX * z : BX * (z + 1), :]).astype(F32)
        for q, g in enumerate((gx, gy, upper - lower)):
            j = q * NZ + z
            v = pred[BX * j : BX * (j + 1), :]
            corrected[BX * j : BX * (j + 1), :] = fluid * (v - (0.5 * TIME_STEP) * g)


def both_ways(axis, to_low, to_high):
    n = lax.axis_size(axis)
    up = [(i, (i + 1) % n) for i in range(n)]
    down = [((i + 1) % n, i) for i in range(n)]
    return lax.ppermute(to_high, axis, up), lax.ppermute(to_low, axis, down)


def body(velocity, old_tendency, obstacle):
    nx = lax.axis_size("gx")
    index = lax.axis_index("gx").astype(jnp.int32).reshape(1)
    vel = velocity.reshape(3 * NZ * BX, BY)
    old = old_tendency.reshape(3 * NZ * BX, BY)
    obst = obstacle.reshape(NZ * BX, BY)

    first, last, cols = call(edges_kernel, (vmem(96, BY), vmem(96, BY), vmem(2, BX, BY)), (vel,), name="edges")
    x_low, x_high = both_ways("gx", first, last)
    c_left, c_right = both_ways("gy", cols, cols)
    pred, source, to_low, to_high = call(
        momentum_kernel,
        (vmem(3 * NZ * BX, BY), vmem(NZ, BX, BY), vmem(37, 8, BY), vmem(37, 8, BY)),
        (vel, old, obst, x_low, x_high, c_left, c_right),
        [(2, BX, BY)],
        name="momentum",
    )
    from_low, from_high = both_ways("gx", to_low, to_high)
    wide, to_left, to_right = call(
        widen_x_kernel,
        (vmem(NZ + 1, 32, BY), vmem(17, 32, BY), vmem(17, 32, BY)),
        (source, to_low, to_high, from_low, from_high),
        name="widen_x",
    )
    from_left, from_right = both_ways("gy", to_left, to_right)
    fd0_red, fd0_black, black0, sent = call(
        fine_down_kernel,
        (vmem(16, 32, 256), vmem(16, 32, 256), vmem(16, 32, 256), vmem(nx, 16, 8, BY)),
        (wide, from_left, from_right),
        [(16, 32, 256), (256, 256), (256, 128)],
        name="fine_down",
    )
    gathered = lax.all_to_all(sent, "gx", 0, 0)
    x1 = 8 * nx
    fd1_red, fd1_black, black1, coarse = call(
        functools.partial(middle_down_kernel, nx),
        (vmem(8, x1, BY), vmem(8, x1, BY), vmem(8, x1, BY), vmem(8, x1 // 2, BY)),
        (index, gathered),
        [(8, x1, BY), (8 * x1, BY)],
        in_specs=[pl.BlockSpec(memory_space=pltpu.SMEM), pl.BlockSpec(memory_space=pltpu.VMEM)],
        name="middle_down",
    )
    g_left, g_right = both_ways("gy", coarse, coarse)
    x2 = x1 // 2
    corrected, pressure = call(
        functools.partial(up_kernel, nx),
        (vmem(3 * NZ * BX, BY), vmem(NZ * BX, BY)),
        (coarse, g_left, g_right, fd1_red, fd1_black, black1, fd0_red, fd0_black, black0, pred, obst),
        [(4, x2, BY)] * 4
        + [(4 * x2, BY), (2 * x2, BY)]
        + [(8, x1, BY)] * 2
        + [(max(8 * x1, 256), BY)]
        + [(16, 32, 256)] * 2
        + [(2, 512, BY)],
        name="up",
    )
    return corrected.reshape(3, NZ, BX, BY), pressure.reshape(NZ, BX, BY)


def solution(mesh):
    placed = (P(None, None, "gx", "gy"), P(None, None, "gx", "gy"), P(None, "gx", "gy"))
    return jax.shard_map(
        body,
        mesh=mesh,
        in_specs=placed,
        out_specs=(P(None, None, "gx", "gy"), P(None, "gx", "gy")),
        check_vma=False,
    )
```

```python
import functools

import jax
import jax.numpy as jnp
from jax import lax
from jax.experimental import pallas as pl
from jax.experimental.pallas import tpu as pltpu
from jax.sharding import PartitionSpec as P

TIME_STEP = 0.25
VISCOSITY = 0.1
WEIGHT_NEW = 15.0 / 16.0
WEIGHT_OLD = -25.0 / 48.0
HELMHOLTZ = 1.0e-4
INTERPRET = False
F32 = jnp.float32
NZ = 32
BX = 16
BY = 128


def vmem(*shape):
    return jax.ShapeDtypeStruct(shape, F32)


def call(kernel, outs, args, scratch=(), in_specs=None, name=None):
    return pl.pallas_call(
        kernel,
        out_shape=outs,
        in_specs=in_specs or [pl.BlockSpec(memory_space=pltpu.VMEM)] * len(args),
        scratch_shapes=[pltpu.VMEM(s, F32) for s in scratch],
        compiler_params=pltpu.CompilerParams(vmem_limit_bytes=16 << 20),
        interpret=INTERPRET,
        name=name,
    )(*args)


def turn(a, shift, axis):
    return pltpu.roll(a, shift % a.shape[axis], axis)


def lanes(rows, cols=128):
    return lax.broadcasted_iota(jnp.int32, (rows, cols), 1)


def rows_of(rows, cols=128):
    return lax.broadcasted_iota(jnp.int32, (rows, cols), 0)


def odd_cells(rows, cols):
    return (rows_of(rows, cols) + lanes(rows, cols)) % 2 == 1


def diag(level, m):
    return HELMHOLTZ + (4.0 + m) / float(4**level)


def at_end(colour, k, count, odd, inner, end):
    if k == 0:
        return jnp.where(odd, inner, end) if colour == 0 else jnp.where(odd, end, inner)
    if k == count - 1:
        return jnp.where(odd, end, inner) if colour == 0 else jnp.where(odd, inner, end)
    return inner


def pack(low, high, odd):
    return jnp.where(odd, high, low), jnp.where(odd, low, high)


def scaled(value, level, colour, k, count, odd):
    return value * at_end(colour, k, count, odd, 1.0 / diag(level, 2), 1.0 / diag(level, 1))


def neighbours(src, colour, k, count, odd):
    b = src[k]
    zero = jnp.zeros_like(b)
    above = src[k + 1] if k < count - 1 else zero
    below = src[k - 1] if k > 0 else zero
    z = jnp.where(odd, above, below) if colour == 0 else jnp.where(odd, below, above)
    return turn(b, 1, 0) + turn(b, -1, 0) + turn(b, 1, 1) + turn(b, -1, 1) + (b + z)


def relaxed(src, fd, level, colour, k, count, odd):
    s = float(4**level)
    c = at_end(colour, k, count, odd, 1.0 / s / diag(level, 2), 1.0 / s / diag(level, 1))
    return fd[k] + c * neighbours(src, colour, k, count, odd)


def half_sweep(dst, src, fd, level, colour, count, odd):
    for k in range(count):
        dst[k] = relaxed(src, fd, level, colour, k, count, odd)


def residual(red, black, fd, level, k, count, odd):
    d = at_end(0, k, count, odd, diag(level, 2), diag(level, 1))
    return d * (relaxed(black, fd, level, 0, k, count, odd) - red[k])


def halving(n, m, target):
    i = lax.broadcasted_iota(jnp.int32, (n, m), 0)
    return (i // 2 == target).astype(F32)


def doubling(n, m, target):
    i = lax.broadcasted_iota(jnp.int32, (n, m), 0)
    return (i == target).astype(F32)


def matmul(a, b):
    return jnp.dot(a, b, precision=lax.Precision.HIGHEST, preferred_element_type=F32)


def edges_kernel(vel, row_first, row_last, cols):
    n = 3 * NZ
    row_first[...] = vel[pl.ds(0, n, stride=BX), :]
    row_last[...] = vel[pl.ds(BX - 1, n, stride=BX), :]
    lane = lanes(BX)
    for half in range(2):
        acc = jnp.zeros((BX, BY), F32)
        for j in range(64 * half, min(64 * half + 64, n)):
            v = vel[BX * j : BX * (j + 1), :]
            t = 2 * (j - 64 * half)
            acc = jnp.where(lane == t, turn(v, t, 1), acc)
            acc = jnp.where(lane == t + 1, turn(v, t + 2, 1), acc)
        cols[half] = acc


def momentum_kernel(vel, old, obst, x_low, x_high, c_left, c_right, pred, source, to_low, to_high, mixed):
    lane = lanes(BX)
    row = rows_of(BX)
    for half in range(2):
        mixed[half] = jnp.where(lane % 2 == 0, c_right[half], c_left[half])

    def cut(ref, j):
        return ref[BX * j : BX * (j + 1), :]

    for z in range(NZ):
        fluid = (1 - cut(obst, z)).astype(F32)
        now = [cut(vel, q * NZ + z) for q in range(3)]
        for q in range(3):
            j = q * NZ + z
            v = now[q]
            below_x = jnp.broadcast_to(x_low[j : j + 1, :], (BX, BY))
            above_x = jnp.broadcast_to(x_high[j : j + 1, :], (BX, BY))
            minus_x = jnp.where(row == 0, below_x, turn(v, 1, 0))
            plus_x = jnp.where(row == BX - 1, above_x, turn(v, -1, 0))
            edge = turn(mixed[j // 64], -(2 * (j % 64) + 1), 1)
            minus_y = jnp.where(lane == 0, edge, turn(v, 1, 1))
            plus_y = jnp.where(lane == BY - 1, edge, turn(v, -1, 1))
            zero = jnp.zeros_like(v)
            upper = cut(vel, j + 1) if z < NZ - 1 else zero
            lower = cut(vel, j - 1) if z > 0 else zero
            advect = (now[0] * (plus_x - minus_x) + now[1] * (plus_y - minus_y) + now[2] * (upper - lower)) * 0.5
            diffuse = plus_x + minus_x + plus_y + minus_y + upper + lower - 6.0 * v
            tendency = VISCOSITY * diffuse - advect
            pred[BX * j : BX * (j + 1), :] = fluid * (
                v + TIME_STEP * (WEIGHT_NEW * tendency + WEIGHT_OLD * cut(old, j))
            )
    scale = -0.5 / TIME_STEP
    columns = jnp.zeros((BX, BY), F32)
    for z in range(NZ):
        u = cut(pred, z)
        v = cut(pred, NZ + z)
        zero = jnp.zeros_like(u)
        upper = cut(pred, 2 * NZ + z + 1) if z < NZ - 1 else zero
        lower = cut(pred, 2 * NZ + z - 1) if z > 0 else zero
        east = jnp.where(row == BX - 1, 0.0, turn(u, -1, 0))
        west = jnp.where(row == 0, 0.0, turn(u, 1, 0))
        north = jnp.where(lane == BY - 1, 0.0, turn(v, -1, 1))
        south = jnp.where(lane == 0, 0.0, turn(v, 1, 1))
        s = scale * ((east - west) + (north - south) + (upper - lower))
        source[z] = s
        to_low[z] = s[:8]
        to_high[z] = s[8:]
        columns = jnp.where(lane == 2 * z, turn(v, 2 * z, 1), columns)
        columns = jnp.where(lane == 2 * z + 1, turn(v, 2 * z + 2, 1), columns)
    first = scale * pred[pl.ds(0, NZ, stride=BX), :]
    last = scale * pred[pl.ds(BX - 1, NZ, stride=BX), :]
    for g in range(4):
        to_low[NZ + g] = first[8 * g : 8 * g + 8]
        to_high[NZ + g] = last[8 * g : 8 * g + 8]
    columns = scale * columns
    to_low[NZ + 4] = columns[:8]
    to_high[NZ + 4] = columns[8:]


def widen_x_kernel(source, to_low, to_high, from_low, from_high, wide, to_left, to_right):
    lane = lanes(32)
    row8 = rows_of(8)
    row16 = rows_of(BX)

    def line(ref, z, n):
        g = NZ + z // 8
        r = z % 8
        return jnp.broadcast_to(ref[g, r : r + 1, :], (n, BY))

    for z in range(NZ):
        a = from_low[z] + jnp.where(row8 == 7, line(to_low, z, 8), 0.0)
        c = from_high[z] - jnp.where(row8 == 0, line(to_high, z, 8), 0.0)
        b = source[z]
        b = b - jnp.where(row16 == 0, line(from_low, z, BX), 0.0)
        b = b + jnp.where(row16 == BX - 1, line(from_high, z, BX), 0.0)
        wide[z, 0:8, :] = a
        wide[z, 8:24, :] = b
        wide[z, 24:32, :] = c
    wide[NZ, 0:8, :] = from_low[NZ + 4]
    wide[NZ, 8:16, :] = to_low[NZ + 4]
    wide[NZ, 16:24, :] = to_high[NZ + 4]
    wide[NZ, 24:32, :] = from_high[NZ + 4]
    half = NZ // 2
    for h in range(half):
        a = wide[h]
        b = turn(wide[h + half], 64, 1)
        to_left[h] = jnp.where(lane < 64, a, b)
        to_right[h] = jnp.where(lane < 64, b, a)
    to_left[half] = wide[NZ]
    to_right[half] = wide[NZ]


def fine_down_kernel(wide, from_left, from_right, fd_red, fd_black, black, sent, red, res, thin):
    lane = lanes(32)
    odd = odd_cells(32, 256)
    half = NZ // 2
    slots = NZ // 2
    own = wide[NZ]
    other = jnp.where(lane % 2 == 0, from_right[half], -from_left[half])
    own = jnp.where(lane % 2 == 0, own, -own)

    def layer(z):
        t0 = wide[z]
        h = z % half
        if z < half:
            t1 = jnp.where(lane < 64, from_right[h], from_left[h])
        else:
            t1 = turn(jnp.where(lane < 64, from_left[h], from_right[h]), 64, 1)
        shift = -(2 * z + 1)
        edge = (lane == 0) | (lane == BY - 1)
        t0 = t0 + jnp.where(edge, turn(other, shift, 1), 0.0)
        t1 = t1 + jnp.where(edge, turn(own, shift, 1), 0.0)
        return jnp.concatenate([t0, t1], axis=1)

    for k in range(slots):
        r, b = pack(layer(2 * k), layer(2 * k + 1), odd)
        r = scaled(r, 0, 0, k, slots, odd)
        fd_red[k] = r
        fd_black[k] = scaled(b, 0, 1, k, slots, odd)
    half_sweep(black, fd_red, fd_black, 0, 1, slots, odd)
    half_sweep(red, black, fd_red, 0, 0, slots, odd)
    half_sweep(black, red, fd_black, 0, 1, slots, odd)
    for k in range(slots):
        r = residual(red, black, fd_red, 0, k, slots, odd)
        res[BX * k : BX * (k + 1), :] = r[8:24]
    matrix = 0.125 * halving(256, 128, lax.broadcasted_iota(jnp.int32, (256, 128), 1))
    thin[...] = matmul(res[...], matrix)
    v = thin[pl.ds(0, 8 * slots, stride=2), :] + thin[pl.ds(1, 8 * slots, stride=2), :]
    for k in range(slots):
        for d in range(sent.shape[0]):
            sent[d, k] = v[8 * k : 8 * k + 8]


def middle_down_kernel(nx, index, gathered, fd_red, fd_black, black, coarse, red, res):
    ring = 8 * nx
    slots = 8
    odd8 = odd_cells(8, 128)
    odd = odd_cells(ring, 128)
    for j in range(nx):
        d = lax.rem(index[0] + j, nx)
        for k in range(slots):
            r, b = pack(gathered[d, 2 * k], gathered[d, 2 * k + 1], odd8)
            fd_red[k, 8 * j : 8 * j + 8, :] = scaled(r, 1, 0, k, slots, odd8)
            fd_black[k, 8 * j : 8 * j + 8, :] = scaled(b, 1, 1, k, slots, odd8)
    half_sweep(black, fd_red, fd_black, 1, 1, slots, odd)
    half_sweep(red, black, fd_red, 1, 0, slots, odd)
    half_sweep(black, red, fd_black, 1, 1, slots, odd)
    for k in range(slots):
        res[ring * k : ring * (k + 1), :] = residual(red, black, fd_red, 1, k, slots, odd)
    lane = lax.broadcasted_iota(jnp.int32, (128, 128), 1)
    column = jnp.where(lane < 32, lane, jnp.where(lane < 80, lane - 32, jnp.where(lane < 96, lane - 32, lane - 96)))
    res[...] = matmul(res[...], 0.125 * halving(128, 128, column))
    n = slots * ring // 2
    v = res[pl.ds(0, n, stride=2), :] + res[pl.ds(1, n, stride=2), :]
    for k in range(slots):
        coarse[k] = v[ring // 2 * k : ring // 2 * (k + 1)]


def up_kernel(
    nx, g_own, g_left, g_right, fd1_red, fd1_black, black1_in, fd0_red, fd0_black, black0_in, pred, obst,
    corrected, pressure, fd2_red, fd2_black, red2, black2, res2, fd3, red1, black1, big1, red0, black0, big0,
):
    x2 = 4 * nx
    lane = lanes(x2)
    odd2 = odd_cells(x2, 128)
    slots2 = 4

    def rhs2(z):
        return jnp.where(lane < 32, g_own[z], jnp.where(lane < 80, g_right[z], g_left[z]))

    for k in range(slots2):
        r, b = pack(rhs2(2 * k), rhs2(2 * k + 1), odd2)
        fd2_red[k] = scaled(r, 2, 0, k, slots2, odd2)
        fd2_black[k] = scaled(b, 2, 1, k, slots2, odd2)
    half_sweep(black2, fd2_red, fd2_black, 2, 1, slots2, odd2)
    half_sweep(red2, black2, fd2_red, 2, 0, slots2, odd2)
    half_sweep(black2, red2, fd2_black, 2, 1, slots2, odd2)
    for k in range(slots2):
        res2[x2 * k : x2 * (k + 1), :] = residual(red2, black2, fd2_red, 2, k, slots2, odd2)
    col = lax.broadcasted_iota(jnp.int32, (128, 128), 1)
    res2[...] = matmul(res2[...], 0.125 * halving(128, 128, col % 64))
    n = slots2 * x2 // 2
    x3 = x2 // 2
    fd3[...] = res2[pl.ds(0, n, stride=2), :] + res2[pl.ds(1, n, stride=2), :]

    odd3 = odd_cells(x3, 128)
    fr, fb = [], []
    for k in range(2):
        r, b = pack(fd3[x3 * 2 * k : x3 * (2 * k + 1), :], fd3[x3 * (2 * k + 1) : x3 * (2 * k + 2), :], odd3)
        fr.append(scaled(r, 3, 0, k, 2, odd3))
        fb.append(scaled(b, 3, 1, k, 2, odd3))
    r = fr
    for step in range(8):
        if step > 0:
            r = [relaxed(b, fr, 3, 0, k, 2, odd3) for k in range(2)]
        b = [relaxed(r, fb, 3, 1, k, 2, odd3) for k in range(2)]

    def layers(red, black, odd):
        return jnp.where(odd, black, red), jnp.where(odd, red, black)

    parts = []
    for k in range(2):
        parts += layers(r[k], b[k], odd3)
    e = matmul(jnp.concatenate(parts, axis=0), doubling(128, 128, col // 2))
    res2[pl.ds(0, n, stride=2), :] = e
    res2[pl.ds(1, n, stride=2), :] = e
    for k in range(slots2):
        black2[k] = black2[k] + res2[x2 * k : x2 * (k + 1), :]
    half_sweep(red2, black2, fd2_red, 2, 0, slots2, odd2)
    half_sweep(black2, red2, fd2_black, 2, 1, slots2, odd2)
    half_sweep(red2, black2, fd2_red, 2, 0, slots2, odd2)
    half_sweep(black2, red2, fd2_black, 2, 1, slots2, odd2)

    x1 = 8 * nx
    odd1 = odd_cells(x1, 128)
    slots1 = 8
    for k in range(slots2):
        low, high = layers(red2[k], black2[k], odd2)
        res2[x2 * k : x2 * (k + 1), :] = low
        fd3[0 : x2, :] = high
        big1[x1 * 2 * k : x1 * 2 * k + x2, :] = res2[x2 * k : x2 * (k + 1), :]
        big1[x1 * 2 * k + x2 : x1 * 2 * k + 2 * x2, :] = fd3[0 : x2, :]
    stacked = jnp.concatenate([big1[x1 * 2 * k : x1 * 2 * k + 2 * x2, :] for k in range(slots2)], axis=0)
    e = matmul(stacked, doubling(128, 128, jnp.where(col < 96, col // 2, col // 2 + 64)))
    m = 8 * x2
    big1[pl.ds(0, m, stride=2), :] = e
    big1[pl.ds(1, m, stride=2), :] = e
    for k in range(slots1):
        black1[k] = black1_in[k] + big1[x1 * k : x1 * (k + 1), :]
    half_sweep(red1, black1, fd1_red, 1, 0, slots1, odd1)
    half_sweep(black1, red1, fd1_black, 1, 1, slots1, odd1)
    half_sweep(red1, black1, fd1_red, 1, 0, slots1, odd1)
    half_sweep(black1, red1, fd1_black, 1, 1, slots1, odd1)

    slots0 = NZ // 2
    for k in range(slots1):
        low, high = layers(red1[k], black1[k], odd1)
        for i, v in enumerate((low, high)):
            at = 16 * (2 * k + i)
            big1[at : at + 16, :] = turn(v, 4, 0)[0:16]
    wide_col = lax.broadcasted_iota(jnp.int32, (128, 256), 1)
    e = matmul(big1[0 : 16 * slots0, :], doubling(128, 256, wide_col // 2))
    for t in range(2):
        part = e[:, 128 * t : 128 * t + 128]
        big0[t, pl.ds(0, 16 * slots0, stride=2), :] = part
        big0[t, pl.ds(1, 16 * slots0, stride=2), :] = part
    odd0 = odd_cells(32, 256)
    for k in range(slots0):
        add = jnp.concatenate([big0[t, 32 * k : 32 * (k + 1), :] for t in range(2)], axis=1)
        black0[k] = black0_in[k] + add
    half_sweep(red0, black0, fd0_red, 0, 0, slots0, odd0)
    half_sweep(black0, red0, fd0_black, 0, 1, slots0, odd0)
    half_sweep(red0, black0, fd0_red, 0, 0, slots0, odd0)
    half_sweep(black0, red0, fd0_black, 0, 1, slots0, odd0)
    for k in range(slots0):
        low, high = layers(red0[k], black0[k], odd0)
        red0[k] = low
        black0[k] = high

    def full(z):
        return (black0 if z % 2 else red0)[z // 2]

    for z in range(NZ):
        p = full(z)
        own = p[8:24, 0:128]
        pressure[BX * z : BX * (z + 1), :] = own
        zero = jnp.zeros_like(own)
        upper = full(z + 1)[8:24, 0:128] if z < NZ - 1 else zero
        lower = full(z - 1)[8:24, 0:128] if z > 0 else zero
        gx = turn(p, -1, 0)[8:24, 0:128] - turn(p, 1, 0)[8:24, 0:128]
        mid = p[8:24]
        gy = turn(mid, -1, 1)[:, 0:128] - turn(mid, 1, 1)[:, 0:128]
        fluid = (1 - obst[BX * z : BX * (z + 1), :]).astype(F32)
        for q, g in enumerate((gx, gy, upper - lower)):
            j = q * NZ + z
            v = pred[BX * j : BX * (j + 1), :]
            corrected[BX * j : BX * (j + 1), :] = fluid * (v - (0.5 * TIME_STEP) * g)


def both_ways(axis, to_low, to_high):
    n = lax.axis_size(axis)
    up = [(i, (i + 1) % n) for i in range(n)]
    down = [((i + 1) % n, i) for i in range(n)]
    return lax.ppermute(to_high, axis, up), lax.ppermute(to_low, axis, down)


def body(velocity, old_tendency, obstacle):
    nx = lax.axis_size("gx")
    index = lax.axis_index("gx").astype(jnp.int32).reshape(1)
    vel = velocity.reshape(3 * NZ * BX, BY)
    old = old_tendency.reshape(3 * NZ * BX, BY)
    obst = obstacle.reshape(NZ * BX, BY)

    first, last, cols = call(edges_kernel, (vmem(96, BY), vmem(96, BY), vmem(2, BX, BY)), (vel,), name="edges")
    x_low, x_high = both_ways("gx", first, last)
    c_left, c_right = both_ways("gy", cols, cols)
    pred, source, to_low, to_high = call(
        momentum_kernel,
        (vmem(3 * NZ * BX, BY), vmem(NZ, BX, BY), vmem(37, 8, BY), vmem(37, 8, BY)),
        (vel, old, obst, x_low, x_high, c_left, c_right),
        [(2, BX, BY)],
        name="momentum",
    )
    from_low, from_high = both_ways("gx", to_low, to_high)
    wide, to_left, to_right = call(
        widen_x_kernel,
        (vmem(NZ + 1, 32, BY), vmem(17, 32, BY), vmem(17, 32, BY)),
        (source, to_low, to_high, from_low, from_high),
        name="widen_x",
    )
    from_left, from_right = both_ways("gy", to_left, to_right)
    fd0_red, fd0_black, black0, sent = call(
        fine_down_kernel,
        (vmem(16, 32, 256), vmem(16, 32, 256), vmem(16, 32, 256), vmem(nx, 16, 8, BY)),
        (wide, from_left, from_right),
        [(16, 32, 256), (256, 256), (256, 128)],
        name="fine_down",
    )
    gathered = lax.all_to_all(sent, "gx", 0, 0)
    x1 = 8 * nx
    fd1_red, fd1_black, black1, coarse = call(
        functools.partial(middle_down_kernel, nx),
        (vmem(8, x1, BY), vmem(8, x1, BY), vmem(8, x1, BY), vmem(8, x1 // 2, BY)),
        (index, gathered),
        [(8, x1, BY), (8 * x1, BY)],
        in_specs=[pl.BlockSpec(memory_space=pltpu.SMEM), pl.BlockSpec(memory_space=pltpu.VMEM)],
        name="middle_down",
    )
    g_left, g_right = both_ways("gy", coarse, coarse)
    x2 = x1 // 2
    corrected, pressure = call(
        functools.partial(up_kernel, nx),
        (vmem(3 * NZ * BX, BY), vmem(NZ * BX, BY)),
        (coarse, g_left, g_right, fd1_red, fd1_black, black1, fd0_red, fd0_black, black0, pred, obst),
        [(4, x2, BY)] * 4
        + [(4 * x2, BY), (2 * x2, BY)]
        + [(8, x1, BY)] * 2
        + [(max(8 * x1, 256), BY)]
        + [(16, 32, 256)] * 2
        + [(2, 512, BY)],
        name="up",
    )
    return corrected.reshape(3, NZ, BX, BY), pressure.reshape(NZ, BX, BY)


def solution(mesh):
    placed = (P(None, None, "gx", "gy"), P(None, None, "gx", "gy"), P(None, "gx", "gy"))
    return jax.shard_map(
        body,
        mesh=mesh,
        in_specs=placed,
        out_specs=(P(None, None, "gx", "gy"), P(None, "gx", "gy")),
        check_vma=False,
    )
```

```python
import functools

import jax
import jax.numpy as jnp
from jax import lax
from jax.experimental import pallas as pl
from jax.experimental.pallas import tpu as pltpu
from jax.sharding import PartitionSpec as P

TIME_STEP = 0.25
VISCOSITY = 0.1
WEIGHT_NEW = 15.0 / 16.0
WEIGHT_OLD = -25.0 / 48.0
HELMHOLTZ = 1.0e-4
SCALE = -0.5 / TIME_STEP
INTERPRET = False
F32 = jnp.float32
NZ = 32
BX = 16
BY = 128


def vmem(*shape):
    return jax.ShapeDtypeStruct(shape, F32)


def call(kernel, outs, args, scratch=(), in_specs=None, name=None):
    return pl.pallas_call(
        kernel,
        out_shape=outs,
        in_specs=in_specs or [pl.BlockSpec(memory_space=pltpu.VMEM)] * len(args),
        scratch_shapes=[pltpu.VMEM(s, F32) for s in scratch],
        compiler_params=pltpu.CompilerParams(vmem_limit_bytes=16 << 20),
        interpret=INTERPRET,
        name=name,
    )(*args)


def turn(a, shift, axis):
    return pltpu.roll(a, shift % a.shape[axis], axis)


def lanes(rows, cols=128):
    return lax.broadcasted_iota(jnp.int32, (rows, cols), 1)


def rows_of(rows, cols=128):
    return lax.broadcasted_iota(jnp.int32, (rows, cols), 0)


def odd_cells(rows, cols):
    return (rows_of(rows, cols) + lanes(rows, cols)) % 2 == 1


def diag(level, m):
    return HELMHOLTZ + (4.0 + m) / float(4**level)


def at_end(colour, k, count, odd, inner, end):
    if k == 0:
        return jnp.where(odd, inner, end) if colour == 0 else jnp.where(odd, end, inner)
    if k == count - 1:
        return jnp.where(odd, end, inner) if colour == 0 else jnp.where(odd, inner, end)
    return inner


def pack(low, high, odd):
    return jnp.where(odd, high, low), jnp.where(odd, low, high)


def scaled(value, level, colour, k, count, odd):
    return value * at_end(colour, k, count, odd, 1.0 / diag(level, 2), 1.0 / diag(level, 1))


def neighbours(src, colour, k, count, odd):
    b = src[k]
    zero = jnp.zeros_like(b)
    above = src[k + 1] if k < count - 1 else zero
    below = src[k - 1] if k > 0 else zero
    z = jnp.where(odd, above, below) if colour == 0 else jnp.where(odd, below, above)
    return turn(b, 1, 0) + turn(b, -1, 0) + turn(b, 1, 1) + turn(b, -1, 1) + (b + z)


def relaxed(src, fd, level, colour, k, count, odd):
    s = float(4**level)
    c = at_end(colour, k, count, odd, 1.0 / s / diag(level, 2), 1.0 / s / diag(level, 1))
    return fd[k] + c * neighbours(src, colour, k, count, odd)


def half_sweep(dst, src, fd, level, colour, count, odd):
    for k in range(count):
        dst[k] = relaxed(src, fd, level, colour, k, count, odd)


def residual(red, black, fd, level, k, count, odd):
    d = at_end(0, k, count, odd, diag(level, 2), diag(level, 1))
    return d * (relaxed(black, fd, level, 0, k, count, odd) - red[k])


def halving(n, m, target):
    i = lax.broadcasted_iota(jnp.int32, (n, m), 0)
    return (i // 2 == target).astype(F32)


def doubling(n, m, target):
    i = lax.broadcasted_iota(jnp.int32, (n, m), 0)
    return (i == target).astype(F32)


def matmul(a, b):
    return jnp.dot(a, b, precision=lax.Precision.HIGHEST, preferred_element_type=F32)


def local_kernel(vel, old, obst, pred, source, to_low, to_high, edge_x):
    lane = lanes(BX)
    row = rows_of(BX)

    def cut(ref, j):
        return ref[BX * j : BX * (j + 1), :]

    packs = [jnp.zeros((BX, BY), F32) for _ in range(3)]

    def put(pack, value, at):
        return jnp.where((lane == at) | (lane == at + 1), turn(value, at + 1, 1), pack)

    for z in range(NZ):
        fluid = (1 - cut(obst, z)).astype(F32)
        now = [cut(vel, q * NZ + z) for q in range(3)]
        for q in range(3):
            j = q * NZ + z
            v = now[q]
            minus_x = jnp.where(row == 0, 0.0, turn(v, 1, 0))
            plus_x = jnp.where(row == BX - 1, 0.0, turn(v, -1, 0))
            minus_y = jnp.where(lane == 0, 0.0, turn(v, 1, 1))
            plus_y = jnp.where(lane == BY - 1, 0.0, turn(v, -1, 1))
            zero = jnp.zeros_like(v)
            upper = cut(vel, j + 1) if z < NZ - 1 else zero
            lower = cut(vel, j - 1) if z > 0 else zero
            advect = (now[0] * (plus_x - minus_x) + now[1] * (plus_y - minus_y) + now[2] * (upper - lower)) * 0.5
            diffuse = plus_x + minus_x + plus_y + minus_y + upper + lower - 6.0 * v
            tendency = VISCOSITY * diffuse - advect
            p = fluid * (v + TIME_STEP * (WEIGHT_NEW * tendency + WEIGHT_OLD * cut(old, j)))
            pred[BX * j : BX * (j + 1), :] = p
            if q == 1:
                pv = p
        weight = (TIME_STEP * WEIGHT_NEW) * fluid
        across_x = weight * (VISCOSITY + jnp.where(row == 0, 0.5, -0.5) * now[0])
        across_x = jnp.where((row == 0) | (row == BX - 1), across_x, 0.0)
        across_y = weight * (VISCOSITY + jnp.where(lane == 0, 0.5, -0.5) * now[1])
        edge_x[BX * z : BX * (z + 1), :] = across_x
        for t, pair in enumerate(((now[0], now[1]), (now[2], across_y), (pv, across_x))):
            for i in range(2):
                packs[t] = put(packs[t], pair[i], 64 * i + 2 * z)
    for z in range(NZ):
        u = cut(pred, z)
        v = cut(pred, NZ + z)
        zero = jnp.zeros_like(u)
        upper = cut(pred, 2 * NZ + z + 1) if z < NZ - 1 else zero
        lower = cut(pred, 2 * NZ + z - 1) if z > 0 else zero
        east = jnp.where(row == BX - 1, 0.0, turn(u, -1, 0))
        west = jnp.where(row == 0, 0.0, turn(u, 1, 0))
        north = jnp.where(lane == BY - 1, 0.0, turn(v, -1, 1))
        south = jnp.where(lane == 0, 0.0, turn(v, 1, 1))
        s = SCALE * ((east - west) + (north - south) + (upper - lower))
        source[BX * z : BX * (z + 1), :] = s
        to_low[8 * z : 8 * z + 8, :] = s[:8]
        to_high[8 * z : 8 * z + 8, :] = s[8:]
    for ref, r in ((to_low, 0), (to_high, BX - 1)):
        at = 8 * NZ
        ref[at : at + NZ, :] = edge_x[pl.ds(r, NZ, stride=BX), :]
        ref[at + NZ : at + 4 * NZ, :] = vel[pl.ds(r, 3 * NZ, stride=BX), :]
        ref[at + 4 * NZ : at + 5 * NZ, :] = pred[pl.ds(r, NZ, stride=BX), :]
        for t in range(3):
            ref[at + 5 * NZ + BX * t : at + 5 * NZ + BX * (t + 1), :] = packs[t]


def join_x_kernel(source, to_low, to_high, from_low, from_high, wide, to_left, to_right, fix_rows):
    lane = lanes(NZ)
    layer = rows_of(NZ)

    def line(ref, i):
        at = 8 * NZ + NZ * i
        return ref[at : at + NZ, :]

    def slope_y(f):
        return jnp.where(lane == BY - 1, 0.0, turn(f, -1, 1)) - jnp.where(lane == 0, 0.0, turn(f, 1, 1))

    def slope_z(f):
        return jnp.where(layer == NZ - 1, 0.0, turn(f, -1, 0)) - jnp.where(layer == 0, 0.0, turn(f, 1, 0))

    for z in range(NZ):
        wide[32 * z : 32 * z + 8, :] = from_low[8 * z : 8 * z + 8, :]
        wide[32 * z + 8 : 32 * z + 24, :] = source[BX * z : BX * (z + 1), :]
        wide[32 * z + 24 : 32 * z + 32, :] = from_high[8 * z : 8 * z + 8, :]

    def add(row, value):
        at = pl.ds(row, NZ, stride=32)
        wide[at, :] = wide[at, :] + SCALE * value

    for near, far, row, step, sign in ((to_low, from_low, 8, -1, 1.0), (to_high, from_high, 23, 1, -1.0)):
        inner = [line(near, 0) * line(far, 1 + q) for q in range(3)]
        outer = [line(far, 0) * line(near, 1 + q) for q in range(3)]
        add(row - step, -sign * inner[0])
        add(row, -sign * (line(far, 4) + outer[0]) + slope_y(inner[1]) + slope_z(inner[2]))
        add(row + step, sign * (line(near, 4) + inner[0]) + slope_y(outer[1]) + slope_z(outer[2]))
        add(row + 2 * step, sign * outer[0])
        for q in range(3):
            at = NZ * (3 * (step > 0) + q)
            fix_rows[at : at + NZ, :] = inner[q]

    stack = []
    for t in range(3):
        at = 13 * NZ + BX * t
        stack.append(jnp.concatenate([ref[at : at + BX, :] for ref in (from_low, to_low, from_high)], axis=0))
    first = rows_of(48) % BX == 0
    other = jnp.where(first, turn(stack[0], 1, 0), turn(stack[0], -1, 0))
    stack[2] = stack[2] + turn(stack[2] * other, 64, 1)
    half = NZ // 2
    lane = lanes(32)
    for h in range(half):
        a = wide[32 * h : 32 * h + 32, :]
        b = turn(wide[32 * (h + half) : 32 * (h + half) + 32, :], 64, 1)
        to_left[32 * h : 32 * h + 32, :] = jnp.where(lane < 64, a, b)
        to_right[32 * h : 32 * h + 32, :] = jnp.where(lane < 64, b, a)
    for t in range(3):
        at = 32 * half + 48 * t
        to_left[at : at + 48, :] = stack[t]
        to_right[at : at + 48, :] = stack[t]


def fine_down_kernel(
    wide, sent_left, from_left, from_right, fd_red, fd_black, black, sent, fix_cols, red, res, thin
):
    lane = lanes(32)
    odd = odd_cells(32, 256)
    half = NZ // 2
    slots = NZ // 2

    lane48 = lanes(48)
    even = lane48 % 2 == 0
    low_half = lane48 < 64

    def pack_of(ref, t):
        at = 32 * half + 48 * t
        return ref[at : at + 48, :]

    def swap(f):
        return turn(f, 64, 1)

    def both(f):
        return jnp.where(low_half, swap(f), f)

    def facing(left, right):
        return jnp.where(even, turn(right, -1, 1), turn(left, 1, 1))

    def slope_x(f):
        return turn(f, -1, 0) - turn(f, 1, 0)

    def slope_z(f):
        above = jnp.where(lane48 >= 2 * NZ - 2, 0.0, turn(f, -2, 1))
        below = jnp.where(lane48 < 2, 0.0, turn(f, 2, 1))
        return above - below

    def signed(f):
        return jnp.where(even, f, -f)

    own = [pack_of(sent_left, t) for t in range(3)]
    left = [pack_of(from_left, t) for t in range(3)]
    right = [pack_of(from_right, t) for t in range(3)]
    near = both(own[1])
    inner_uv = near * facing(left[0], right[0])
    inner_w = near * facing(left[1], right[1])
    far = both(jnp.where(even, left[1], right[1]))
    outer_uv = far * facing(own[0], own[0])
    outer_w = far * facing(own[1], own[1])
    inner_v = swap(inner_uv)
    outer_v = swap(outer_uv)
    pv_far = jnp.where(even, left[2], right[2]) + outer_v
    pv_own = own[2] + inner_v
    e0 = signed(facing(pv_far, pv_far)) + slope_x(inner_uv) + slope_z(inner_w)
    e1 = signed(facing(pv_own, pv_own)) + slope_x(outer_uv) + slope_z(outer_w)
    i = lax.broadcasted_iota(jnp.int32, (128, 128), 0)
    j = lax.broadcasted_iota(jnp.int32, (128, 128), 1)
    side = i % 2
    to = 4 * ((i % 64) // 2) + jnp.where(i < 64, 1 + side, 3 * side)
    order = SCALE * (to == j).astype(F32)
    mixed = []
    for e, v in ((e0, inner_v), (e1, outer_v)):
        mixed.append(matmul(jnp.where(low_half, e, swap(signed(v)))[8:40], order))
    fix_cols[0] = inner_uv[16:32]
    fix_cols[1] = inner_w[16:32]
    edge = (lane < 2) | (lane >= BY - 2)

    def layer(z):
        t0 = wide[32 * z : 32 * z + 32, :]
        h = z % half
        a = from_right[32 * h : 32 * h + 32, :]
        b = from_left[32 * h : 32 * h + 32, :]
        if z < half:
            t1 = jnp.where(lane < 64, a, b)
        else:
            t1 = turn(jnp.where(lane < 64, b, a), 64, 1)
        t0 = t0 + jnp.where(edge, turn(mixed[0], 126 - 4 * z, 1), 0.0)
        t1 = t1 + jnp.where(edge, turn(mixed[1], 126 - 4 * z, 1), 0.0)
        return jnp.concatenate([t0, t1], axis=1)

    for k in range(slots):
        r, b = pack(layer(2 * k), layer(2 * k + 1), odd)
        fd_red[k] = scaled(r, 0, 0, k, slots, odd)
        fd_black[k] = scaled(b, 0, 1, k, slots, odd)
    half_sweep(black, fd_red, fd_black, 0, 1, slots, odd)
    half_sweep(red, black, fd_red, 0, 0, slots, odd)
    half_sweep(black, red, fd_black, 0, 1, slots, odd)
    for k in range(slots):
        r = residual(red, black, fd_red, 0, k, slots, odd)
        res[BX * k : BX * (k + 1), :] = r[8:24]
    matrix = 0.125 * halving(256, 128, lax.broadcasted_iota(jnp.int32, (256, 128), 1))
    thin[...] = matmul(res[...], matrix)
    v = thin[pl.ds(0, 8 * slots, stride=2), :] + thin[pl.ds(1, 8 * slots, stride=2), :]
    for k in range(slots):
        for d in range(sent.shape[0]):
            sent[d, k] = v[8 * k : 8 * k + 8]


def predictor_kernel(pred, fix_rows, fix_cols, done):
    lane = lanes(BX)
    row = rows_of(BX)
    edge = (lane == 0) | (lane == BY - 1)
    for j in range(3 * NZ):
        q, z = divmod(j, NZ)
        low = jnp.broadcast_to(fix_rows[j : j + 1, :], (BX, BY))
        high = jnp.broadcast_to(fix_rows[3 * NZ + j : 3 * NZ + j + 1, :], (BX, BY))
        rim = jnp.where(row == 0, low, jnp.where(row == BX - 1, high, 0.0))
        column = turn(fix_cols[q // 2], -(64 * (q % 2) + 2 * z + 1), 1)
        rim = rim + jnp.where(edge, column, 0.0)
        done[BX * j : BX * (j + 1), :] = pred[BX * j : BX * (j + 1), :] + rim


def middle_down_kernel(nx, index, gathered, fd_red, fd_black, black, coarse, red, res):
    ring = 8 * nx
    slots = 8
    odd8 = odd_cells(8, 128)
    odd = odd_cells(ring, 128)
    for j in range(nx):
        d = lax.rem(index[0] + j, nx)
        for k in range(slots):
            r, b = pack(gathered[d, 2 * k], gathered[d, 2 * k + 1], odd8)
            fd_red[k, 8 * j : 8 * j + 8, :] = scaled(r, 1, 0, k, slots, odd8)
            fd_black[k, 8 * j : 8 * j + 8, :] = scaled(b, 1, 1, k, slots, odd8)
    half_sweep(black, fd_red, fd_black, 1, 1, slots, odd)
    half_sweep(red, black, fd_red, 1, 0, slots, odd)
    half_sweep(black, red, fd_black, 1, 1, slots, odd)
    for k in range(slots):
        res[ring * k : ring * (k + 1), :] = residual(red, black, fd_red, 1, k, slots, odd)
    lane = lax.broadcasted_iota(jnp.int32, (128, 128), 1)
    column = jnp.where(lane < 32, lane, jnp.where(lane < 80, lane - 32, jnp.where(lane < 96, lane - 32, lane - 96)))
    res[...] = matmul(res[...], 0.125 * halving(128, 128, column))
    n = slots * ring // 2
    v = res[pl.ds(0, n, stride=2), :] + res[pl.ds(1, n, stride=2), :]
    for k in range(slots):
        coarse[k] = v[ring // 2 * k : ring // 2 * (k + 1)]


def up_kernel(
    nx, g_own, g_left, g_right, fd1_red, fd1_black, black1_in, fd0_red, fd0_black, black0_in, pred, obst,
    corrected, pressure, fd2_red, fd2_black, red2, black2, res2, fd3, red1, black1, big1, red0, black0, big0,
):
    x2 = 4 * nx
    lane = lanes(x2)
    odd2 = odd_cells(x2, 128)
    slots2 = 4

    def rhs2(z):
        return jnp.where(lane < 32, g_own[z], jnp.where(lane < 80, g_right[z], g_left[z]))

    for k in range(slots2):
        r, b = pack(rhs2(2 * k), rhs2(2 * k + 1), odd2)
        fd2_red[k] = scaled(r, 2, 0, k, slots2, odd2)
        fd2_black[k] = scaled(b, 2, 1, k, slots2, odd2)
    half_sweep(black2, fd2_red, fd2_black, 2, 1, slots2, odd2)
    half_sweep(red2, black2, fd2_red, 2, 0, slots2, odd2)
    half_sweep(black2, red2, fd2_black, 2, 1, slots2, odd2)
    for k in range(slots2):
        res2[x2 * k : x2 * (k + 1), :] = residual(red2, black2, fd2_red, 2, k, slots2, odd2)
    col = lax.broadcasted_iota(jnp.int32, (128, 128), 1)
    res2[...] = matmul(res2[...], 0.125 * halving(128, 128, col % 64))
    n = slots2 * x2 // 2
    x3 = x2 // 2
    fd3[...] = res2[pl.ds(0, n, stride=2), :] + res2[pl.ds(1, n, stride=2), :]

    odd3 = odd_cells(x3, 128)
    fr, fb = [], []
    for k in range(2):
        r, b = pack(fd3[x3 * 2 * k : x3 * (2 * k + 1), :], fd3[x3 * (2 * k + 1) : x3 * (2 * k + 2), :], odd3)
        fr.append(scaled(r, 3, 0, k, 2, odd3))
        fb.append(scaled(b, 3, 1, k, 2, odd3))
    r = fr
    for step in range(8):
        if step > 0:
            r = [relaxed(b, fr, 3, 0, k, 2, odd3) for k in range(2)]
        b = [relaxed(r, fb, 3, 1, k, 2, odd3) for k in range(2)]

    def layers(red, black, odd):
        return jnp.where(odd, black, red), jnp.where(odd, red, black)

    parts = []
    for k in range(2):
        parts += layers(r[k], b[k], odd3)
    e = matmul(jnp.concatenate(parts, axis=0), doubling(128, 128, col // 2))
    res2[pl.ds(0, n, stride=2), :] = e
    res2[pl.ds(1, n, stride=2), :] = e
    for k in range(slots2):
        black2[k] = black2[k] + res2[x2 * k : x2 * (k + 1), :]
    half_sweep(red2, black2, fd2_red, 2, 0, slots2, odd2)
    half_sweep(black2, red2, fd2_black, 2, 1, slots2, odd2)
    half_sweep(red2, black2, fd2_red, 2, 0, slots2, odd2)
    half_sweep(black2, red2, fd2_black, 2, 1, slots2, odd2)

    x1 = 8 * nx
    odd1 = odd_cells(x1, 128)
    slots1 = 8
    for k in range(slots2):
        low, high = layers(red2[k], black2[k], odd2)
        res2[x2 * k : x2 * (k + 1), :] = low
        fd3[0 : x2, :] = high
        big1[x1 * 2 * k : x1 * 2 * k + x2, :] = res2[x2 * k : x2 * (k + 1), :]
        big1[x1 * 2 * k + x2 : x1 * 2 * k + 2 * x2, :] = fd3[0 : x2, :]
    stacked = jnp.concatenate([big1[x1 * 2 * k : x1 * 2 * k + 2 * x2, :] for k in range(slots2)], axis=0)
    e = matmul(stacked, doubling(128, 128, jnp.where(col < 96, col // 2, col // 2 + 64)))
    m = 8 * x2
    big1[pl.ds(0, m, stride=2), :] = e
    big1[pl.ds(1, m, stride=2), :] = e
    for k in range(slots1):
        black1[k] = black1_in[k] + big1[x1 * k : x1 * (k + 1), :]
    half_sweep(red1, black1, fd1_red, 1, 0, slots1, odd1)
    half_sweep(black1, red1, fd1_black, 1, 1, slots1, odd1)
    half_sweep(red1, black1, fd1_red, 1, 0, slots1, odd1)
    half_sweep(black1, red1, fd1_black, 1, 1, slots1, odd1)

    slots0 = NZ // 2
    for k in range(slots1):
        low, high = layers(red1[k], black1[k], odd1)
        for i, v in enumerate((low, high)):
            at = 16 * (2 * k + i)
            big1[at : at + 16, :] = turn(v, 4, 0)[0:16]
    wide_col = lax.broadcasted_iota(jnp.int32, (128, 256), 1)
    e = matmul(big1[0 : 16 * slots0, :], doubling(128, 256, wide_col // 2))
    for t in range(2):
        part = e[:, 128 * t : 128 * t + 128]
        big0[t, pl.ds(0, 16 * slots0, stride=2), :] = part
        big0[t, pl.ds(1, 16 * slots0, stride=2), :] = part
    odd0 = odd_cells(32, 256)
    for k in range(slots0):
        add = jnp.concatenate([big0[t, 32 * k : 32 * (k + 1), :] for t in range(2)], axis=1)
        black0[k] = black0_in[k] + add
    half_sweep(red0, black0, fd0_red, 0, 0, slots0, odd0)
    half_sweep(black0, red0, fd0_black, 0, 1, slots0, odd0)
    half_sweep(red0, black0, fd0_red, 0, 0, slots0, odd0)
    half_sweep(black0, red0, fd0_black, 0, 1, slots0, odd0)
    for k in range(slots0):
        low, high = layers(red0[k], black0[k], odd0)
        red0[k] = low
        black0[k] = high

    def full(z):
        return (black0 if z % 2 else red0)[z // 2]

    for z in range(NZ):
        p = full(z)
        own = p[8:24, 0:128]
        pressure[BX * z : BX * (z + 1), :] = own
        zero = jnp.zeros_like(own)
        upper = full(z + 1)[8:24, 0:128] if z < NZ - 1 else zero
        lower = full(z - 1)[8:24, 0:128] if z > 0 else zero
        gx = turn(p, -1, 0)[8:24, 0:128] - turn(p, 1, 0)[8:24, 0:128]
        mid = p[8:24]
        gy = turn(mid, -1, 1)[:, 0:128] - turn(mid, 1, 1)[:, 0:128]
        fluid = (1 - obst[BX * z : BX * (z + 1), :]).astype(F32)
        for q, g in enumerate((gx, gy, upper - lower)):
            j = q * NZ + z
            v = pred[BX * j : BX * (j + 1), :]
            corrected[BX * j : BX * (j + 1), :] = fluid * (v - (0.5 * TIME_STEP) * g)


def both_ways(axis, to_low, to_high):
    n = lax.axis_size(axis)
    up = [(i, (i + 1) % n) for i in range(n)]
    down = [((i + 1) % n, i) for i in range(n)]
    return lax.ppermute(to_high, axis, up), lax.ppermute(to_low, axis, down)


def body(velocity, old_tendency, obstacle):
    nx = lax.axis_size("gx")
    index = lax.axis_index("gx").astype(jnp.int32).reshape(1)
    vel = velocity.reshape(3 * NZ * BX, BY)
    old = old_tendency.reshape(3 * NZ * BX, BY)
    obst = obstacle.reshape(NZ * BX, BY)

    pred, source, to_low, to_high = call(
        local_kernel,
        (vmem(3 * NZ * BX, BY), vmem(NZ * BX, BY), vmem(464, BY), vmem(464, BY)),
        (vel, old, obst),
        [(NZ * BX, BY)],
        name="local",
    )
    from_low, from_high = both_ways("gx", to_low, to_high)
    wide, to_left, to_right, fix_rows = call(
        join_x_kernel,
        (vmem(NZ * 32, BY), vmem(656, BY), vmem(656, BY), vmem(6 * NZ, BY)),
        (source, to_low, to_high, from_low, from_high),
        name="join_x",
    )
    from_left, from_right = both_ways("gy", to_left, to_right)
    fd0_red, fd0_black, black0, sent, fix_cols = call(
        fine_down_kernel,
        (vmem(16, 32, 256), vmem(16, 32, 256), vmem(16, 32, 256), vmem(nx, 16, 8, BY), vmem(2, BX, BY)),
        (wide, to_left, from_left, from_right),
        [(16, 32, 256), (256, 256), (256, 128)],
        name="fine_down",
    )
    pred = call(predictor_kernel, vmem(3 * NZ * BX, BY), (pred, fix_rows, fix_cols), name="predictor")
    gathered = lax.all_to_all(sent, "gx", 0, 0)
    x1 = 8 * nx
    fd1_red, fd1_black, black1, coarse = call(
        functools.partial(middle_down_kernel, nx),
        (vmem(8, x1, BY), vmem(8, x1, BY), vmem(8, x1, BY), vmem(8, x1 // 2, BY)),
        (index, gathered),
        [(8, x1, BY), (8 * x1, BY)],
        in_specs=[pl.BlockSpec(memory_space=pltpu.SMEM), pl.BlockSpec(memory_space=pltpu.VMEM)],
        name="middle_down",
    )
    g_left, g_right = both_ways("gy", coarse, coarse)
    x2 = x1 // 2
    corrected, pressure = call(
        functools.partial(up_kernel, nx),
        (vmem(3 * NZ * BX, BY), vmem(NZ * BX, BY)),
        (coarse, g_left, g_right, fd1_red, fd1_black, black1, fd0_red, fd0_black, black0, pred, obst),
        [(4, x2, BY)] * 4
        + [(4 * x2, BY), (2 * x2, BY)]
        + [(8, x1, BY)] * 2
        + [(max(8 * x1, 256), BY)]
        + [(16, 32, 256)] * 2
        + [(2, 512, BY)],
        name="up",
    )
    return corrected.reshape(3, NZ, BX, BY), pressure.reshape(NZ, BX, BY)


def solution(mesh):
    placed = (P(None, None, "gx", "gy"), P(None, None, "gx", "gy"), P(None, "gx", "gy"))
    return jax.shard_map(
        body,
        mesh=mesh,
        in_specs=placed,
        out_specs=(P(None, None, "gx", "gy"), P(None, "gx", "gy")),
        check_vma=False,
    )
```

```python
import functools

import jax
import jax.numpy as jnp
from jax import lax
from jax.experimental import pallas as pl
from jax.experimental.pallas import tpu as pltpu
from jax.sharding import PartitionSpec as P

TIME_STEP = 0.25
VISCOSITY = 0.1
WEIGHT_NEW = 15.0 / 16.0
WEIGHT_OLD = -25.0 / 48.0
HELMHOLTZ = 1.0e-4
SCALE = -0.5 / TIME_STEP
INTERPRET = False
F32 = jnp.float32
NZ = 32
BX = 16
BY = 128
WX = 40
CHUNKS = 4


def vmem(*shape):
    return jax.ShapeDtypeStruct(shape, F32)


def call(kernel, outs, args, scratch=(), in_specs=None, name=None):
    return pl.pallas_call(
        kernel,
        out_shape=outs,
        in_specs=in_specs or [pl.BlockSpec(memory_space=pltpu.VMEM)] * len(args),
        scratch_shapes=[pltpu.VMEM(s, F32) if isinstance(s, tuple) else s for s in scratch],
        compiler_params=pltpu.CompilerParams(vmem_limit_bytes=16 << 20),
        interpret=INTERPRET,
        name=name,
    )(*args)


def turn(a, shift, axis):
    return pltpu.roll(a, shift % a.shape[axis], axis)


def lanes(rows, cols=128):
    return lax.broadcasted_iota(jnp.int32, (rows, cols), 1)


def rows_of(rows, cols=128):
    return lax.broadcasted_iota(jnp.int32, (rows, cols), 0)


def odd_cells(rows, cols):
    return (rows_of(rows, cols) + lanes(rows, cols)) % 2 == 1


def diag(level, m):
    return HELMHOLTZ + (4.0 + m) / float(4**level)


def at_end(colour, k, count, odd, inner, end):
    if k == 0:
        return jnp.where(odd, inner, end) if colour == 0 else jnp.where(odd, end, inner)
    if k == count - 1:
        return jnp.where(odd, end, inner) if colour == 0 else jnp.where(odd, inner, end)
    return inner


def pack(low, high, odd):
    return jnp.where(odd, high, low), jnp.where(odd, low, high)


def scaled(value, level, colour, k, count, odd):
    return value * at_end(colour, k, count, odd, 1.0 / diag(level, 2), 1.0 / diag(level, 1))


def neighbours(src, colour, k, count, odd):
    b = src[k]
    zero = jnp.zeros_like(b)
    above = src[k + 1] if k < count - 1 else zero
    below = src[k - 1] if k > 0 else zero
    z = jnp.where(odd, above, below) if colour == 0 else jnp.where(odd, below, above)
    return turn(b, 1, 0) + turn(b, -1, 0) + turn(b, 1, 1) + turn(b, -1, 1) + (b + z)


def relaxed(src, fd, level, colour, k, count, odd):
    s = float(4**level)
    c = at_end(colour, k, count, odd, 1.0 / s / diag(level, 2), 1.0 / s / diag(level, 1))
    return fd[k] + c * neighbours(src, colour, k, count, odd)


def half_sweep(dst, src, fd, level, colour, count, odd):
    for k in range(count):
        dst[k] = relaxed(src, fd, level, colour, k, count, odd)


def residual(red, black, fd, level, k, count, odd):
    d = at_end(0, k, count, odd, diag(level, 2), diag(level, 1))
    return d * (relaxed(black, fd, level, 0, k, count, odd) - red[k])


def halving(n, m, target):
    i = lax.broadcasted_iota(jnp.int32, (n, m), 0)
    return (i // 2 == target).astype(F32)


def doubling(n, m, target):
    i = lax.broadcasted_iota(jnp.int32, (n, m), 0)
    return (i == target).astype(F32)


def matmul(a, b):
    return jnp.dot(a, b, precision=lax.Precision.HIGHEST, preferred_element_type=F32)


def local_kernel(vel_hbm, old_hbm, obst_hbm, pred, source, to_low, to_high, vel, old, obst, edge_x, sems):
    lane = lanes(BX)
    row = rows_of(BX)
    depth = NZ // CHUNKS
    copies = []
    for c in range(CHUNKS):
        group = []
        for i, (src, dst, q) in enumerate(
            [(vel_hbm, vel, q) for q in range(3)] + [(old_hbm, old, q) for q in range(3)] + [(obst_hbm, obst, 0)]
        ):
            at = pl.ds((q * NZ + c * depth) * BX, depth * BX)
            group.append(pltpu.make_async_copy(src.at[at, :], dst.at[at, :], sems.at[c, i]))
        copies.append(group)
    for c in range(CHUNKS):
        for copy in copies[c]:
            copy.start()

    def cut(ref, j):
        return ref[BX * j : BX * (j + 1), :]

    packs = [jnp.zeros((BX, BY), F32) for _ in range(3)]

    def put(pack, value, at):
        return jnp.where((lane == at) | (lane == at + 1), turn(value, at + 1, 1), pack)

    for copy in copies[0]:
        copy.wait()
    for z in range(NZ):
        if z % depth == depth - 1 and z < NZ - 1:
            for copy in copies[z // depth + 1]:
                copy.wait()
        fluid = (1 - cut(obst, z)).astype(F32)
        now = [cut(vel, q * NZ + z) for q in range(3)]
        for q in range(3):
            j = q * NZ + z
            v = now[q]
            minus_x = jnp.where(row == 0, 0.0, turn(v, 1, 0))
            plus_x = jnp.where(row == BX - 1, 0.0, turn(v, -1, 0))
            minus_y = jnp.where(lane == 0, 0.0, turn(v, 1, 1))
            plus_y = jnp.where(lane == BY - 1, 0.0, turn(v, -1, 1))
            zero = jnp.zeros_like(v)
            upper = cut(vel, j + 1) if z < NZ - 1 else zero
            lower = cut(vel, j - 1) if z > 0 else zero
            advect = (now[0] * (plus_x - minus_x) + now[1] * (plus_y - minus_y) + now[2] * (upper - lower)) * 0.5
            diffuse = plus_x + minus_x + plus_y + minus_y + upper + lower - 6.0 * v
            tendency = VISCOSITY * diffuse - advect
            p = fluid * (v + TIME_STEP * (WEIGHT_NEW * tendency + WEIGHT_OLD * cut(old, j)))
            pred[BX * j : BX * (j + 1), :] = p
            if q == 1:
                pv = p
        weight = (TIME_STEP * WEIGHT_NEW) * fluid
        across_x = weight * (VISCOSITY + jnp.where(row == 0, 0.5, -0.5) * now[0])
        across_x = jnp.where((row == 0) | (row == BX - 1), across_x, 0.0)
        across_y = weight * (VISCOSITY + jnp.where(lane == 0, 0.5, -0.5) * now[1])
        edge_x[BX * z : BX * (z + 1), :] = across_x
        for t, pair in enumerate(((now[0], now[1]), (now[2], across_y), (pv, across_x))):
            for i in range(2):
                packs[t] = put(packs[t], pair[i], 64 * i + 2 * z)
    for z in range(NZ):
        u = cut(pred, z)
        v = cut(pred, NZ + z)
        zero = jnp.zeros_like(u)
        upper = cut(pred, 2 * NZ + z + 1) if z < NZ - 1 else zero
        lower = cut(pred, 2 * NZ + z - 1) if z > 0 else zero
        east = jnp.where(row == BX - 1, 0.0, turn(u, -1, 0))
        west = jnp.where(row == 0, 0.0, turn(u, 1, 0))
        north = jnp.where(lane == BY - 1, 0.0, turn(v, -1, 1))
        south = jnp.where(lane == 0, 0.0, turn(v, 1, 1))
        s = SCALE * ((east - west) + (north - south) + (upper - lower))
        source[BX * z : BX * (z + 1), :] = s
        to_low[8 * z : 8 * z + 8, :] = s[:8]
        to_high[8 * z : 8 * z + 8, :] = s[8:]
    half = NZ // 2
    sub = rows_of(8)
    for h in range(half):
        at = 8 * (NZ + h)
        a = source[BX * h : BX * (h + 1), :]
        b = source[BX * (h + half) : BX * (h + half + 1), :]
        to_low[at : at + 8, :] = jnp.where(sub < 4, a[8:], turn(b[8:], 4, 0))
        to_high[at : at + 8, :] = jnp.where(sub < 4, turn(b[:8], 4, 0), a[:8])
    for ref, r in ((to_low, 0), (to_high, BX - 1)):
        at = 12 * NZ
        ref[at : at + NZ, :] = edge_x[pl.ds(r, NZ, stride=BX), :]
        ref[at + NZ : at + 4 * NZ, :] = vel[pl.ds(r, 3 * NZ, stride=BX), :]
        ref[at + 4 * NZ : at + 5 * NZ, :] = pred[pl.ds(r, NZ, stride=BX), :]
        for t in range(3):
            ref[at + 5 * NZ + BX * t : at + 5 * NZ + BX * (t + 1), :] = packs[t]


def join_x_kernel(source, to_low, to_high, from_low, from_high, wide, to_left, to_right, fix_rows):
    lane = lanes(NZ)
    layer = rows_of(NZ)
    sub = rows_of(8)
    half = NZ // 2

    def line(ref, i):
        at = 12 * NZ + NZ * i
        return ref[at : at + NZ, :]

    def slope_y(f):
        return jnp.where(lane == BY - 1, 0.0, turn(f, -1, 1)) - jnp.where(lane == 0, 0.0, turn(f, 1, 1))

    def slope_z(f):
        return jnp.where(layer == NZ - 1, 0.0, turn(f, -1, 0)) - jnp.where(layer == 0, 0.0, turn(f, 1, 0))

    for z in range(NZ):
        w = WX * z
        wide[w : w + 16, :] = source[BX * z : BX * (z + 1), :]
        wide[w + 16 : w + 24, :] = from_high[8 * z : 8 * z + 8, :]
        at = 8 * (NZ + z % half)
        high = from_high[at : at + 8, :]
        low = from_low[at : at + 8, :]
        if z < half:
            wide[w + 24 : w + 32, :] = jnp.where(sub < 4, high, low)
        else:
            wide[w + 24 : w + 32, :] = turn(jnp.where(sub < 4, low, high), 4, 0)
        wide[w + 32 : w + 40, :] = from_low[8 * z : 8 * z + 8, :]

    def add(row, value):
        at = pl.ds(row % WX, NZ, stride=WX)
        wide[at, :] = wide[at, :] + SCALE * value

    for near, far, row, step, sign in ((to_low, from_low, 0, -1, 1.0), (to_high, from_high, 15, 1, -1.0)):
        inner = [line(near, 0) * line(far, 1 + q) for q in range(3)]
        outer = [line(far, 0) * line(near, 1 + q) for q in range(3)]
        add(row - step, -sign * inner[0])
        add(row, -sign * (line(far, 4) + outer[0]) + slope_y(inner[1]) + slope_z(inner[2]))
        add(row + step, sign * (line(near, 4) + inner[0]) + slope_y(outer[1]) + slope_z(outer[2]))
        add(row + 2 * step, sign * outer[0])
        for q in range(3):
            at = NZ * (3 * (step > 0) + q)
            fix_rows[at : at + NZ, :] = inner[q]

    stack = []
    for t in range(3):
        at = 17 * NZ + BX * t
        stack.append(jnp.concatenate([ref[at : at + BX, :] for ref in (to_low, from_high, from_low)], axis=0))
    first = rows_of(48) % BX == 0
    other = jnp.where(first, turn(stack[0], 1, 0), turn(stack[0], -1, 0))
    stack[2] = stack[2] + turn(stack[2] * other, 64, 1)
    lane = lanes(WX)
    for h in range(half):
        a = wide[WX * h : WX * (h + 1), :]
        b = turn(wide[WX * (h + half) : WX * (h + half + 1), :], 64, 1)
        to_left[WX * h : WX * (h + 1), :] = jnp.where(lane < 64, a, b)
        to_right[WX * h : WX * (h + 1), :] = jnp.where(lane < 64, b, a)
    for t in range(3):
        at = WX * half + 48 * t
        to_left[at : at + 48, :] = stack[t]
        to_right[at : at + 48, :] = stack[t]


def trimmed(a):
    return jnp.concatenate([a[0:24], a[32:40]], axis=0)


def fine_down_kernel(
    wide, sent_left, from_left, from_right,
    fd0_red, fd0_black, black0, sent, own1, up1, down1, fix_cols,
    fd_red, fd_black, red, black, res, thin, fd1_red, fd1_black, red1, black1, res1,
):
    lane = lanes(WX)
    odd = odd_cells(WX, 256)
    half = NZ // 2
    slots = NZ // 2

    lane48 = lanes(48)
    even = lane48 % 2 == 0
    low_half = lane48 < 64

    def pack_of(ref, t):
        at = WX * half + 48 * t
        return ref[at : at + 48, :]

    def swap(f):
        return turn(f, 64, 1)

    def both(f):
        return jnp.where(low_half, swap(f), f)

    def facing(left, right):
        return jnp.where(even, turn(right, -1, 1), turn(left, 1, 1))

    def slope_x(f):
        return turn(f, -1, 0) - turn(f, 1, 0)

    def slope_z(f):
        above = jnp.where(lane48 >= 2 * NZ - 2, 0.0, turn(f, -2, 1))
        below = jnp.where(lane48 < 2, 0.0, turn(f, 2, 1))
        return above - below

    def signed(f):
        return jnp.where(even, f, -f)

    own = [pack_of(sent_left, t) for t in range(3)]
    left = [pack_of(from_left, t) for t in range(3)]
    right = [pack_of(from_right, t) for t in range(3)]
    near = both(own[1])
    inner_uv = near * facing(left[0], right[0])
    inner_w = near * facing(left[1], right[1])
    far = both(jnp.where(even, left[1], right[1]))
    outer_uv = far * facing(own[0], own[0])
    outer_w = far * facing(own[1], own[1])
    inner_v = swap(inner_uv)
    outer_v = swap(outer_uv)
    pv_far = jnp.where(even, left[2], right[2]) + outer_v
    pv_own = own[2] + inner_v
    e0 = signed(facing(pv_far, pv_far)) + slope_x(inner_uv) + slope_z(inner_w)
    e1 = signed(facing(pv_own, pv_own)) + slope_x(outer_uv) + slope_z(outer_w)
    i = lax.broadcasted_iota(jnp.int32, (128, 128), 0)
    j = lax.broadcasted_iota(jnp.int32, (128, 128), 1)
    side = i % 2
    to = 4 * ((i % 64) // 2) + jnp.where(i < 64, 1 + side, 3 * side)
    order = SCALE * (to == j).astype(F32)
    mixed = []
    for e, v in ((e0, inner_v), (e1, outer_v)):
        m = jnp.where(low_half, e, swap(signed(v)))
        m = jnp.concatenate([m[0:24], jnp.where(rows_of(8) < 4, m[24:32], m[32:40]), m[40:48]], axis=0)
        mixed.append(matmul(m, order))
    fix_cols[0] = inner_uv[0:16]
    fix_cols[1] = inner_w[0:16]
    edge = (lane < 2) | (lane >= BY - 2)

    def layer(z):
        t0 = wide[WX * z : WX * (z + 1), :]
        h = z % half
        a = from_right[WX * h : WX * (h + 1), :]
        b = from_left[WX * h : WX * (h + 1), :]
        if z < half:
            t1 = jnp.where(lane < 64, a, b)
        else:
            t1 = turn(jnp.where(lane < 64, b, a), 64, 1)
        t0 = t0 + jnp.where(edge, turn(mixed[0], 126 - 4 * z, 1), 0.0)
        t1 = t1 + jnp.where(edge, turn(mixed[1], 126 - 4 * z, 1), 0.0)
        return jnp.concatenate([t0, t1], axis=1)

    for k in range(slots):
        r, b = pack(layer(2 * k), layer(2 * k + 1), odd)
        r = scaled(r, 0, 0, k, slots, odd)
        b = scaled(b, 0, 1, k, slots, odd)
        fd_red[k] = r
        fd_black[k] = b
        fd0_red[k] = trimmed(r)
        fd0_black[k] = trimmed(b)
    half_sweep(black, fd_red, fd_black, 0, 1, slots, odd)
    half_sweep(red, black, fd_red, 0, 0, slots, odd)
    half_sweep(black, red, fd_black, 0, 1, slots, odd)
    for k in range(slots):
        black0[k] = trimmed(black[k])
        res[32 * k : 32 * (k + 1), :] = trimmed(residual(red, black, fd_red, 0, k, slots, odd))
    matrix = 0.125 * halving(256, 128, lax.broadcasted_iota(jnp.int32, (256, 128), 1))
    thin[...] = matmul(res[...], matrix)
    n = BX * slots
    own1[...] = thin[pl.ds(0, n, stride=2), :] + thin[pl.ds(1, n, stride=2), :]

    odd1 = odd_cells(16, 128)
    slots1 = slots // 2
    sub = rows_of(8)

    def plane(z):
        return own1[16 * z : 16 * (z + 1), :]

    for z in range(slots):
        a, b = plane(z)[:8], plane(z)[8:]
        up1[8 * z : 8 * z + 8, :] = jnp.where(sub < 4, a, b)
        down1[8 * z : 8 * z + 8, :] = jnp.where(sub < 4, b, a)
    for k in range(slots1):
        r, b = pack(plane(2 * k), plane(2 * k + 1), odd1)
        fd1_red[k] = scaled(r, 1, 0, k, slots1, odd1)
        fd1_black[k] = scaled(b, 1, 1, k, slots1, odd1)
    half_sweep(black1, fd1_red, fd1_black, 1, 1, slots1, odd1)
    half_sweep(red1, black1, fd1_red, 1, 0, slots1, odd1)
    half_sweep(black1, red1, fd1_black, 1, 1, slots1, odd1)
    for k in range(slots1):
        res1[8 * k : 8 * k + 8, :] = residual(red1, black1, fd1_red, 1, k, slots1, odd1)[:8]
    res1[...] = matmul(res1[...], 0.125 * halving(128, 128, j % 64))
    v = res1[pl.ds(0, 32, stride=2), :] + res1[pl.ds(1, 32, stride=2), :]
    v = jnp.where(lanes(16) < 64, v[:16], v[16:])
    for d in range(sent.shape[0]):
        sent[d] = v


def predictor_kernel(pred, fix_rows, fix_cols, done):
    lane = lanes(BX)
    row = rows_of(BX)
    edge = (lane == 0) | (lane == BY - 1)
    for j in range(3 * NZ):
        q, z = divmod(j, NZ)
        low = jnp.broadcast_to(fix_rows[j : j + 1, :], (BX, BY))
        high = jnp.broadcast_to(fix_rows[3 * NZ + j : 3 * NZ + j + 1, :], (BX, BY))
        rim = jnp.where(row == 0, low, jnp.where(row == BX - 1, high, 0.0))
        column = turn(fix_cols[q // 2], -(64 * (q % 2) + 2 * z + 1), 1)
        rim = rim + jnp.where(edge, column, 0.0)
        done[BX * j : BX * (j + 1), :] = pred[BX * j : BX * (j + 1), :] + rim


def middle_kernel(own1, from_low, from_high, fd_red, fd_black, black, red):
    slots = 8
    odd = odd_cells(32, 128)
    sub = rows_of(8)

    def plane(z):
        a = own1[16 * z : 16 * z + 8, :]
        b = own1[16 * z + 8 : 16 * z + 16, :]
        low = from_low[8 * z : 8 * z + 8, :]
        high = from_high[8 * z : 8 * z + 8, :]
        tiles = [a] + [jnp.where(sub < 4, p, q) for p, q in ((b, high), (high, low), (low, b))]
        return jnp.concatenate(tiles, axis=0)

    for k in range(slots):
        r, b = pack(plane(2 * k), plane(2 * k + 1), odd)
        fd_red[k] = scaled(r, 1, 0, k, slots, odd)
        fd_black[k] = scaled(b, 1, 1, k, slots, odd)
    half_sweep(black, fd_red, fd_black, 1, 1, slots, odd)
    half_sweep(red, black, fd_red, 1, 0, slots, odd)
    half_sweep(black, red, fd_black, 1, 1, slots, odd)


def up_kernel(
    nx, index, g_own, g_left, g_right, fd1_red, fd1_black, black1_in, fd0_red, fd0_black, black0_in, pred, obst,
    corrected, pressure, fd2_red, fd2_black, red2, black2, res2, fd3, red1, black1, big1, red0, black0, big0, ring,
):
    x2 = 4 * nx
    lane = lanes(x2)
    odd2 = odd_cells(x2, 128)
    slots2 = 4

    for i, g in enumerate((g_own, g_right, g_left)):
        for j in range(nx):
            d = lax.rem(index[0] + j, nx)
            for z in range(4):
                ring[4 * i + z, 4 * j : 4 * j + 4, :] = g[d, 4 * z : 4 * z + 4, :]

    def rhs2(z):
        lift = 64 * (z // 4)
        own, right, left = (ring[4 * i + z % 4] for i in range(3))
        own = turn(own, -lift, 1) if lift else own
        right = turn(right, 32 - lift, 1)
        left = jnp.where(lane < 96, turn(left, 32 - lift, 1), turn(left, 96 - lift, 1))
        return jnp.where(lane < 32, own, jnp.where(lane < 80, right, left))

    for k in range(slots2):
        r, b = pack(rhs2(2 * k), rhs2(2 * k + 1), odd2)
        fd2_red[k] = scaled(r, 2, 0, k, slots2, odd2)
        fd2_black[k] = scaled(b, 2, 1, k, slots2, odd2)
    half_sweep(black2, fd2_red, fd2_black, 2, 1, slots2, odd2)
    half_sweep(red2, black2, fd2_red, 2, 0, slots2, odd2)
    half_sweep(black2, red2, fd2_black, 2, 1, slots2, odd2)
    for k in range(slots2):
        res2[x2 * k : x2 * (k + 1), :] = residual(red2, black2, fd2_red, 2, k, slots2, odd2)
    col = lax.broadcasted_iota(jnp.int32, (128, 128), 1)
    res2[...] = matmul(res2[...], 0.125 * halving(128, 128, col % 64))
    n = slots2 * x2 // 2
    x3 = x2 // 2
    fd3[...] = res2[pl.ds(0, n, stride=2), :] + res2[pl.ds(1, n, stride=2), :]

    odd3 = odd_cells(x3, 128)
    fr, fb = [], []
    for k in range(2):
        r, b = pack(fd3[x3 * 2 * k : x3 * (2 * k + 1), :], fd3[x3 * (2 * k + 1) : x3 * (2 * k + 2), :], odd3)
        fr.append(scaled(r, 3, 0, k, 2, odd3))
        fb.append(scaled(b, 3, 1, k, 2, odd3))
    r = fr
    for step in range(8):
        if step > 0:
            r = [relaxed(b, fr, 3, 0, k, 2, odd3) for k in range(2)]
        b = [relaxed(r, fb, 3, 1, k, 2, odd3) for k in range(2)]

    def layers(red, black, odd):
        return jnp.where(odd, black, red), jnp.where(odd, red, black)

    parts = []
    for k in range(2):
        parts += layers(r[k], b[k], odd3)
    e = matmul(jnp.concatenate(parts, axis=0), doubling(128, 128, col // 2))
    res2[pl.ds(0, n, stride=2), :] = e
    res2[pl.ds(1, n, stride=2), :] = e
    for k in range(slots2):
        black2[k] = black2[k] + res2[x2 * k : x2 * (k + 1), :]
    half_sweep(red2, black2, fd2_red, 2, 0, slots2, odd2)
    half_sweep(black2, red2, fd2_black, 2, 1, slots2, odd2)
    half_sweep(red2, black2, fd2_red, 2, 0, slots2, odd2)
    half_sweep(black2, red2, fd2_black, 2, 1, slots2, odd2)

    odd1 = odd_cells(32, 128)
    slots1 = 8
    sub = rows_of(8)
    for k in range(slots2):
        for i, v in enumerate(layers(red2[k], black2[k], odd2)):
            at = 16 * (2 * k + i)
            big1[at : at + 8, :] = v[0:8]
            big1[at + 8 : at + 16, :] = jnp.where(sub < 2, v[8:16] if nx > 2 else v[0:8], v[x2 - 8 : x2])
    e = matmul(big1[0 : 16 * slots1, :], doubling(128, 128, jnp.where(col < 96, col // 2, col // 2 + 64)))
    big1[pl.ds(0, 16 * slots1, stride=2), :] = e
    big1[pl.ds(1, 16 * slots1, stride=2), :] = e
    for k in range(slots1):
        black1[k] = black1_in[k] + big1[32 * k : 32 * (k + 1), :]
    half_sweep(red1, black1, fd1_red, 1, 0, slots1, odd1)
    half_sweep(black1, red1, fd1_black, 1, 1, slots1, odd1)
    half_sweep(red1, black1, fd1_red, 1, 0, slots1, odd1)
    half_sweep(black1, red1, fd1_black, 1, 1, slots1, odd1)

    slots0 = NZ // 2
    for k in range(slots1):
        low, high = layers(red1[k], black1[k], odd1)
        for i, v in enumerate((low, high)):
            at = 16 * (2 * k + i)
            big1[at : at + 8, :] = v[0:8]
            big1[at + 8 : at + 16, :] = jnp.where(sub < 4, v[8:16], v[24:32])
    wide_col = lax.broadcasted_iota(jnp.int32, (128, 256), 1)
    e = matmul(big1[0 : 16 * slots0, :], doubling(128, 256, wide_col // 2))
    for t in range(2):
        part = e[:, 128 * t : 128 * t + 128]
        big0[t, pl.ds(0, 16 * slots0, stride=2), :] = part
        big0[t, pl.ds(1, 16 * slots0, stride=2), :] = part
    odd0 = odd_cells(32, 256)
    for k in range(slots0):
        add = jnp.concatenate([big0[t, 32 * k : 32 * (k + 1), :] for t in range(2)], axis=1)
        black0[k] = black0_in[k] + add
    half_sweep(red0, black0, fd0_red, 0, 0, slots0, odd0)
    half_sweep(black0, red0, fd0_black, 0, 1, slots0, odd0)
    half_sweep(red0, black0, fd0_red, 0, 0, slots0, odd0)
    half_sweep(black0, red0, fd0_black, 0, 1, slots0, odd0)
    for k in range(slots0):
        low, high = layers(red0[k], black0[k], odd0)
        red0[k] = low
        black0[k] = high

    def full(z):
        return (black0 if z % 2 else red0)[z // 2]

    for z in range(NZ):
        p = full(z)
        own = p[0:16, 0:128]
        pressure[BX * z : BX * (z + 1), :] = own
        zero = jnp.zeros_like(own)
        upper = full(z + 1)[0:16, 0:128] if z < NZ - 1 else zero
        lower = full(z - 1)[0:16, 0:128] if z > 0 else zero
        gx = turn(p, -1, 0)[0:16, 0:128] - turn(p, 1, 0)[0:16, 0:128]
        mid = p[0:16]
        gy = turn(mid, -1, 1)[:, 0:128] - turn(mid, 1, 1)[:, 0:128]
        fluid = (1 - obst[BX * z : BX * (z + 1), :]).astype(F32)
        for q, g in enumerate((gx, gy, upper - lower)):
            j = q * NZ + z
            v = pred[BX * j : BX * (j + 1), :]
            corrected[BX * j : BX * (j + 1), :] = fluid * (v - (0.5 * TIME_STEP) * g)


def both_ways(axis, to_low, to_high):
    n = lax.axis_size(axis)
    up = [(i, (i + 1) % n) for i in range(n)]
    down = [((i + 1) % n, i) for i in range(n)]
    return lax.ppermute(to_high, axis, up), lax.ppermute(to_low, axis, down)


def body(velocity, old_tendency, obstacle):
    nx = lax.axis_size("gx")
    index = lax.axis_index("gx").astype(jnp.int32).reshape(1)
    vel = velocity.reshape(3 * NZ * BX, BY)
    old = old_tendency.reshape(3 * NZ * BX, BY)
    obst = obstacle.reshape(NZ * BX, BY)

    block = 3 * NZ * BX
    anywhere = [pl.BlockSpec(memory_space=pltpu.HBM)] * 3
    pred, source, to_low, to_high = call(
        local_kernel,
        (vmem(block, BY), vmem(NZ * BX, BY), vmem(592, BY), vmem(592, BY)),
        tuple(pltpu.with_memory_space_constraint(a, pltpu.HBM) for a in (vel, old, obst)),
        [
            pltpu.VMEM((block, BY), F32),
            pltpu.VMEM((block, BY), F32),
            pltpu.VMEM((NZ * BX, BY), jnp.int32),
            pltpu.VMEM((NZ * BX, BY), F32),
            pltpu.SemaphoreType.DMA((CHUNKS, 7)),
        ],
        in_specs=anywhere,
        name="local",
    )
    from_low, from_high = both_ways("gx", to_low, to_high)
    wide, to_left, to_right, fix_rows = call(
        join_x_kernel,
        (vmem(NZ * WX, BY), vmem(784, BY), vmem(784, BY), vmem(6 * NZ, BY)),
        (source, to_low, to_high, from_low, from_high),
        name="join_x",
    )
    from_left, from_right = both_ways("gy", to_left, to_right)
    fd0_red, fd0_black, black0, sent, own1, up1, down1, fix_cols = call(
        fine_down_kernel,
        (
            vmem(16, 32, 256),
            vmem(16, 32, 256),
            vmem(16, 32, 256),
            vmem(nx, 16, BY),
            vmem(256, BY),
            vmem(128, BY),
            vmem(128, BY),
            vmem(2, BX, BY),
        ),
        (wide, to_left, from_left, from_right),
        [(16, WX, 256)] * 4 + [(512, 256), (512, BY)] + [(8, 16, BY)] * 4 + [(64, BY)],
        name="fine_down",
    )
    gathered = lax.all_to_all(sent, "gx", 0, 0)
    low1, high1 = both_ways("gx", down1, up1)
    fd1_red, fd1_black, black1 = call(
        middle_kernel, (vmem(8, 32, BY),) * 3, (own1, low1, high1), [(8, 32, BY)], name="middle"
    )
    pred = call(predictor_kernel, vmem(block, BY), (pred, fix_rows, fix_cols), name="predictor")
    g_left, g_right = both_ways("gy", gathered, gathered)
    x2 = 4 * nx
    corrected, pressure = call(
        functools.partial(up_kernel, nx),
        (vmem(block, BY), vmem(NZ * BX, BY)),
        (index, gathered, g_left, g_right, fd1_red, fd1_black, black1, fd0_red, fd0_black, black0, pred, obst),
        [(4, x2, BY)] * 4
        + [(4 * x2, BY), (2 * x2, BY)]
        + [(8, 32, BY)] * 2
        + [(256, BY)]
        + [(16, 32, 256)] * 2
        + [(2, 512, BY), (12, x2, BY)],
        in_specs=[pl.BlockSpec(memory_space=pltpu.SMEM)] + [pl.BlockSpec(memory_space=pltpu.VMEM)] * 11,
        name="up",
    )
    return corrected.reshape(3, NZ, BX, BY), pressure.reshape(NZ, BX, BY)


def solution(mesh):
    placed = (P(None, None, "gx", "gy"), P(None, None, "gx", "gy"), P(None, "gx", "gy"))
    return jax.shard_map(
        body,
        mesh=mesh,
        in_specs=placed,
        out_specs=(P(None, None, "gx", "gy"), P(None, "gx", "gy")),
        check_vma=False,
    )
```

```python
import functools

import jax
import jax.numpy as jnp
from jax import lax
from jax.experimental import pallas as pl
from jax.experimental.pallas import tpu as pltpu
from jax.sharding import PartitionSpec as P

TIME_STEP = 0.25
VISCOSITY = 0.1
WEIGHT_NEW = 15.0 / 16.0
WEIGHT_OLD = -25.0 / 48.0
HELMHOLTZ = 1.0e-4
SCALE = -0.5 / TIME_STEP
INTERPRET = False
F32 = jnp.float32
NZ = 32
BX = 16
BY = 128
WX = 40
CHUNKS = 8


def vmem(*shape):
    return jax.ShapeDtypeStruct(shape, F32)


def call(kernel, outs, args, scratch=(), in_specs=None, out_specs=None, name=None):
    everywhere = pl.BlockSpec(memory_space=pltpu.VMEM)
    return pl.pallas_call(
        kernel,
        out_shape=outs,
        out_specs=out_specs or jax.tree.map(lambda _: everywhere, outs),
        in_specs=in_specs or [everywhere] * len(args),
        scratch_shapes=[pltpu.VMEM(s, F32) if isinstance(s, tuple) else s for s in scratch],
        compiler_params=pltpu.CompilerParams(vmem_limit_bytes=16 << 20),
        interpret=INTERPRET,
        name=name,
    )(*args)


def turn(a, shift, axis):
    return pltpu.roll(a, shift % a.shape[axis], axis)


def lanes(rows, cols=128):
    return lax.broadcasted_iota(jnp.int32, (rows, cols), 1)


def rows_of(rows, cols=128):
    return lax.broadcasted_iota(jnp.int32, (rows, cols), 0)


def odd_cells(rows, cols):
    return (rows_of(rows, cols) + lanes(rows, cols)) % 2 == 1


def diag(level, m):
    return HELMHOLTZ + (4.0 + m) / float(4**level)


def at_end(colour, k, count, odd, inner, end):
    if k == 0:
        return jnp.where(odd, inner, end) if colour == 0 else jnp.where(odd, end, inner)
    if k == count - 1:
        return jnp.where(odd, end, inner) if colour == 0 else jnp.where(odd, inner, end)
    return inner


def pack(low, high, odd):
    return jnp.where(odd, high, low), jnp.where(odd, low, high)


def scaled(value, level, colour, k, count, odd):
    return value * at_end(colour, k, count, odd, 1.0 / diag(level, 2), 1.0 / diag(level, 1))


def neighbours(src, colour, k, count, odd):
    b = src[k]
    zero = jnp.zeros_like(b)
    above = src[k + 1] if k < count - 1 else zero
    below = src[k - 1] if k > 0 else zero
    z = jnp.where(odd, above, below) if colour == 0 else jnp.where(odd, below, above)
    return turn(b, 1, 0) + turn(b, -1, 0) + turn(b, 1, 1) + turn(b, -1, 1) + (b + z)


def relaxed(src, fd, level, colour, k, count, odd):
    s = float(4**level)
    c = at_end(colour, k, count, odd, 1.0 / s / diag(level, 2), 1.0 / s / diag(level, 1))
    return fd[k] + c * neighbours(src, colour, k, count, odd)


def half_sweep(dst, src, fd, level, colour, count, odd):
    for k in range(count):
        dst[k] = relaxed(src, fd, level, colour, k, count, odd)


def residual(red, black, fd, level, k, count, odd):
    d = at_end(0, k, count, odd, diag(level, 2), diag(level, 1))
    return d * (relaxed(black, fd, level, 0, k, count, odd) - red[k])


def halving(n, m, target):
    i = lax.broadcasted_iota(jnp.int32, (n, m), 0)
    return (i // 2 == target).astype(F32)


def doubling(n, m, target):
    i = lax.broadcasted_iota(jnp.int32, (n, m), 0)
    return (i == target).astype(F32)


def matmul(a, b):
    return jnp.dot(a, b, precision=lax.Precision.HIGHEST, preferred_element_type=F32)


def local_kernel(vel_hbm, old_hbm, obst_hbm, pred, source, to_low, to_high, vel, old, obst, edge_x, sems):
    lane = lanes(BX)
    row = rows_of(BX)
    depth = NZ // CHUNKS
    copies = []
    for c in range(CHUNKS):
        group = []
        for i, (src, dst, q) in enumerate(
            [(vel_hbm, vel, q) for q in range(3)] + [(old_hbm, old, q) for q in range(3)] + [(obst_hbm, obst, 0)]
        ):
            at = pl.ds((q * NZ + c * depth) * BX, depth * BX)
            group.append(pltpu.make_async_copy(src.at[at, :], dst.at[at, :], sems.at[c, i]))
        copies.append(group)
    for c in range(CHUNKS):
        for copy in copies[c]:
            copy.start()

    def cut(ref, j):
        return ref[BX * j : BX * (j + 1), :]

    packs = [jnp.zeros((BX, BY), F32) for _ in range(3)]

    def put(pack, value, at):
        return jnp.where((lane == at) | (lane == at + 1), turn(value, at + 1, 1), pack)

    for copy in copies[0]:
        copy.wait()
    for z in range(NZ):
        if z % depth == depth - 1 and z < NZ - 1:
            for copy in copies[z // depth + 1]:
                copy.wait()
        fluid = (1 - cut(obst, z)).astype(F32)
        now = [cut(vel, q * NZ + z) for q in range(3)]
        for q in range(3):
            j = q * NZ + z
            v = now[q]
            minus_x = jnp.where(row == 0, 0.0, turn(v, 1, 0))
            plus_x = jnp.where(row == BX - 1, 0.0, turn(v, -1, 0))
            minus_y = jnp.where(lane == 0, 0.0, turn(v, 1, 1))
            plus_y = jnp.where(lane == BY - 1, 0.0, turn(v, -1, 1))
            zero = jnp.zeros_like(v)
            upper = cut(vel, j + 1) if z < NZ - 1 else zero
            lower = cut(vel, j - 1) if z > 0 else zero
            advect = (now[0] * (plus_x - minus_x) + now[1] * (plus_y - minus_y) + now[2] * (upper - lower)) * 0.5
            diffuse = plus_x + minus_x + plus_y + minus_y + upper + lower - 6.0 * v
            tendency = VISCOSITY * diffuse - advect
            p = fluid * (v + TIME_STEP * (WEIGHT_NEW * tendency + WEIGHT_OLD * cut(old, j)))
            pred[BX * j : BX * (j + 1), :] = p
            if q == 1:
                pv = p
        weight = (TIME_STEP * WEIGHT_NEW) * fluid
        across_x = weight * (VISCOSITY + jnp.where(row == 0, 0.5, -0.5) * now[0])
        across_x = jnp.where((row == 0) | (row == BX - 1), across_x, 0.0)
        across_y = weight * (VISCOSITY + jnp.where(lane == 0, 0.5, -0.5) * now[1])
        edge_x[BX * z : BX * (z + 1), :] = across_x
        for t, pair in enumerate(((now[0], now[1]), (now[2], across_y), (pv, across_x))):
            for i in range(2):
                packs[t] = put(packs[t], pair[i], 64 * i + 2 * z)
    for z in range(NZ):
        u = cut(pred, z)
        v = cut(pred, NZ + z)
        zero = jnp.zeros_like(u)
        upper = cut(pred, 2 * NZ + z + 1) if z < NZ - 1 else zero
        lower = cut(pred, 2 * NZ + z - 1) if z > 0 else zero
        east = jnp.where(row == BX - 1, 0.0, turn(u, -1, 0))
        west = jnp.where(row == 0, 0.0, turn(u, 1, 0))
        north = jnp.where(lane == BY - 1, 0.0, turn(v, -1, 1))
        south = jnp.where(lane == 0, 0.0, turn(v, 1, 1))
        s = SCALE * ((east - west) + (north - south) + (upper - lower))
        source[BX * z : BX * (z + 1), :] = s
        to_low[8 * z : 8 * z + 8, :] = s[:8]
        to_high[8 * z : 8 * z + 8, :] = s[8:]
    half = NZ // 2
    sub = rows_of(8)
    for h in range(half):
        at = 8 * (NZ + h)
        a = source[BX * h : BX * (h + 1), :]
        b = source[BX * (h + half) : BX * (h + half + 1), :]
        to_low[at : at + 8, :] = jnp.where(sub < 4, a[8:], turn(b[8:], 4, 0))
        to_high[at : at + 8, :] = jnp.where(sub < 4, turn(b[:8], 4, 0), a[:8])
    for ref, r in ((to_low, 0), (to_high, BX - 1)):
        at = 12 * NZ
        ref[at : at + NZ, :] = edge_x[pl.ds(r, NZ, stride=BX), :]
        ref[at + NZ : at + 4 * NZ, :] = vel[pl.ds(r, 3 * NZ, stride=BX), :]
        ref[at + 4 * NZ : at + 5 * NZ, :] = pred[pl.ds(r, NZ, stride=BX), :]
        for t in range(3):
            ref[at + 5 * NZ + BX * t : at + 5 * NZ + BX * (t + 1), :] = packs[t]


def join_x_kernel(source, to_low, to_high, from_low, from_high, wide, to_left, to_right, fix_rows):
    lane = lanes(NZ)
    layer = rows_of(NZ)
    sub = rows_of(8)
    half = NZ // 2

    def line(ref, i):
        at = 12 * NZ + NZ * i
        return ref[at : at + NZ, :]

    def slope_y(f):
        return jnp.where(lane == BY - 1, 0.0, turn(f, -1, 1)) - jnp.where(lane == 0, 0.0, turn(f, 1, 1))

    def slope_z(f):
        return jnp.where(layer == NZ - 1, 0.0, turn(f, -1, 0)) - jnp.where(layer == 0, 0.0, turn(f, 1, 0))

    for z in range(NZ):
        w = WX * z
        wide[w : w + 16, :] = source[BX * z : BX * (z + 1), :]
        wide[w + 16 : w + 24, :] = from_high[8 * z : 8 * z + 8, :]
        at = 8 * (NZ + z % half)
        high = from_high[at : at + 8, :]
        low = from_low[at : at + 8, :]
        if z < half:
            wide[w + 24 : w + 32, :] = jnp.where(sub < 4, high, low)
        else:
            wide[w + 24 : w + 32, :] = turn(jnp.where(sub < 4, low, high), 4, 0)
        wide[w + 32 : w + 40, :] = from_low[8 * z : 8 * z + 8, :]

    def add(row, value):
        at = pl.ds(row % WX, NZ, stride=WX)
        wide[at, :] = wide[at, :] + SCALE * value

    for near, far, row, step, sign in ((to_low, from_low, 0, -1, 1.0), (to_high, from_high, 15, 1, -1.0)):
        inner = [line(near, 0) * line(far, 1 + q) for q in range(3)]
        outer = [line(far, 0) * line(near, 1 + q) for q in range(3)]
        add(row - step, -sign * inner[0])
        add(row, -sign * (line(far, 4) + outer[0]) + slope_y(inner[1]) + slope_z(inner[2]))
        add(row + step, sign * (line(near, 4) + inner[0]) + slope_y(outer[1]) + slope_z(outer[2]))
        add(row + 2 * step, sign * outer[0])
        for q in range(3):
            at = NZ * (3 * (step > 0) + q)
            fix_rows[at : at + NZ, :] = inner[q]

    stack = []
    for t in range(3):
        at = 17 * NZ + BX * t
        stack.append(jnp.concatenate([ref[at : at + BX, :] for ref in (to_low, from_high, from_low)], axis=0))
    first = rows_of(48) % BX == 0
    other = jnp.where(first, turn(stack[0], 1, 0), turn(stack[0], -1, 0))
    stack[2] = stack[2] + turn(stack[2] * other, 64, 1)
    lane = lanes(WX)
    for h in range(half):
        a = wide[WX * h : WX * (h + 1), :]
        b = turn(wide[WX * (h + half) : WX * (h + half + 1), :], 64, 1)
        to_left[WX * h : WX * (h + 1), :] = jnp.where(lane < 64, a, b)
        to_right[WX * h : WX * (h + 1), :] = jnp.where(lane < 64, b, a)
    for t in range(3):
        at = WX * half + 48 * t
        to_left[at : at + 48, :] = stack[t]
        to_right[at : at + 48, :] = stack[t]


def trimmed(a):
    return jnp.concatenate([a[0:24], a[32:40]], axis=0)


def fine_down_kernel(
    wide, sent_left, from_left, from_right,
    fd0_red, fd0_black, black0, sent_hbm, own1, up1, down1, fix_cols,
    fd_red, fd_black, red, black, res, thin, fd1_red, fd1_black, red1, black1, res1, sent, sems,
):
    lane = lanes(WX)
    odd = odd_cells(WX, 256)
    half = NZ // 2
    slots = NZ // 2

    lane48 = lanes(48)
    even = lane48 % 2 == 0
    low_half = lane48 < 64

    def pack_of(ref, t):
        at = WX * half + 48 * t
        return ref[at : at + 48, :]

    def swap(f):
        return turn(f, 64, 1)

    def both(f):
        return jnp.where(low_half, swap(f), f)

    def facing(left, right):
        return jnp.where(even, turn(right, -1, 1), turn(left, 1, 1))

    def slope_x(f):
        return turn(f, -1, 0) - turn(f, 1, 0)

    def slope_z(f):
        above = jnp.where(lane48 >= 2 * NZ - 2, 0.0, turn(f, -2, 1))
        below = jnp.where(lane48 < 2, 0.0, turn(f, 2, 1))
        return above - below

    def signed(f):
        return jnp.where(even, f, -f)

    own = [pack_of(sent_left, t) for t in range(3)]
    left = [pack_of(from_left, t) for t in range(3)]
    right = [pack_of(from_right, t) for t in range(3)]
    near = both(own[1])
    inner_uv = near * facing(left[0], right[0])
    inner_w = near * facing(left[1], right[1])
    far = both(jnp.where(even, left[1], right[1]))
    outer_uv = far * facing(own[0], own[0])
    outer_w = far * facing(own[1], own[1])
    inner_v = swap(inner_uv)
    outer_v = swap(outer_uv)
    pv_far = jnp.where(even, left[2], right[2]) + outer_v
    pv_own = own[2] + inner_v
    e0 = signed(facing(pv_far, pv_far)) + slope_x(inner_uv) + slope_z(inner_w)
    e1 = signed(facing(pv_own, pv_own)) + slope_x(outer_uv) + slope_z(outer_w)
    i = lax.broadcasted_iota(jnp.int32, (128, 128), 0)
    j = lax.broadcasted_iota(jnp.int32, (128, 128), 1)
    side = i % 2
    to = 4 * ((i % 64) // 2) + jnp.where(i < 64, 1 + side, 3 * side)
    order = SCALE * (to == j).astype(F32)
    mixed = []
    for e, v in ((e0, inner_v), (e1, outer_v)):
        m = jnp.where(low_half, e, swap(signed(v)))
        m = jnp.concatenate([m[0:24], jnp.where(rows_of(8) < 4, m[24:32], m[32:40]), m[40:48]], axis=0)
        mixed.append(matmul(m, order))
    edge = (lane < 2) | (lane >= BY - 2)

    def layer(z):
        t0 = wide[WX * z : WX * (z + 1), :]
        h = z % half
        a = from_right[WX * h : WX * (h + 1), :]
        b = from_left[WX * h : WX * (h + 1), :]
        if z < half:
            t1 = jnp.where(lane < 64, a, b)
        else:
            t1 = turn(jnp.where(lane < 64, b, a), 64, 1)
        t0 = t0 + jnp.where(edge, turn(mixed[0], 126 - 4 * z, 1), 0.0)
        t1 = t1 + jnp.where(edge, turn(mixed[1], 126 - 4 * z, 1), 0.0)
        return jnp.concatenate([t0, t1], axis=1)

    for k in range(slots):
        r, b = pack(layer(2 * k), layer(2 * k + 1), odd)
        r = scaled(r, 0, 0, k, slots, odd)
        b = scaled(b, 0, 1, k, slots, odd)
        fd_red[k] = r
        fd_black[k] = b
        fd0_red[k] = trimmed(r)
        fd0_black[k] = trimmed(b)
    half_sweep(black, fd_red, fd_black, 0, 1, slots, odd)
    half_sweep(red, black, fd_red, 0, 0, slots, odd)
    half_sweep(black, red, fd_black, 0, 1, slots, odd)
    for k in range(slots):
        res[32 * k : 32 * (k + 1), :] = trimmed(residual(red, black, fd_red, 0, k, slots, odd))
    matrix = 0.125 * halving(256, 128, lax.broadcasted_iota(jnp.int32, (256, 128), 1))
    thin[...] = matmul(res[...], matrix)
    n = BX * slots
    own1[...] = thin[pl.ds(0, n, stride=2), :] + thin[pl.ds(1, n, stride=2), :]

    odd1 = odd_cells(16, 128)
    slots1 = slots // 2
    sub = rows_of(8)

    def plane(z):
        return own1[16 * z : 16 * (z + 1), :]

    for k in range(slots1):
        r, b = pack(plane(2 * k), plane(2 * k + 1), odd1)
        fd1_red[k] = scaled(r, 1, 0, k, slots1, odd1)
        fd1_black[k] = scaled(b, 1, 1, k, slots1, odd1)
    half_sweep(black1, fd1_red, fd1_black, 1, 1, slots1, odd1)
    half_sweep(red1, black1, fd1_red, 1, 0, slots1, odd1)
    half_sweep(black1, red1, fd1_black, 1, 1, slots1, odd1)
    for k in range(slots1):
        res1[8 * k : 8 * k + 8, :] = residual(red1, black1, fd1_red, 1, k, slots1, odd1)[:8]
    res1[...] = matmul(res1[...], 0.125 * halving(128, 128, j % 64))
    v = res1[pl.ds(0, 32, stride=2), :] + res1[pl.ds(1, 32, stride=2), :]
    sent[...] = jnp.where(lanes(16) < 64, v[:16], v[16:])
    copies = [pltpu.make_async_copy(sent, sent_hbm.at[d], sems.at[d]) for d in range(sent_hbm.shape[0])]
    for copy in copies:
        copy.start()
    for k in range(slots):
        black0[k] = trimmed(black[k])
    for z in range(slots):
        a, b = plane(z)[:8], plane(z)[8:]
        up1[8 * z : 8 * z + 8, :] = jnp.where(sub < 4, a, b)
        down1[8 * z : 8 * z + 8, :] = jnp.where(sub < 4, b, a)
    fix_cols[0] = inner_uv[0:16]
    fix_cols[1] = inner_w[0:16]
    for copy in copies:
        copy.wait()


def predictor_kernel(pred, fix_rows, fix_cols, done):
    lane = lanes(BX)
    row = rows_of(BX)
    edge = (lane == 0) | (lane == BY - 1)
    for j in range(3 * NZ):
        q, z = divmod(j, NZ)
        low = jnp.broadcast_to(fix_rows[j : j + 1, :], (BX, BY))
        high = jnp.broadcast_to(fix_rows[3 * NZ + j : 3 * NZ + j + 1, :], (BX, BY))
        rim = jnp.where(row == 0, low, jnp.where(row == BX - 1, high, 0.0))
        column = turn(fix_cols[q // 2], -(64 * (q % 2) + 2 * z + 1), 1)
        rim = rim + jnp.where(edge, column, 0.0)
        done[BX * j : BX * (j + 1), :] = pred[BX * j : BX * (j + 1), :] + rim


def middle_kernel(own1, from_low, from_high, fd_red, fd_black, black, red):
    slots = 8
    odd = odd_cells(32, 128)
    sub = rows_of(8)

    def plane(z):
        a = own1[16 * z : 16 * z + 8, :]
        b = own1[16 * z + 8 : 16 * z + 16, :]
        low = from_low[8 * z : 8 * z + 8, :]
        high = from_high[8 * z : 8 * z + 8, :]
        tiles = [a] + [jnp.where(sub < 4, p, q) for p, q in ((b, high), (high, low), (low, b))]
        return jnp.concatenate(tiles, axis=0)

    for k in range(slots):
        r, b = pack(plane(2 * k), plane(2 * k + 1), odd)
        fd_red[k] = scaled(r, 1, 0, k, slots, odd)
        fd_black[k] = scaled(b, 1, 1, k, slots, odd)
    half_sweep(black, fd_red, fd_black, 1, 1, slots, odd)
    half_sweep(red, black, fd_red, 1, 0, slots, odd)
    half_sweep(black, red, fd_black, 1, 1, slots, odd)


def up_kernel(
    nx, g_own, g_left, g_right, fd1_red, fd1_black, black1_in, fd0_red, fd0_black, black0_in, pred, obst,
    corrected_hbm, pressure_hbm, fd2_red, fd2_black, red2, black2, res2, fd3, red1, black1, big1, red0, black0, big0, ring, corrected, pressure, sems,
):
    x2 = 4 * nx
    lane = lanes(x2)
    odd2 = odd_cells(x2, 128)
    slots2 = 4

    for i, g in enumerate((g_own, g_right, g_left)):
        for j in range(nx):
            d = lax.rem(lax.axis_index("gx") + j, nx)
            for z in range(4):
                ring[4 * i + z, 4 * j : 4 * j + 4, :] = g[d, 4 * z : 4 * z + 4, :]

    def rhs2(z):
        lift = 64 * (z // 4)
        own, right, left = (ring[4 * i + z % 4] for i in range(3))
        own = turn(own, -lift, 1) if lift else own
        right = turn(right, 32 - lift, 1)
        left = jnp.where(lane < 96, turn(left, 32 - lift, 1), turn(left, 96 - lift, 1))
        return jnp.where(lane < 32, own, jnp.where(lane < 80, right, left))

    for k in range(slots2):
        r, b = pack(rhs2(2 * k), rhs2(2 * k + 1), odd2)
        fd2_red[k] = scaled(r, 2, 0, k, slots2, odd2)
        fd2_black[k] = scaled(b, 2, 1, k, slots2, odd2)
    half_sweep(black2, fd2_red, fd2_black, 2, 1, slots2, odd2)
    half_sweep(red2, black2, fd2_red, 2, 0, slots2, odd2)
    half_sweep(black2, red2, fd2_black, 2, 1, slots2, odd2)
    for k in range(slots2):
        res2[x2 * k : x2 * (k + 1), :] = residual(red2, black2, fd2_red, 2, k, slots2, odd2)
    col = lax.broadcasted_iota(jnp.int32, (128, 128), 1)
    res2[...] = matmul(res2[...], 0.125 * halving(128, 128, col % 64))
    n = slots2 * x2 // 2
    x3 = x2 // 2
    fd3[...] = res2[pl.ds(0, n, stride=2), :] + res2[pl.ds(1, n, stride=2), :]

    odd3 = odd_cells(x3, 128)
    fr, fb = [], []
    for k in range(2):
        r, b = pack(fd3[x3 * 2 * k : x3 * (2 * k + 1), :], fd3[x3 * (2 * k + 1) : x3 * (2 * k + 2), :], odd3)
        fr.append(scaled(r, 3, 0, k, 2, odd3))
        fb.append(scaled(b, 3, 1, k, 2, odd3))
    r = fr
    for step in range(8):
        if step > 0:
            r = [relaxed(b, fr, 3, 0, k, 2, odd3) for k in range(2)]
        b = [relaxed(r, fb, 3, 1, k, 2, odd3) for k in range(2)]

    def layers(red, black, odd):
        return jnp.where(odd, black, red), jnp.where(odd, red, black)

    parts = []
    for k in range(2):
        parts += layers(r[k], b[k], odd3)
    e = matmul(jnp.concatenate(parts, axis=0), doubling(128, 128, col // 2))
    res2[pl.ds(0, n, stride=2), :] = e
    res2[pl.ds(1, n, stride=2), :] = e
    for k in range(slots2):
        black2[k] = black2[k] + res2[x2 * k : x2 * (k + 1), :]
    half_sweep(red2, black2, fd2_red, 2, 0, slots2, odd2)
    half_sweep(black2, red2, fd2_black, 2, 1, slots2, odd2)
    half_sweep(red2, black2, fd2_red, 2, 0, slots2, odd2)
    half_sweep(black2, red2, fd2_black, 2, 1, slots2, odd2)

    odd1 = odd_cells(32, 128)
    slots1 = 8
    sub = rows_of(8)
    for k in range(slots2):
        for i, v in enumerate(layers(red2[k], black2[k], odd2)):
            at = 16 * (2 * k + i)
            big1[at : at + 8, :] = v[0:8]
            big1[at + 8 : at + 16, :] = jnp.where(sub < 2, v[8:16] if nx > 2 else v[0:8], v[x2 - 8 : x2])
    e = matmul(big1[0 : 16 * slots1, :], doubling(128, 128, jnp.where(col < 96, col // 2, col // 2 + 64)))
    big1[pl.ds(0, 16 * slots1, stride=2), :] = e
    big1[pl.ds(1, 16 * slots1, stride=2), :] = e
    for k in range(slots1):
        black1[k] = black1_in[k] + big1[32 * k : 32 * (k + 1), :]
    half_sweep(red1, black1, fd1_red, 1, 0, slots1, odd1)
    half_sweep(black1, red1, fd1_black, 1, 1, slots1, odd1)
    half_sweep(red1, black1, fd1_red, 1, 0, slots1, odd1)
    half_sweep(black1, red1, fd1_black, 1, 1, slots1, odd1)

    slots0 = NZ // 2
    for k in range(slots1):
        low, high = layers(red1[k], black1[k], odd1)
        for i, v in enumerate((low, high)):
            at = 16 * (2 * k + i)
            big1[at : at + 8, :] = v[0:8]
            big1[at + 8 : at + 16, :] = jnp.where(sub < 4, v[8:16], v[24:32])
    wide_col = lax.broadcasted_iota(jnp.int32, (128, 256), 1)
    e = matmul(big1[0 : 16 * slots0, :], doubling(128, 256, wide_col // 2))
    for t in range(2):
        part = e[:, 128 * t : 128 * t + 128]
        big0[t, pl.ds(0, 16 * slots0, stride=2), :] = part
        big0[t, pl.ds(1, 16 * slots0, stride=2), :] = part
    odd0 = odd_cells(32, 256)
    for k in range(slots0):
        add = jnp.concatenate([big0[t, 32 * k : 32 * (k + 1), :] for t in range(2)], axis=1)
        black0[k] = black0_in[k] + add
    half_sweep(red0, black0, fd0_red, 0, 0, slots0, odd0)
    half_sweep(black0, red0, fd0_black, 0, 1, slots0, odd0)
    half_sweep(red0, black0, fd0_red, 0, 0, slots0, odd0)
    half_sweep(black0, red0, fd0_black, 0, 1, slots0, odd0)
    for k in range(slots0):
        low, high = layers(red0[k], black0[k], odd0)
        red0[k] = low
        black0[k] = high

    depth = 8
    copies = []

    def full(z):
        return (black0 if z % 2 else red0)[z // 2]

    for z in range(NZ):
        p = full(z)
        own = p[0:16, 0:128]
        pressure[BX * z : BX * (z + 1), :] = own
        zero = jnp.zeros_like(own)
        upper = full(z + 1)[0:16, 0:128] if z < NZ - 1 else zero
        lower = full(z - 1)[0:16, 0:128] if z > 0 else zero
        gx = turn(p, -1, 0)[0:16, 0:128] - turn(p, 1, 0)[0:16, 0:128]
        mid = p[0:16]
        gy = turn(mid, -1, 1)[:, 0:128] - turn(mid, 1, 1)[:, 0:128]
        fluid = (1 - obst[BX * z : BX * (z + 1), :]).astype(F32)
        for q, g in enumerate((gx, gy, upper - lower)):
            j = q * NZ + z
            v = pred[BX * j : BX * (j + 1), :]
            corrected[BX * j : BX * (j + 1), :] = fluid * (v - (0.5 * TIME_STEP) * g)
        if z % depth == depth - 1:
            c = z // depth
            for i in range(4):
                src, dst = (corrected, corrected_hbm) if i < 3 else (pressure, pressure_hbm)
                at = pl.ds(((i % 3) * NZ + c * depth) * BX, depth * BX)
                copies.append(pltpu.make_async_copy(src.at[at, :], dst.at[at, :], sems.at[c, i]))
                copies[-1].start()
    for copy in copies:
        copy.wait()


def both_ways(axis, to_low, to_high):
    n = lax.axis_size(axis)
    up = [(i, (i + 1) % n) for i in range(n)]
    down = [((i + 1) % n, i) for i in range(n)]
    return lax.ppermute(to_high, axis, up), lax.ppermute(to_low, axis, down)


def body(velocity, old_tendency, obstacle):
    nx = lax.axis_size("gx")
    vel = velocity.reshape(3 * NZ * BX, BY)
    old = old_tendency.reshape(3 * NZ * BX, BY)
    obst = obstacle.reshape(NZ * BX, BY)

    block = 3 * NZ * BX
    within = pl.BlockSpec(memory_space=pltpu.VMEM)
    anywhere = [pl.BlockSpec(memory_space=pltpu.HBM)] * 3
    pred, source, to_low, to_high = call(
        local_kernel,
        (vmem(block, BY), vmem(NZ * BX, BY), vmem(592, BY), vmem(592, BY)),
        tuple(pltpu.with_memory_space_constraint(a, pltpu.HBM) for a in (vel, old, obst)),
        [
            pltpu.VMEM((block, BY), F32),
            pltpu.VMEM((block, BY), F32),
            pltpu.VMEM((NZ * BX, BY), jnp.int32),
            pltpu.VMEM((NZ * BX, BY), F32),
            pltpu.SemaphoreType.DMA((CHUNKS, 7)),
        ],
        in_specs=anywhere,
        name="local",
    )
    from_low, from_high = both_ways("gx", to_low, to_high)
    wide, to_left, to_right, fix_rows = call(
        join_x_kernel,
        (vmem(NZ * WX, BY), vmem(784, BY), vmem(784, BY), vmem(6 * NZ, BY)),
        (source, to_low, to_high, from_low, from_high),
        name="join_x",
    )
    from_left, from_right = both_ways("gy", to_left, to_right)
    fd0_red, fd0_black, black0, sent, own1, up1, down1, fix_cols = call(
        fine_down_kernel,
        (
            vmem(16, 32, 256),
            vmem(16, 32, 256),
            vmem(16, 32, 256),
            vmem(nx, 16, BY),
            vmem(256, BY),
            vmem(128, BY),
            vmem(128, BY),
            vmem(2, BX, BY),
        ),
        (wide, to_left, from_left, from_right),
        [(16, WX, 256)] * 4
        + [(512, 256), (512, BY)]
        + [(8, 16, BY)] * 4
        + [(64, BY), (16, BY), pltpu.SemaphoreType.DMA((nx,))],
        out_specs=(within,) * 3 + (pl.BlockSpec(memory_space=pl.ANY),) + (within,) * 4,
        name="fine_down",
    )
    gathered = lax.all_to_all(sent, "gx", 0, 0)
    low1, high1 = both_ways("gx", down1, up1)
    fd1_red, fd1_black, black1 = call(
        middle_kernel, (vmem(8, 32, BY),) * 3, (own1, low1, high1), [(8, 32, BY)], name="middle"
    )
    pred = call(predictor_kernel, vmem(block, BY), (pred, fix_rows, fix_cols), name="predictor")
    g_left, g_right = both_ways("gy", gathered, gathered)
    x2 = 4 * nx
    corrected, pressure = call(
        functools.partial(up_kernel, nx),
        (vmem(block, BY), vmem(NZ * BX, BY)),
        (gathered, g_left, g_right, fd1_red, fd1_black, black1, fd0_red, fd0_black, black0, pred, obst),
        [(4, x2, BY)] * 4
        + [(4 * x2, BY), (2 * x2, BY)]
        + [(8, 32, BY)] * 2
        + [(256, BY)]
        + [(16, 32, 256)] * 2
        + [(2, 512, BY), (12, x2, BY), (block, BY), (NZ * BX, BY), pltpu.SemaphoreType.DMA((4, 4))],
        out_specs=(pl.BlockSpec(memory_space=pl.ANY),) * 2,
        name="up",
    )
    return corrected.reshape(3, NZ, BX, BY), pressure.reshape(NZ, BX, BY)


def solution(mesh):
    placed = (P(None, None, "gx", "gy"), P(None, None, "gx", "gy"), P(None, "gx", "gy"))
    return jax.shard_map(
        body,
        mesh=mesh,
        in_specs=placed,
        out_specs=(P(None, None, "gx", "gy"), P(None, "gx", "gy")),
        check_vma=False,
    )
```

```python
import functools

import jax
import jax.numpy as jnp
from jax import lax
from jax.experimental import pallas as pl
from jax.experimental.pallas import tpu as pltpu
from jax.sharding import PartitionSpec as P

TIME_STEP = 0.25
VISCOSITY = 0.1
WEIGHT_NEW = 15.0 / 16.0
WEIGHT_OLD = -25.0 / 48.0
HELMHOLTZ = 1.0e-4
SCALE = -0.5 / TIME_STEP
INTERPRET = False
F32 = jnp.float32
NZ = 32
BX = 16
BY = 128
WX = 40
CHUNKS = 8


def vmem(*shape):
    return jax.ShapeDtypeStruct(shape, F32)


def call(kernel, outs, args, scratch=(), in_specs=None, out_specs=None, name=None):
    everywhere = pl.BlockSpec(memory_space=pltpu.VMEM)
    return pl.pallas_call(
        kernel,
        out_shape=outs,
        out_specs=out_specs or jax.tree.map(lambda _: everywhere, outs),
        in_specs=in_specs or [everywhere] * len(args),
        scratch_shapes=[pltpu.VMEM(s, F32) if isinstance(s, tuple) else s for s in scratch],
        compiler_params=pltpu.CompilerParams(vmem_limit_bytes=16 << 20),
        interpret=INTERPRET,
        name=name,
    )(*args)


def turn(a, shift, axis):
    return pltpu.roll(a, shift % a.shape[axis], axis)


def lanes(rows, cols=128):
    return lax.broadcasted_iota(jnp.int32, (rows, cols), 1)


def rows_of(rows, cols=128):
    return lax.broadcasted_iota(jnp.int32, (rows, cols), 0)


def odd_cells(rows, cols):
    return (rows_of(rows, cols) + lanes(rows, cols)) % 2 == 1


def diag(level, m):
    return HELMHOLTZ + (4.0 + m) / float(4**level)


def at_end(colour, k, count, odd, inner, end):
    if k == 0:
        return jnp.where(odd, inner, end) if colour == 0 else jnp.where(odd, end, inner)
    if k == count - 1:
        return jnp.where(odd, end, inner) if colour == 0 else jnp.where(odd, inner, end)
    return inner


def pack(low, high, odd):
    return jnp.where(odd, high, low), jnp.where(odd, low, high)


def scaled(value, level, colour, k, count, odd):
    return value * at_end(colour, k, count, odd, 1.0 / diag(level, 2), 1.0 / diag(level, 1))


def put(dst, k, tiles):
    n = tiles[0].shape[0]
    for t, v in enumerate(tiles):
        dst[t, k, 8 : 8 + n, :] = v
        dst[t, k, 7:8, :] = v[n - 1 : n]
        dst[t, k, 8 + n : 9 + n, :] = v[0:1]


def get(src, k, shift=0):
    tiles, _, rows, _ = src.shape
    return [src[t, k, 8 + shift : rows - 8 + shift, :] for t in range(tiles)]


def beside(tiles):
    if len(tiles) == 1:
        return [turn(tiles[0], 1, 1) + turn(tiles[0], -1, 1)]
    lane = lanes(tiles[0].shape[0])
    out = []
    for own, other in (tiles, tiles[::-1]):
        last = jnp.where(lane == BY - 1, other, own)
        first = jnp.where(lane == 0, other, own)
        out.append(turn(last, 1, 1) + turn(first, -1, 1))
    return out


def vertical(above, below, colour, odd):
    return jnp.where(odd, above, below) if colour == 0 else jnp.where(odd, below, above)


def weight_of(level, colour, k, count, odd):
    s = float(4**level)
    return at_end(colour, k, count, odd, 1.0 / s / diag(level, 2), 1.0 / s / diag(level, 1))


def relaxed(src, fd, level, colour, k, count, odd):
    b = get(src, k)
    zero = [jnp.zeros_like(v) for v in b]
    above = get(src, k + 1) if k < count - 1 else zero
    below = get(src, k - 1) if k > 0 else zero
    c = weight_of(level, colour, k, count, odd)
    out = []
    for t, (y, low, high) in enumerate(zip(beside(b), get(src, k, -1), get(src, k, 1))):
        z = vertical(above[t], below[t], colour, odd)
        out.append(fd[t, k] + c * ((y + (low + high)) + (b[t] + z)))
    return out


def half_sweep(dst, src, fd, level, colour, count, odd):
    for k in range(count):
        put(dst, k, relaxed(src, fd, level, colour, k, count, odd))


def first_sweeps(red, black, fd_red, fd_black, level, count, odd):
    for k in range(count):
        put(red, k, [fd_red[t, k] for t in range(red.shape[0])])
    half_sweep(black, red, fd_black, level, 1, count, odd)
    half_sweep(red, black, fd_red, level, 0, count, odd)
    half_sweep(black, red, fd_black, level, 1, count, odd)


def last_sweeps(red, black, fd_red, fd_black, level, count, odd):
    for _ in range(2):
        half_sweep(red, black, fd_red, level, 0, count, odd)
        half_sweep(black, red, fd_black, level, 1, count, odd)


def residual(red, black, fd, level, k, count, odd):
    d = at_end(0, k, count, odd, diag(level, 2), diag(level, 1))
    return [d * (new - old) for new, old in zip(relaxed(black, fd, level, 0, k, count, odd), get(red, k))]


def shifted(slots, reach):
    return {s: [turn(v, s, 1) if s else v for v in slots] for s in range(-reach, reach + 1)}


def relaxed_shifted(src, fd, reach, level, colour, parity):
    out = {}
    for s in range(-reach, reach + 1):
        odd = parity[s % 2]
        slots = src[s]
        count = len(slots)
        new = []
        for k in range(count):
            b = slots[k]
            zero = jnp.zeros_like(b)
            z = vertical(slots[k + 1] if k < count - 1 else zero, slots[k - 1] if k > 0 else zero, colour, odd)
            y = src[s - 1][k] + src[s + 1][k]
            x = turn(b, 1, 0) + turn(b, -1, 0)
            new.append(fd[s][k] + weight_of(level, colour, k, count, odd) * ((y + x) + (b + z)))
        out[s] = new
    return out


def halving(n, m, target):
    i = lax.broadcasted_iota(jnp.int32, (n, m), 0)
    return (i // 2 == target).astype(F32)


def doubling(n, m, target):
    i = lax.broadcasted_iota(jnp.int32, (n, m), 0)
    return (i == target).astype(F32)


def matmul(a, b):
    return jnp.dot(a, b, precision=lax.Precision.HIGHEST, preferred_element_type=F32)


def local_kernel(vel_hbm, old_hbm, obst_hbm, pred, source, to_low, to_high, vel, old, obst, edge_x, sems):
    lane = lanes(BX)
    row = rows_of(BX)
    depth = NZ // CHUNKS
    copies = []
    for c in range(CHUNKS):
        group = []
        for i, (src, dst, q) in enumerate(
            [(vel_hbm, vel, q) for q in range(3)] + [(old_hbm, old, q) for q in range(3)] + [(obst_hbm, obst, 0)]
        ):
            at = pl.ds((q * NZ + c * depth) * BX, depth * BX)
            group.append(pltpu.make_async_copy(src.at[at, :], dst.at[at, :], sems.at[c, i]))
        copies.append(group)
    for c in range(CHUNKS):
        for copy in copies[c]:
            copy.start()

    def cut(ref, j):
        return ref[BX * j : BX * (j + 1), :]

    packs = [jnp.zeros((BX, BY), F32) for _ in range(3)]

    def put_pair(pack, value, at):
        return jnp.where((lane == at) | (lane == at + 1), turn(value, at + 1, 1), pack)

    for copy in copies[0]:
        copy.wait()
    for z in range(NZ):
        if z % depth == depth - 1 and z < NZ - 1:
            for copy in copies[z // depth + 1]:
                copy.wait()
        fluid = (1 - cut(obst, z)).astype(F32)
        now = [cut(vel, q * NZ + z) for q in range(3)]
        spread = (TIME_STEP * WEIGHT_NEW * VISCOSITY) * fluid
        carry = (TIME_STEP * WEIGHT_NEW * 0.5) * fluid
        flow = [carry * v for v in now]
        plus = [spread - v for v in flow]
        minus = [spread + v for v in flow]
        across_x = jnp.where(row == 0, minus[0], jnp.where(row == BX - 1, plus[0], 0.0))
        across_y = jnp.where(lane == 0, minus[1], plus[1])
        plus_x = jnp.where(row == BX - 1, 0.0, plus[0])
        minus_x = jnp.where(row == 0, 0.0, minus[0])
        plus_y = jnp.where(lane == BY - 1, 0.0, plus[1])
        minus_y = jnp.where(lane == 0, 0.0, minus[1])
        keep = (1.0 - 6.0 * TIME_STEP * WEIGHT_NEW * VISCOSITY) * fluid
        past = (TIME_STEP * WEIGHT_OLD) * fluid
        for q in range(3):
            j = q * NZ + z
            v = now[q]
            p = keep * v + past * cut(old, j)
            p = p + (plus_x * turn(v, -1, 0) + minus_x * turn(v, 1, 0))
            p = p + (plus_y * turn(v, -1, 1) + minus_y * turn(v, 1, 1))
            if z < NZ - 1:
                p = p + plus[2] * cut(vel, j + 1)
            if z > 0:
                p = p + minus[2] * cut(vel, j - 1)
            pred[BX * j : BX * (j + 1), :] = p
            if q == 1:
                pv = p
        edge_x[BX * z : BX * (z + 1), :] = across_x
        for t, pair in enumerate(((now[0], now[1]), (now[2], across_y), (pv, across_x))):
            for i in range(2):
                packs[t] = put_pair(packs[t], pair[i], 64 * i + 2 * z)
    for z in range(NZ):
        u = cut(pred, z)
        v = cut(pred, NZ + z)
        zero = jnp.zeros_like(u)
        upper = cut(pred, 2 * NZ + z + 1) if z < NZ - 1 else zero
        lower = cut(pred, 2 * NZ + z - 1) if z > 0 else zero
        east = jnp.where(row == BX - 1, 0.0, turn(u, -1, 0))
        west = jnp.where(row == 0, 0.0, turn(u, 1, 0))
        north = jnp.where(lane == BY - 1, 0.0, turn(v, -1, 1))
        south = jnp.where(lane == 0, 0.0, turn(v, 1, 1))
        s = SCALE * ((east - west) + (north - south) + (upper - lower))
        source[BX * z : BX * (z + 1), :] = s
        to_low[8 * z : 8 * z + 8, :] = s[:8]
        to_high[8 * z : 8 * z + 8, :] = s[8:]
    half = NZ // 2
    sub = rows_of(8)
    for h in range(half):
        at = 8 * (NZ + h)
        a = source[BX * h : BX * (h + 1), :]
        b = source[BX * (h + half) : BX * (h + half + 1), :]
        to_low[at : at + 8, :] = jnp.where(sub < 4, a[8:], turn(b[8:], 4, 0))
        to_high[at : at + 8, :] = jnp.where(sub < 4, turn(b[:8], 4, 0), a[:8])
    for ref, r in ((to_low, 0), (to_high, BX - 1)):
        at = 12 * NZ
        ref[at : at + NZ, :] = edge_x[pl.ds(r, NZ, stride=BX), :]
        ref[at + NZ : at + 4 * NZ, :] = vel[pl.ds(r, 3 * NZ, stride=BX), :]
        ref[at + 4 * NZ : at + 5 * NZ, :] = pred[pl.ds(r, NZ, stride=BX), :]
        for t in range(3):
            ref[at + 5 * NZ + BX * t : at + 5 * NZ + BX * (t + 1), :] = packs[t]


def join_x_kernel(source, to_low, to_high, from_low, from_high, wide, to_left, to_right, fix_rows):
    lane = lanes(NZ)
    layer = rows_of(NZ)
    sub = rows_of(8)
    half = NZ // 2

    def line(ref, i):
        at = 12 * NZ + NZ * i
        return ref[at : at + NZ, :]

    def slope_y(f):
        return jnp.where(lane == BY - 1, 0.0, turn(f, -1, 1)) - jnp.where(lane == 0, 0.0, turn(f, 1, 1))

    def slope_z(f):
        return jnp.where(layer == NZ - 1, 0.0, turn(f, -1, 0)) - jnp.where(layer == 0, 0.0, turn(f, 1, 0))

    for z in range(NZ):
        w = WX * z
        wide[w : w + 16, :] = source[BX * z : BX * (z + 1), :]
        wide[w + 16 : w + 24, :] = from_high[8 * z : 8 * z + 8, :]
        at = 8 * (NZ + z % half)
        high = from_high[at : at + 8, :]
        low = from_low[at : at + 8, :]
        if z < half:
            wide[w + 24 : w + 32, :] = jnp.where(sub < 4, high, low)
        else:
            wide[w + 24 : w + 32, :] = turn(jnp.where(sub < 4, low, high), 4, 0)
        wide[w + 32 : w + 40, :] = from_low[8 * z : 8 * z + 8, :]

    def add(row, value):
        at = pl.ds(row % WX, NZ, stride=WX)
        wide[at, :] = wide[at, :] + SCALE * value

    for near, far, row, step, sign in ((to_low, from_low, 0, -1, 1.0), (to_high, from_high, 15, 1, -1.0)):
        inner = [line(near, 0) * line(far, 1 + q) for q in range(3)]
        outer = [line(far, 0) * line(near, 1 + q) for q in range(3)]
        add(row - step, -sign * inner[0])
        add(row, -sign * (line(far, 4) + outer[0]) + slope_y(inner[1]) + slope_z(inner[2]))
        add(row + step, sign * (line(near, 4) + inner[0]) + slope_y(outer[1]) + slope_z(outer[2]))
        add(row + 2 * step, sign * outer[0])
        for q in range(3):
            at = NZ * (3 * (step > 0) + q)
            fix_rows[at : at + NZ, :] = inner[q]

    stack = []
    for t in range(3):
        at = 17 * NZ + BX * t
        stack.append(jnp.concatenate([ref[at : at + BX, :] for ref in (to_low, from_high, from_low)], axis=0))
    first = rows_of(48) % BX == 0
    other = jnp.where(first, turn(stack[0], 1, 0), turn(stack[0], -1, 0))
    stack[2] = stack[2] + turn(stack[2] * other, 64, 1)
    lane = lanes(WX)
    for h in range(half):
        a = wide[WX * h : WX * (h + 1), :]
        b = turn(wide[WX * (h + half) : WX * (h + half + 1), :], 64, 1)
        to_left[WX * h : WX * (h + 1), :] = jnp.where(lane < 64, a, b)
        to_right[WX * h : WX * (h + 1), :] = jnp.where(lane < 64, b, a)
    for t in range(3):
        at = WX * half + 48 * t
        to_left[at : at + 48, :] = stack[t]
        to_right[at : at + 48, :] = stack[t]


def trimmed(a):
    return jnp.concatenate([a[0:24], a[32:40]], axis=0)


def fine_down_kernel(
    wide, sent_left, from_left, from_right,
    fd0_red, fd0_black, black0, sent_hbm, own1, up1, down1, fix_cols,
    fd_red, fd_black, red, black, res, thin, fd1_red, fd1_black, red1, black1, res1, sent, sems,
):
    lane = lanes(WX)
    odd = odd_cells(WX, 128)
    half = NZ // 2
    slots = NZ // 2

    lane48 = lanes(48)
    even = lane48 % 2 == 0
    low_half = lane48 < 64

    def pack_of(ref, t):
        at = WX * half + 48 * t
        return ref[at : at + 48, :]

    def swap(f):
        return turn(f, 64, 1)

    def both(f):
        return jnp.where(low_half, swap(f), f)

    def facing(left, right):
        return jnp.where(even, turn(right, -1, 1), turn(left, 1, 1))

    def slope_x(f):
        return turn(f, -1, 0) - turn(f, 1, 0)

    def slope_z(f):
        above = jnp.where(lane48 >= 2 * NZ - 2, 0.0, turn(f, -2, 1))
        below = jnp.where(lane48 < 2, 0.0, turn(f, 2, 1))
        return above - below

    def signed(f):
        return jnp.where(even, f, -f)

    own = [pack_of(sent_left, t) for t in range(3)]
    left = [pack_of(from_left, t) for t in range(3)]
    right = [pack_of(from_right, t) for t in range(3)]
    near = both(own[1])
    inner_uv = near * facing(left[0], right[0])
    inner_w = near * facing(left[1], right[1])
    far = both(jnp.where(even, left[1], right[1]))
    outer_uv = far * facing(own[0], own[0])
    outer_w = far * facing(own[1], own[1])
    inner_v = swap(inner_uv)
    outer_v = swap(outer_uv)
    pv_far = jnp.where(even, left[2], right[2]) + outer_v
    pv_own = own[2] + inner_v
    e0 = signed(facing(pv_far, pv_far)) + slope_x(inner_uv) + slope_z(inner_w)
    e1 = signed(facing(pv_own, pv_own)) + slope_x(outer_uv) + slope_z(outer_w)
    i = lax.broadcasted_iota(jnp.int32, (128, 128), 0)
    j = lax.broadcasted_iota(jnp.int32, (128, 128), 1)
    side = i % 2
    to = 4 * ((i % 64) // 2) + jnp.where(i < 64, 1 + side, 3 * side)
    order = SCALE * (to == j).astype(F32)
    mixed = []
    for e, v in ((e0, inner_v), (e1, outer_v)):
        m = jnp.where(low_half, e, swap(signed(v)))
        m = jnp.concatenate([m[0:24], jnp.where(rows_of(8) < 4, m[24:32], m[32:40]), m[40:48]], axis=0)
        mixed.append(matmul(m, order))
    edge = (lane < 2) | (lane >= BY - 2)

    def layer(z):
        t0 = wide[WX * z : WX * (z + 1), :]
        h = z % half
        a = from_right[WX * h : WX * (h + 1), :]
        b = from_left[WX * h : WX * (h + 1), :]
        if z < half:
            t1 = jnp.where(lane < 64, a, b)
        else:
            t1 = turn(jnp.where(lane < 64, b, a), 64, 1)
        t0 = t0 + jnp.where(edge, turn(mixed[0], 126 - 4 * z, 1), 0.0)
        t1 = t1 + jnp.where(edge, turn(mixed[1], 126 - 4 * z, 1), 0.0)
        return t0, t1

    for k in range(slots):
        for t, (low, high) in enumerate(zip(layer(2 * k), layer(2 * k + 1))):
            r, b = pack(low, high, odd)
            r = scaled(r, 0, 0, k, slots, odd)
            b = scaled(b, 0, 1, k, slots, odd)
            fd_red[t, k] = r
            fd_black[t, k] = b
            fd0_red[t, k] = trimmed(r)
            fd0_black[t, k] = trimmed(b)
    first_sweeps(red, black, fd_red, fd_black, 0, slots, odd)
    for k in range(slots):
        for t, r in enumerate(residual(red, black, fd_red, 0, k, slots, odd)):
            res[32 * k : 32 * (k + 1), 128 * t : 128 * t + 128] = trimmed(r)
    matrix = 0.125 * halving(256, 128, lax.broadcasted_iota(jnp.int32, (256, 128), 1))
    thin[...] = matmul(res[...], matrix)
    n = BX * slots
    own1[...] = thin[pl.ds(0, n, stride=2), :] + thin[pl.ds(1, n, stride=2), :]

    odd1 = odd_cells(16, 128)
    slots1 = slots // 2
    sub = rows_of(8)

    def plane(z):
        return own1[16 * z : 16 * (z + 1), :]

    for k in range(slots1):
        r, b = pack(plane(2 * k), plane(2 * k + 1), odd1)
        fd1_red[0, k] = scaled(r, 1, 0, k, slots1, odd1)
        fd1_black[0, k] = scaled(b, 1, 1, k, slots1, odd1)
    first_sweeps(red1, black1, fd1_red, fd1_black, 1, slots1, odd1)
    for k in range(slots1):
        res1[8 * k : 8 * k + 8, :] = residual(red1, black1, fd1_red, 1, k, slots1, odd1)[0][:8]
    res1[...] = matmul(res1[...], 0.125 * halving(128, 128, j % 64))
    v = res1[pl.ds(0, 32, stride=2), :] + res1[pl.ds(1, 32, stride=2), :]
    sent[...] = jnp.where(lanes(16) < 64, v[:16], v[16:])
    copies = [pltpu.make_async_copy(sent, sent_hbm.at[d], sems.at[d]) for d in range(sent_hbm.shape[0])]
    for copy in copies:
        copy.start()
    for k in range(slots):
        for t, v in enumerate(get(black, k)):
            black0[t, k] = trimmed(v)
    for z in range(slots):
        a, b = plane(z)[:8], plane(z)[8:]
        up1[8 * z : 8 * z + 8, :] = jnp.where(sub < 4, a, b)
        down1[8 * z : 8 * z + 8, :] = jnp.where(sub < 4, b, a)
    fix_cols[0] = inner_uv[0:16]
    fix_cols[1] = inner_w[0:16]
    for copy in copies:
        copy.wait()


def predictor_kernel(pred, fix_rows, fix_cols, done):
    lane = lanes(BX)
    row = rows_of(BX)
    edge = (lane == 0) | (lane == BY - 1)
    for j in range(3 * NZ):
        q, z = divmod(j, NZ)
        low = jnp.broadcast_to(fix_rows[j : j + 1, :], (BX, BY))
        high = jnp.broadcast_to(fix_rows[3 * NZ + j : 3 * NZ + j + 1, :], (BX, BY))
        rim = jnp.where(row == 0, low, jnp.where(row == BX - 1, high, 0.0))
        column = turn(fix_cols[q // 2], -(64 * (q % 2) + 2 * z + 1), 1)
        rim = rim + jnp.where(edge, column, 0.0)
        done[BX * j : BX * (j + 1), :] = pred[BX * j : BX * (j + 1), :] + rim


def middle_kernel(own1, from_low, from_high, fd_red, fd_black, done, red, black):
    slots = 8
    odd = odd_cells(32, 128)
    sub = rows_of(8)

    def plane(z):
        a = own1[16 * z : 16 * z + 8, :]
        b = own1[16 * z + 8 : 16 * z + 16, :]
        low = from_low[8 * z : 8 * z + 8, :]
        high = from_high[8 * z : 8 * z + 8, :]
        tiles = [a] + [jnp.where(sub < 4, p, q) for p, q in ((b, high), (high, low), (low, b))]
        return jnp.concatenate(tiles, axis=0)

    for k in range(slots):
        r, b = pack(plane(2 * k), plane(2 * k + 1), odd)
        fd_red[0, k] = scaled(r, 1, 0, k, slots, odd)
        fd_black[0, k] = scaled(b, 1, 1, k, slots, odd)
    first_sweeps(red, black, fd_red, fd_black, 1, slots, odd)
    for k in range(slots):
        done[k] = get(black, k)[0]


def up_kernel(
    nx, g_own, g_left, g_right, fd1_red, fd1_black, black1_in, fd0_red, fd0_black, black0_in, pred, obst,
    corrected_hbm, pressure_hbm, fd2_red, fd2_black, red2, black2, res2, fd3, red1, black1, big1, red0, black0, big0, ring, corrected, pressure, sems,
):
    x2 = 4 * nx
    lane = lanes(x2)
    odd2 = odd_cells(x2, 128)
    slots2 = 4

    for i, g in enumerate((g_own, g_right, g_left)):
        for j in range(nx):
            d = lax.rem(lax.axis_index("gx") + j, nx)
            for z in range(4):
                ring[4 * i + z, 4 * j : 4 * j + 4, :] = g[d, 4 * z : 4 * z + 4, :]

    def rhs2(z):
        lift = 64 * (z // 4)
        own, right, left = (ring[4 * i + z % 4] for i in range(3))
        own = turn(own, -lift, 1) if lift else own
        right = turn(right, 32 - lift, 1)
        left = jnp.where(lane < 96, turn(left, 32 - lift, 1), turn(left, 96 - lift, 1))
        return jnp.where(lane < 32, own, jnp.where(lane < 80, right, left))

    for k in range(slots2):
        r, b = pack(rhs2(2 * k), rhs2(2 * k + 1), odd2)
        fd2_red[0, k] = scaled(r, 2, 0, k, slots2, odd2)
        fd2_black[0, k] = scaled(b, 2, 1, k, slots2, odd2)
    first_sweeps(red2, black2, fd2_red, fd2_black, 2, slots2, odd2)
    for k in range(slots2):
        res2[x2 * k : x2 * (k + 1), :] = residual(red2, black2, fd2_red, 2, k, slots2, odd2)[0]
    col = lax.broadcasted_iota(jnp.int32, (128, 128), 1)
    res2[...] = matmul(res2[...], 0.125 * halving(128, 128, col % 64))
    n = slots2 * x2 // 2
    x3 = x2 // 2
    fd3[...] = res2[pl.ds(0, n, stride=2), :] + res2[pl.ds(1, n, stride=2), :]

    odd3 = odd_cells(x3, 128)
    fr, fb = [], []
    for k in range(2):
        r, b = pack(fd3[x3 * 2 * k : x3 * (2 * k + 1), :], fd3[x3 * (2 * k + 1) : x3 * (2 * k + 2), :], odd3)
        fr.append(scaled(r, 3, 0, k, 2, odd3))
        fb.append(scaled(b, 3, 1, k, 2, odd3))
    parity = (odd3, jnp.logical_not(odd3))
    fr, fb = shifted(fr, 3), shifted(fb, 2)
    b = relaxed_shifted(fr, fb, 2, 3, 1, parity)
    r = relaxed_shifted(b, fr, 1, 3, 0, parity)
    b = relaxed_shifted(r, fb, 0, 3, 1, parity)
    for _ in range(3):
        b = shifted(b[0], 4)
        for reach in (3, 1):
            r = relaxed_shifted(b, fr, reach, 3, 0, parity)
            b = relaxed_shifted(r, fb, reach - 1, 3, 1, parity)
    r, b = r[0], b[0]

    def layers(red, black, odd):
        return jnp.where(odd, black, red), jnp.where(odd, red, black)

    parts = []
    for k in range(2):
        parts += layers(r[k], b[k], odd3)
    e = matmul(jnp.concatenate(parts, axis=0), doubling(128, 128, col // 2))
    res2[pl.ds(0, n, stride=2), :] = e
    res2[pl.ds(1, n, stride=2), :] = e
    for k in range(slots2):
        put(black2, k, [get(black2, k)[0] + res2[x2 * k : x2 * (k + 1), :]])
    last_sweeps(red2, black2, fd2_red, fd2_black, 2, slots2, odd2)

    odd1 = odd_cells(32, 128)
    slots1 = 8
    sub = rows_of(8)
    for k in range(slots2):
        for i, v in enumerate(layers(get(red2, k)[0], get(black2, k)[0], odd2)):
            at = 16 * (2 * k + i)
            big1[at : at + 8, :] = v[0:8]
            big1[at + 8 : at + 16, :] = jnp.where(sub < 2, v[8:16] if nx > 2 else v[0:8], v[x2 - 8 : x2])
    e = matmul(big1[0 : 16 * slots1, :], doubling(128, 128, jnp.where(col < 96, col // 2, col // 2 + 64)))
    big1[pl.ds(0, 16 * slots1, stride=2), :] = e
    big1[pl.ds(1, 16 * slots1, stride=2), :] = e
    for k in range(slots1):
        put(black1, k, [black1_in[k] + big1[32 * k : 32 * (k + 1), :]])
    last_sweeps(red1, black1, fd1_red, fd1_black, 1, slots1, odd1)

    slots0 = NZ // 2
    for k in range(slots1):
        low, high = layers(get(red1, k)[0], get(black1, k)[0], odd1)
        for i, v in enumerate((low, high)):
            at = 16 * (2 * k + i)
            big1[at : at + 8, :] = v[0:8]
            big1[at + 8 : at + 16, :] = jnp.where(sub < 4, v[8:16], v[24:32])
    wide_col = lax.broadcasted_iota(jnp.int32, (128, 256), 1)
    e = matmul(big1[0 : 16 * slots0, :], doubling(128, 256, wide_col // 2))
    for t in range(2):
        part = e[:, 128 * t : 128 * t + 128]
        big0[t, pl.ds(0, 16 * slots0, stride=2), :] = part
        big0[t, pl.ds(1, 16 * slots0, stride=2), :] = part
    odd0 = odd_cells(32, 128)
    for k in range(slots0):
        put(black0, k, [black0_in[t, k] + big0[t, 32 * k : 32 * (k + 1), :] for t in range(2)])
    last_sweeps(red0, black0, fd0_red, fd0_black, 0, slots0, odd0)
    for k in range(slots0):
        pairs = [layers(r, b, odd0) for r, b in zip(get(red0, k), get(black0, k))]
        for i, dst in enumerate((red0, black0)):
            put(dst, k, [pair[i] for pair in pairs])

    depth = 8
    copies = []

    lane = lanes(BX)

    def at(z, t, shift=0):
        return (black0 if z % 2 else red0)[t, z // 2, 8 + shift : 24 + shift, :]

    for z in range(NZ):
        own = at(z, 0)
        pressure[BX * z : BX * (z + 1), :] = own
        zero = jnp.zeros_like(own)
        upper = at(z + 1, 0) if z < NZ - 1 else zero
        lower = at(z - 1, 0) if z > 0 else zero
        gx = at(z, 0, 1) - at(z, 0, -1)
        margin = at(z, 1)
        gy = turn(jnp.where(lane == 0, margin, own), -1, 1) - turn(jnp.where(lane == BY - 1, margin, own), 1, 1)
        fluid = (1 - obst[BX * z : BX * (z + 1), :]).astype(F32)
        for q, g in enumerate((gx, gy, upper - lower)):
            j = q * NZ + z
            v = pred[BX * j : BX * (j + 1), :]
            corrected[BX * j : BX * (j + 1), :] = fluid * (v - (0.5 * TIME_STEP) * g)
        if z % depth == depth - 1:
            c = z // depth
            for i in range(4):
                src, dst = (corrected, corrected_hbm) if i < 3 else (pressure, pressure_hbm)
                part = pl.ds(((i % 3) * NZ + c * depth) * BX, depth * BX)
                copies.append(pltpu.make_async_copy(src.at[part, :], dst.at[part, :], sems.at[c, i]))
                copies[-1].start()
    for copy in copies:
        copy.wait()


def both_ways(axis, to_low, to_high):
    n = lax.axis_size(axis)
    up = [(i, (i + 1) % n) for i in range(n)]
    down = [((i + 1) % n, i) for i in range(n)]
    return lax.ppermute(to_high, axis, up), lax.ppermute(to_low, axis, down)


def body(velocity, old_tendency, obstacle):
    nx = lax.axis_size("gx")
    vel = velocity.reshape(3 * NZ * BX, BY)
    old = old_tendency.reshape(3 * NZ * BX, BY)
    obst = obstacle.reshape(NZ * BX, BY)

    block = 3 * NZ * BX
    within = pl.BlockSpec(memory_space=pltpu.VMEM)
    anywhere = [pl.BlockSpec(memory_space=pltpu.HBM)] * 3
    pred, source, to_low, to_high = call(
        local_kernel,
        (vmem(block, BY), vmem(NZ * BX, BY), vmem(592, BY), vmem(592, BY)),
        tuple(pltpu.with_memory_space_constraint(a, pltpu.HBM) for a in (vel, old, obst)),
        [
            pltpu.VMEM((block, BY), F32),
            pltpu.VMEM((block, BY), F32),
            pltpu.VMEM((NZ * BX, BY), jnp.int32),
            pltpu.VMEM((NZ * BX, BY), F32),
            pltpu.SemaphoreType.DMA((CHUNKS, 7)),
        ],
        in_specs=anywhere,
        name="local",
    )
    from_low, from_high = both_ways("gx", to_low, to_high)
    wide, to_left, to_right, fix_rows = call(
        join_x_kernel,
        (vmem(NZ * WX, BY), vmem(784, BY), vmem(784, BY), vmem(6 * NZ, BY)),
        (source, to_low, to_high, from_low, from_high),
        name="join_x",
    )
    from_left, from_right = both_ways("gy", to_left, to_right)
    fd0_red, fd0_black, black0, sent, own1, up1, down1, fix_cols = call(
        fine_down_kernel,
        (
            vmem(2, 16, 32, BY),
            vmem(2, 16, 32, BY),
            vmem(2, 16, 32, BY),
            vmem(nx, 16, BY),
            vmem(256, BY),
            vmem(128, BY),
            vmem(128, BY),
            vmem(2, BX, BY),
        ),
        (wide, to_left, from_left, from_right),
        [(2, 16, WX, BY)] * 2
        + [(2, 16, WX + 16, BY)] * 2
        + [(512, 256), (512, BY)]
        + [(1, 8, 16, BY)] * 2
        + [(1, 8, 32, BY)] * 2
        + [(64, BY), (16, BY), pltpu.SemaphoreType.DMA((nx,))],
        out_specs=(within,) * 3 + (pl.BlockSpec(memory_space=pl.ANY),) + (within,) * 4,
        name="fine_down",
    )
    gathered = lax.all_to_all(sent, "gx", 0, 0)
    low1, high1 = both_ways("gx", down1, up1)
    fd1_red, fd1_black, black1 = call(
        middle_kernel,
        (vmem(1, 8, 32, BY), vmem(1, 8, 32, BY), vmem(8, 32, BY)),
        (own1, low1, high1),
        [(1, 8, 48, BY)] * 2,
        name="middle",
    )
    pred = call(predictor_kernel, vmem(block, BY), (pred, fix_rows, fix_cols), name="predictor")
    g_left, g_right = both_ways("gy", gathered, gathered)
    x2 = 4 * nx
    corrected, pressure = call(
        functools.partial(up_kernel, nx),
        (vmem(block, BY), vmem(NZ * BX, BY)),
        (gathered, g_left, g_right, fd1_red, fd1_black, black1, fd0_red, fd0_black, black0, pred, obst),
        [(1, 4, x2, BY)] * 2
        + [(1, 4, x2 + 16, BY)] * 2
        + [(4 * x2, BY), (2 * x2, BY)]
        + [(1, 8, 48, BY)] * 2
        + [(256, BY)]
        + [(2, 16, 48, BY)] * 2
        + [(2, 512, BY), (12, x2, BY), (block, BY), (NZ * BX, BY), pltpu.SemaphoreType.DMA((4, 4))],
        out_specs=(pl.BlockSpec(memory_space=pl.ANY),) * 2,
        name="up",
    )
    return corrected.reshape(3, NZ, BX, BY), pressure.reshape(NZ, BX, BY)


def solution(mesh):
    placed = (P(None, None, "gx", "gy"), P(None, None, "gx", "gy"), P(None, "gx", "gy"))
    return jax.shard_map(
        body,
        mesh=mesh,
        in_specs=placed,
        out_specs=(P(None, None, "gx", "gy"), P(None, "gx", "gy")),
        check_vma=False,
    )
```

```python
import functools

import jax
import jax.numpy as jnp
from jax import lax
from jax.experimental import pallas as pl
from jax.experimental.pallas import tpu as pltpu
from jax.sharding import PartitionSpec as P

TIME_STEP = 0.25
VISCOSITY = 0.1
WEIGHT_NEW = 15.0 / 16.0
WEIGHT_OLD = -25.0 / 48.0
HELMHOLTZ = 1.0e-4
SCALE = -0.5 / TIME_STEP
INTERPRET = False
F32 = jnp.float32
NZ = 32
BX = 16
BY = 128
WX = 40
CHUNKS = 8


def vmem(*shape):
    return jax.ShapeDtypeStruct(shape, F32)


def call(kernel, outs, args, scratch=(), in_specs=None, out_specs=None, name=None):
    everywhere = pl.BlockSpec(memory_space=pltpu.VMEM)
    return pl.pallas_call(
        kernel,
        out_shape=outs,
        out_specs=out_specs or jax.tree.map(lambda _: everywhere, outs),
        in_specs=in_specs or [everywhere] * len(args),
        scratch_shapes=[pltpu.VMEM(s, F32) if isinstance(s, tuple) else s for s in scratch],
        compiler_params=pltpu.CompilerParams(vmem_limit_bytes=16 << 20),
        interpret=INTERPRET,
        name=name,
    )(*args)


def turn(a, shift, axis):
    return pltpu.roll(a, shift % a.shape[axis], axis)


def lanes(rows, cols=128):
    return lax.broadcasted_iota(jnp.int32, (rows, cols), 1)


def rows_of(rows, cols=128):
    return lax.broadcasted_iota(jnp.int32, (rows, cols), 0)


def odd_cells(rows, cols):
    return (rows_of(rows, cols) + lanes(rows, cols)) % 2 == 1


def diag(level, m):
    return HELMHOLTZ + (4.0 + m) / float(4**level)


def at_end(colour, k, count, odd, inner, end):
    if k == 0:
        return jnp.where(odd, inner, end) if colour == 0 else jnp.where(odd, end, inner)
    if k == count - 1:
        return jnp.where(odd, end, inner) if colour == 0 else jnp.where(odd, inner, end)
    return inner


def pack(low, high, odd):
    return jnp.where(odd, high, low), jnp.where(odd, low, high)


def scaled(value, level, colour, k, count, odd):
    return value * at_end(colour, k, count, odd, 1.0 / diag(level, 2), 1.0 / diag(level, 1))


def put(dst, k, tiles):
    n = tiles[0].shape[0]
    for t, v in enumerate(tiles):
        dst[t, k, 8 : 8 + n, :] = v
        dst[t, k, 7:8, :] = v[n - 1 : n]
        dst[t, k, 8 + n : 9 + n, :] = v[0:1]


def get(src, k, shift=0):
    tiles, _, rows, _ = src.shape
    return [src[t, k, 8 + shift : rows - 8 + shift, :] for t in range(tiles)]


def beside(tiles):
    if len(tiles) == 1:
        return [turn(tiles[0], 1, 1) + turn(tiles[0], -1, 1)]
    lane = lanes(tiles[0].shape[0])
    out = []
    for own, other in (tiles, tiles[::-1]):
        last = jnp.where(lane == BY - 1, other, own)
        first = jnp.where(lane == 0, other, own)
        out.append(turn(last, 1, 1) + turn(first, -1, 1))
    return out


def vertical(above, below, colour, odd):
    return jnp.where(odd, above, below) if colour == 0 else jnp.where(odd, below, above)


def weight_of(level, colour, k, count, odd):
    s = float(4**level)
    return at_end(colour, k, count, odd, 1.0 / s / diag(level, 2), 1.0 / s / diag(level, 1))


def relaxed(src, fd, level, colour, k, count, odd):
    b = get(src, k)
    zero = [jnp.zeros_like(v) for v in b]
    above = get(src, k + 1) if k < count - 1 else zero
    below = get(src, k - 1) if k > 0 else zero
    c = weight_of(level, colour, k, count, odd)
    out = []
    for t, (y, low, high) in enumerate(zip(beside(b), get(src, k, -1), get(src, k, 1))):
        z = vertical(above[t], below[t], colour, odd)
        out.append(fd[t, k] + c * ((y + (low + high)) + (b[t] + z)))
    return out


def half_sweep(dst, src, fd, level, colour, count, odd):
    for k in range(count):
        put(dst, k, relaxed(src, fd, level, colour, k, count, odd))


def first_sweeps(red, black, fd_red, fd_black, level, count, odd):
    for k in range(count):
        put(red, k, [fd_red[t, k] for t in range(red.shape[0])])
    half_sweep(black, red, fd_black, level, 1, count, odd)
    half_sweep(red, black, fd_red, level, 0, count, odd)
    half_sweep(black, red, fd_black, level, 1, count, odd)


def last_sweeps(red, black, fd_red, fd_black, level, count, odd):
    for _ in range(2):
        half_sweep(red, black, fd_red, level, 0, count, odd)
        half_sweep(black, red, fd_black, level, 1, count, odd)


def residual(red, black, fd, level, k, count, odd):
    d = at_end(0, k, count, odd, diag(level, 2), diag(level, 1))
    return [d * (new - old) for new, old in zip(relaxed(black, fd, level, 0, k, count, odd), get(red, k))]


def shifted(slots, reach):
    return {s: [turn(v, s, 1) if s else v for v in slots] for s in range(-reach, reach + 1)}


def relaxed_shifted(src, fd, reach, level, colour, parity):
    out = {}
    for s in range(-reach, reach + 1):
        odd = parity[s % 2]
        slots = src[s]
        count = len(slots)
        new = []
        for k in range(count):
            b = slots[k]
            zero = jnp.zeros_like(b)
            z = vertical(slots[k + 1] if k < count - 1 else zero, slots[k - 1] if k > 0 else zero, colour, odd)
            y = src[s - 1][k] + src[s + 1][k]
            x = turn(b, 1, 0) + turn(b, -1, 0)
            new.append(fd[s][k] + weight_of(level, colour, k, count, odd) * ((y + x) + (b + z)))
        out[s] = new
    return out


def halving(n, m, target):
    i = lax.broadcasted_iota(jnp.int32, (n, m), 0)
    return (i // 2 == target).astype(F32)


def doubling(n, m, target):
    i = lax.broadcasted_iota(jnp.int32, (n, m), 0)
    return (i == target).astype(F32)


def matmul(a, b):
    return jnp.dot(a, b, precision=lax.Precision.HIGHEST, preferred_element_type=F32)


def local_kernel(vel_hbm, old_hbm, obst_hbm, pred, source, to_low, to_high, vel, old, obst, edge_x, sems):
    lane = lanes(BX)
    row = rows_of(BX)
    depth = NZ // CHUNKS
    copies = []
    for c in range(CHUNKS):
        group = []
        for i, (src, dst, q) in enumerate(
            [(vel_hbm, vel, q) for q in range(3)] + [(old_hbm, old, q) for q in range(3)] + [(obst_hbm, obst, 0)]
        ):
            at = pl.ds((q * NZ + c * depth) * BX, depth * BX)
            group.append(pltpu.make_async_copy(src.at[at, :], dst.at[at, :], sems.at[c, i]))
        copies.append(group)
    for group in copies[:3]:
        for copy in group:
            copy.start()

    def cut(ref, j):
        return ref[BX * j : BX * (j + 1), :]

    packs = [jnp.zeros((BX, BY), F32) for _ in range(3)]

    def put_pair(pack, value, at):
        return jnp.where((lane == at) | (lane == at + 1), turn(value, at + 1, 1), pack)

    for copy in copies[0]:
        copy.wait()
    for z in range(NZ):
        if z % depth == depth - 1 and z < NZ - 1:
            for copy in copies[z // depth + 1]:
                copy.wait()
            for copy in copies[z // depth + 3] if z // depth + 3 < CHUNKS else ():
                copy.start()
        fluid = (1 - cut(obst, z)).astype(F32)
        now = [cut(vel, q * NZ + z) for q in range(3)]
        spread = (TIME_STEP * WEIGHT_NEW * VISCOSITY) * fluid
        carry = (TIME_STEP * WEIGHT_NEW * 0.5) * fluid
        flow = [carry * v for v in now]
        plus = [spread - v for v in flow]
        minus = [spread + v for v in flow]
        across_x = jnp.where(row == 0, minus[0], jnp.where(row == BX - 1, plus[0], 0.0))
        across_y = jnp.where(lane == 0, minus[1], plus[1])
        plus_x = jnp.where(row == BX - 1, 0.0, plus[0])
        minus_x = jnp.where(row == 0, 0.0, minus[0])
        plus_y = jnp.where(lane == BY - 1, 0.0, plus[1])
        minus_y = jnp.where(lane == 0, 0.0, minus[1])
        keep = (1.0 - 6.0 * TIME_STEP * WEIGHT_NEW * VISCOSITY) * fluid
        past = (TIME_STEP * WEIGHT_OLD) * fluid
        for q in range(3):
            j = q * NZ + z
            v = now[q]
            p = keep * v + past * cut(old, j)
            p = p + (plus_x * turn(v, -1, 0) + minus_x * turn(v, 1, 0))
            p = p + (plus_y * turn(v, -1, 1) + minus_y * turn(v, 1, 1))
            if z < NZ - 1:
                p = p + plus[2] * cut(vel, j + 1)
            if z > 0:
                p = p + minus[2] * cut(vel, j - 1)
            pred[BX * j : BX * (j + 1), :] = p
            if q == 1:
                pv = p
        edge_x[BX * z : BX * (z + 1), :] = across_x
        for t, pair in enumerate(((now[0], now[1]), (now[2], across_y), (pv, across_x))):
            for i in range(2):
                packs[t] = put_pair(packs[t], pair[i], 64 * i + 2 * z)
    for z in range(NZ):
        u = cut(pred, z)
        v = cut(pred, NZ + z)
        zero = jnp.zeros_like(u)
        upper = cut(pred, 2 * NZ + z + 1) if z < NZ - 1 else zero
        lower = cut(pred, 2 * NZ + z - 1) if z > 0 else zero
        east = jnp.where(row == BX - 1, 0.0, turn(u, -1, 0))
        west = jnp.where(row == 0, 0.0, turn(u, 1, 0))
        north = jnp.where(lane == BY - 1, 0.0, turn(v, -1, 1))
        south = jnp.where(lane == 0, 0.0, turn(v, 1, 1))
        s = SCALE * ((east - west) + (north - south) + (upper - lower))
        source[BX * z : BX * (z + 1), :] = s
        to_low[8 * z : 8 * z + 8, :] = s[:8]
        to_high[8 * z : 8 * z + 8, :] = s[8:]
    half = NZ // 2
    sub = rows_of(8)
    for h in range(half):
        at = 8 * (NZ + h)
        a = source[BX * h : BX * (h + 1), :]
        b = source[BX * (h + half) : BX * (h + half + 1), :]
        to_low[at : at + 8, :] = jnp.where(sub < 4, a[8:], turn(b[8:], 4, 0))
        to_high[at : at + 8, :] = jnp.where(sub < 4, turn(b[:8], 4, 0), a[:8])
    for ref, r in ((to_low, 0), (to_high, BX - 1)):
        at = 12 * NZ
        ref[at : at + NZ, :] = edge_x[pl.ds(r, NZ, stride=BX), :]
        ref[at + NZ : at + 4 * NZ, :] = vel[pl.ds(r, 3 * NZ, stride=BX), :]
        ref[at + 4 * NZ : at + 5 * NZ, :] = pred[pl.ds(r, NZ, stride=BX), :]
        for t in range(3):
            ref[at + 5 * NZ + BX * t : at + 5 * NZ + BX * (t + 1), :] = packs[t]


def join_x_kernel(source, to_low, to_high, from_low, from_high, wide, to_left, to_right, fix_rows):
    lane = lanes(NZ)
    layer = rows_of(NZ)
    sub = rows_of(8)
    half = NZ // 2

    def line(ref, i):
        at = 12 * NZ + NZ * i
        return ref[at : at + NZ, :]

    def slope_y(f):
        return jnp.where(lane == BY - 1, 0.0, turn(f, -1, 1)) - jnp.where(lane == 0, 0.0, turn(f, 1, 1))

    def slope_z(f):
        return jnp.where(layer == NZ - 1, 0.0, turn(f, -1, 0)) - jnp.where(layer == 0, 0.0, turn(f, 1, 0))

    for z in range(NZ):
        w = WX * z
        wide[w : w + 16, :] = source[BX * z : BX * (z + 1), :]
        wide[w + 16 : w + 24, :] = from_high[8 * z : 8 * z + 8, :]
        at = 8 * (NZ + z % half)
        high = from_high[at : at + 8, :]
        low = from_low[at : at + 8, :]
        if z < half:
            wide[w + 24 : w + 32, :] = jnp.where(sub < 4, high, low)
        else:
            wide[w + 24 : w + 32, :] = turn(jnp.where(sub < 4, low, high), 4, 0)
        wide[w + 32 : w + 40, :] = from_low[8 * z : 8 * z + 8, :]

    def add(row, value):
        at = pl.ds(row % WX, NZ, stride=WX)
        wide[at, :] = wide[at, :] + SCALE * value

    for near, far, row, step, sign in ((to_low, from_low, 0, -1, 1.0), (to_high, from_high, 15, 1, -1.0)):
        inner = [line(near, 0) * line(far, 1 + q) for q in range(3)]
        outer = [line(far, 0) * line(near, 1 + q) for q in range(3)]
        add(row - step, -sign * inner[0])
        add(row, -sign * (line(far, 4) + outer[0]) + slope_y(inner[1]) + slope_z(inner[2]))
        add(row + step, sign * (line(near, 4) + inner[0]) + slope_y(outer[1]) + slope_z(outer[2]))
        add(row + 2 * step, sign * outer[0])
        for q in range(3):
            at = NZ * (3 * (step > 0) + q)
            fix_rows[at : at + NZ, :] = inner[q]

    stack = []
    for t in range(3):
        at = 17 * NZ + BX * t
        stack.append(jnp.concatenate([ref[at : at + BX, :] for ref in (to_low, from_high, from_low)], axis=0))
    first = rows_of(48) % BX == 0
    other = jnp.where(first, turn(stack[0], 1, 0), turn(stack[0], -1, 0))
    stack[2] = stack[2] + turn(stack[2] * other, 64, 1)
    lane = lanes(WX)
    for h in range(half):
        a = wide[WX * h : WX * (h + 1), :]
        b = turn(wide[WX * (h + half) : WX * (h + half + 1), :], 64, 1)
        to_left[WX * h : WX * (h + 1), :] = jnp.where(lane < 64, a, b)
        to_right[WX * h : WX * (h + 1), :] = jnp.where(lane < 64, b, a)
    for t in range(3):
        at = WX * half + 48 * t
        to_left[at : at + 48, :] = stack[t]
        to_right[at : at + 48, :] = stack[t]


def trimmed(a):
    return jnp.concatenate([a[0:24], a[32:40]], axis=0)


def fine_down_kernel(
    wide, sent_left, from_left, from_right,
    fd0_red, fd0_black, black0, sent, own1, up1, down1, fix_cols,
    fd_red, fd_black, red, black, res, thin, fd1_red, fd1_black, red1, black1, res1,
):
    lane = lanes(WX)
    odd = odd_cells(WX, 128)
    half = NZ // 2
    slots = NZ // 2

    lane48 = lanes(48)
    even = lane48 % 2 == 0
    low_half = lane48 < 64

    def pack_of(ref, t):
        at = WX * half + 48 * t
        return ref[at : at + 48, :]

    def swap(f):
        return turn(f, 64, 1)

    def both(f):
        return jnp.where(low_half, swap(f), f)

    def facing(left, right):
        return jnp.where(even, turn(right, -1, 1), turn(left, 1, 1))

    def slope_x(f):
        return turn(f, -1, 0) - turn(f, 1, 0)

    def slope_z(f):
        above = jnp.where(lane48 >= 2 * NZ - 2, 0.0, turn(f, -2, 1))
        below = jnp.where(lane48 < 2, 0.0, turn(f, 2, 1))
        return above - below

    def signed(f):
        return jnp.where(even, f, -f)

    own = [pack_of(sent_left, t) for t in range(3)]
    left = [pack_of(from_left, t) for t in range(3)]
    right = [pack_of(from_right, t) for t in range(3)]
    near = both(own[1])
    inner_uv = near * facing(left[0], right[0])
    inner_w = near * facing(left[1], right[1])
    far = both(jnp.where(even, left[1], right[1]))
    outer_uv = far * facing(own[0], own[0])
    outer_w = far * facing(own[1], own[1])
    inner_v = swap(inner_uv)
    outer_v = swap(outer_uv)
    pv_far = jnp.where(even, left[2], right[2]) + outer_v
    pv_own = own[2] + inner_v
    e0 = signed(facing(pv_far, pv_far)) + slope_x(inner_uv) + slope_z(inner_w)
    e1 = signed(facing(pv_own, pv_own)) + slope_x(outer_uv) + slope_z(outer_w)
    i = lax.broadcasted_iota(jnp.int32, (128, 128), 0)
    j = lax.broadcasted_iota(jnp.int32, (128, 128), 1)
    side = i % 2
    to = 4 * ((i % 64) // 2) + jnp.where(i < 64, 1 + side, 3 * side)
    order = SCALE * (to == j).astype(F32)
    mixed = []
    for e, v in ((e0, inner_v), (e1, outer_v)):
        m = jnp.where(low_half, e, swap(signed(v)))
        m = jnp.concatenate([m[0:24], jnp.where(rows_of(8) < 4, m[24:32], m[32:40]), m[40:48]], axis=0)
        mixed.append(matmul(m, order))
    edge = (lane < 2) | (lane >= BY - 2)

    def layer(z):
        t0 = wide[WX * z : WX * (z + 1), :]
        h = z % half
        a = from_right[WX * h : WX * (h + 1), :]
        b = from_left[WX * h : WX * (h + 1), :]
        if z < half:
            t1 = jnp.where(lane < 64, a, b)
        else:
            t1 = turn(jnp.where(lane < 64, b, a), 64, 1)
        t0 = t0 + jnp.where(edge, turn(mixed[0], 126 - 4 * z, 1), 0.0)
        t1 = t1 + jnp.where(edge, turn(mixed[1], 126 - 4 * z, 1), 0.0)
        return t0, t1

    for k in range(slots):
        for t, (low, high) in enumerate(zip(layer(2 * k), layer(2 * k + 1))):
            r, b = pack(low, high, odd)
            r = scaled(r, 0, 0, k, slots, odd)
            b = scaled(b, 0, 1, k, slots, odd)
            fd_red[t, k] = r
            fd_black[t, k] = b
            fd0_red[t, k] = trimmed(r)
            fd0_black[t, k] = trimmed(b)
    first_sweeps(red, black, fd_red, fd_black, 0, slots, odd)
    for k in range(slots):
        for t, r in enumerate(residual(red, black, fd_red, 0, k, slots, odd)):
            res[32 * k : 32 * (k + 1), 128 * t : 128 * t + 128] = trimmed(r)
    matrix = 0.125 * halving(256, 128, lax.broadcasted_iota(jnp.int32, (256, 128), 1))
    thin[...] = matmul(res[...], matrix)
    n = BX * slots
    own1[...] = thin[pl.ds(0, n, stride=2), :] + thin[pl.ds(1, n, stride=2), :]

    odd1 = odd_cells(16, 128)
    slots1 = slots // 2
    sub = rows_of(8)

    def plane(z):
        return own1[16 * z : 16 * (z + 1), :]

    for k in range(slots1):
        r, b = pack(plane(2 * k), plane(2 * k + 1), odd1)
        fd1_red[0, k] = scaled(r, 1, 0, k, slots1, odd1)
        fd1_black[0, k] = scaled(b, 1, 1, k, slots1, odd1)
    first_sweeps(red1, black1, fd1_red, fd1_black, 1, slots1, odd1)
    for k in range(slots1):
        res1[8 * k : 8 * k + 8, :] = residual(red1, black1, fd1_red, 1, k, slots1, odd1)[0][:8]
    res1[...] = matmul(res1[...], 0.125 * halving(128, 128, j % 64))
    v = res1[pl.ds(0, 32, stride=2), :] + res1[pl.ds(1, 32, stride=2), :]
    sent[...] = jnp.where(lanes(16) < 64, v[:16], v[16:])
    for k in range(slots):
        for t, v in enumerate(get(black, k)):
            black0[t, k] = trimmed(v)
    for z in range(slots):
        a, b = plane(z)[:8], plane(z)[8:]
        up1[8 * z : 8 * z + 8, :] = jnp.where(sub < 4, a, b)
        down1[8 * z : 8 * z + 8, :] = jnp.where(sub < 4, b, a)
    fix_cols[0] = inner_uv[0:16]
    fix_cols[1] = inner_w[0:16]


def predictor_kernel(pred, fix_rows, fix_cols, done):
    lane = lanes(BX)
    row = rows_of(BX)
    edge = (lane == 0) | (lane == BY - 1)
    for j in range(3 * NZ):
        q, z = divmod(j, NZ)
        low = jnp.broadcast_to(fix_rows[j : j + 1, :], (BX, BY))
        high = jnp.broadcast_to(fix_rows[3 * NZ + j : 3 * NZ + j + 1, :], (BX, BY))
        rim = jnp.where(row == 0, low, jnp.where(row == BX - 1, high, 0.0))
        column = turn(fix_cols[q // 2], -(64 * (q % 2) + 2 * z + 1), 1)
        rim = rim + jnp.where(edge, column, 0.0)
        done[BX * j : BX * (j + 1), :] = pred[BX * j : BX * (j + 1), :] + rim


def middle_kernel(own1, from_low, from_high, fd_red, fd_black, done, red, black):
    slots = 8
    odd = odd_cells(32, 128)
    sub = rows_of(8)

    def plane(z):
        a = own1[16 * z : 16 * z + 8, :]
        b = own1[16 * z + 8 : 16 * z + 16, :]
        low = from_low[8 * z : 8 * z + 8, :]
        high = from_high[8 * z : 8 * z + 8, :]
        tiles = [a] + [jnp.where(sub < 4, p, q) for p, q in ((b, high), (high, low), (low, b))]
        return jnp.concatenate(tiles, axis=0)

    for k in range(slots):
        r, b = pack(plane(2 * k), plane(2 * k + 1), odd)
        fd_red[0, k] = scaled(r, 1, 0, k, slots, odd)
        fd_black[0, k] = scaled(b, 1, 1, k, slots, odd)
    first_sweeps(red, black, fd_red, fd_black, 1, slots, odd)
    for k in range(slots):
        done[k] = get(black, k)[0]


def up_kernel(
    nx, g_own, g_left, g_right, fd1_red, fd1_black, black1_in, fd0_red, fd0_black, black0_in, pred, obst,
    corrected_hbm, pressure_hbm, fd2_red, fd2_black, red2, black2, res2, fd3, red1, black1, big1, red0, black0, big0, ring, corrected, pressure, sems,
):
    x2 = 4 * nx
    lane = lanes(x2)
    odd2 = odd_cells(x2, 128)
    slots2 = 4

    for i, g in enumerate((g_own, g_right, g_left)):
        for j in range(nx):
            d = lax.rem(lax.axis_index("gx") + j, nx)
            for z in range(4):
                ring[4 * i + z, 4 * j : 4 * j + 4, :] = g[d, 4 * z : 4 * z + 4, :]

    def rhs2(z):
        lift = 64 * (z // 4)
        own, right, left = (ring[4 * i + z % 4] for i in range(3))
        own = turn(own, -lift, 1) if lift else own
        right = turn(right, 32 - lift, 1)
        left = jnp.where(lane < 96, turn(left, 32 - lift, 1), turn(left, 96 - lift, 1))
        return jnp.where(lane < 32, own, jnp.where(lane < 80, right, left))

    for k in range(slots2):
        r, b = pack(rhs2(2 * k), rhs2(2 * k + 1), odd2)
        fd2_red[0, k] = scaled(r, 2, 0, k, slots2, odd2)
        fd2_black[0, k] = scaled(b, 2, 1, k, slots2, odd2)
    first_sweeps(red2, black2, fd2_red, fd2_black, 2, slots2, odd2)
    for k in range(slots2):
        res2[x2 * k : x2 * (k + 1), :] = residual(red2, black2, fd2_red, 2, k, slots2, odd2)[0]
    col = lax.broadcasted_iota(jnp.int32, (128, 128), 1)
    res2[...] = matmul(res2[...], 0.125 * halving(128, 128, col % 64))
    n = slots2 * x2 // 2
    x3 = x2 // 2
    fd3[...] = res2[pl.ds(0, n, stride=2), :] + res2[pl.ds(1, n, stride=2), :]

    odd3 = odd_cells(x3, 128)
    fr, fb = [], []
    for k in range(2):
        r, b = pack(fd3[x3 * 2 * k : x3 * (2 * k + 1), :], fd3[x3 * (2 * k + 1) : x3 * (2 * k + 2), :], odd3)
        fr.append(scaled(r, 3, 0, k, 2, odd3))
        fb.append(scaled(b, 3, 1, k, 2, odd3))
    parity = (odd3, jnp.logical_not(odd3))
    fr, fb = shifted(fr, 3), shifted(fb, 2)
    b = relaxed_shifted(fr, fb, 2, 3, 1, parity)
    r = relaxed_shifted(b, fr, 1, 3, 0, parity)
    b = relaxed_shifted(r, fb, 0, 3, 1, parity)
    for _ in range(3):
        b = shifted(b[0], 4)
        for reach in (3, 1):
            r = relaxed_shifted(b, fr, reach, 3, 0, parity)
            b = relaxed_shifted(r, fb, reach - 1, 3, 1, parity)
    r, b = r[0], b[0]

    def layers(red, black, odd):
        return jnp.where(odd, black, red), jnp.where(odd, red, black)

    parts = []
    for k in range(2):
        parts += layers(r[k], b[k], odd3)
    e = matmul(jnp.concatenate(parts, axis=0), doubling(128, 128, col // 2))
    res2[pl.ds(0, n, stride=2), :] = e
    res2[pl.ds(1, n, stride=2), :] = e
    for k in range(slots2):
        put(black2, k, [get(black2, k)[0] + res2[x2 * k : x2 * (k + 1), :]])
    last_sweeps(red2, black2, fd2_red, fd2_black, 2, slots2, odd2)

    odd1 = odd_cells(32, 128)
    slots1 = 8
    sub = rows_of(8)
    for k in range(slots2):
        for i, v in enumerate(layers(get(red2, k)[0], get(black2, k)[0], odd2)):
            at = 16 * (2 * k + i)
            big1[at : at + 8, :] = v[0:8]
            big1[at + 8 : at + 16, :] = jnp.where(sub < 2, v[8:16] if nx > 2 else v[0:8], v[x2 - 8 : x2])
    e = matmul(big1[0 : 16 * slots1, :], doubling(128, 128, jnp.where(col < 96, col // 2, col // 2 + 64)))
    big1[pl.ds(0, 16 * slots1, stride=2), :] = e
    big1[pl.ds(1, 16 * slots1, stride=2), :] = e
    for k in range(slots1):
        put(black1, k, [black1_in[k] + big1[32 * k : 32 * (k + 1), :]])
    last_sweeps(red1, black1, fd1_red, fd1_black, 1, slots1, odd1)

    slots0 = NZ // 2
    for k in range(slots1):
        low, high = layers(get(red1, k)[0], get(black1, k)[0], odd1)
        for i, v in enumerate((low, high)):
            at = 16 * (2 * k + i)
            big1[at : at + 8, :] = v[0:8]
            big1[at + 8 : at + 16, :] = jnp.where(sub < 4, v[8:16], v[24:32])
    wide_col = lax.broadcasted_iota(jnp.int32, (128, 256), 1)
    e = matmul(big1[0 : 16 * slots0, :], doubling(128, 256, wide_col // 2))
    for t in range(2):
        part = e[:, 128 * t : 128 * t + 128]
        big0[t, pl.ds(0, 16 * slots0, stride=2), :] = part
        big0[t, pl.ds(1, 16 * slots0, stride=2), :] = part
    odd0 = odd_cells(32, 128)
    for k in range(slots0):
        put(black0, k, [black0_in[t, k] + big0[t, 32 * k : 32 * (k + 1), :] for t in range(2)])
    last_sweeps(red0, black0, fd0_red, fd0_black, 0, slots0, odd0)
    for k in range(slots0):
        pairs = [layers(r, b, odd0) for r, b in zip(get(red0, k), get(black0, k))]
        for i, dst in enumerate((red0, black0)):
            put(dst, k, [pair[i] for pair in pairs])

    depth = 8
    copies = []

    lane = lanes(BX)

    def at(z, t, shift=0):
        return (black0 if z % 2 else red0)[t, z // 2, 8 + shift : 24 + shift, :]

    for z in range(NZ):
        own = at(z, 0)
        pressure[BX * z : BX * (z + 1), :] = own
        zero = jnp.zeros_like(own)
        upper = at(z + 1, 0) if z < NZ - 1 else zero
        lower = at(z - 1, 0) if z > 0 else zero
        gx = at(z, 0, 1) - at(z, 0, -1)
        margin = at(z, 1)
        gy = turn(jnp.where(lane == 0, margin, own), -1, 1) - turn(jnp.where(lane == BY - 1, margin, own), 1, 1)
        fluid = (1 - obst[BX * z : BX * (z + 1), :]).astype(F32)
        for q, g in enumerate((gx, gy, upper - lower)):
            j = q * NZ + z
            v = pred[BX * j : BX * (j + 1), :]
            corrected[BX * j : BX * (j + 1), :] = fluid * (v - (0.5 * TIME_STEP) * g)
        if z % depth == depth - 1:
            c = z // depth
            for i in range(4):
                src, dst = (corrected, corrected_hbm) if i < 3 else (pressure, pressure_hbm)
                part = pl.ds(((i % 3) * NZ + c * depth) * BX, depth * BX)
                copies.append(pltpu.make_async_copy(src.at[part, :], dst.at[part, :], sems.at[c, i]))
                copies[-1].start()
    for copy in copies:
        copy.wait()


def both_ways(axis, to_low, to_high):
    n = lax.axis_size(axis)
    up = [(i, (i + 1) % n) for i in range(n)]
    down = [((i + 1) % n, i) for i in range(n)]
    return lax.ppermute(to_high, axis, up), lax.ppermute(to_low, axis, down)


def body(velocity, old_tendency, obstacle):
    nx = lax.axis_size("gx")
    vel = velocity.reshape(3 * NZ * BX, BY)
    old = old_tendency.reshape(3 * NZ * BX, BY)
    obst = obstacle.reshape(NZ * BX, BY)

    block = 3 * NZ * BX
    anywhere = [pl.BlockSpec(memory_space=pltpu.HBM)] * 3
    pred, source, to_low, to_high = call(
        local_kernel,
        (vmem(block, BY), vmem(NZ * BX, BY), vmem(592, BY), vmem(592, BY)),
        tuple(pltpu.with_memory_space_constraint(a, pltpu.HBM) for a in (vel, old, obst)),
        [
            pltpu.VMEM((block, BY), F32),
            pltpu.VMEM((block, BY), F32),
            pltpu.VMEM((NZ * BX, BY), jnp.int32),
            pltpu.VMEM((NZ * BX, BY), F32),
            pltpu.SemaphoreType.DMA((CHUNKS, 7)),
        ],
        in_specs=anywhere,
        name="local",
    )
    from_low, from_high = both_ways("gx", to_low, to_high)
    wide, to_left, to_right, fix_rows = call(
        join_x_kernel,
        (vmem(NZ * WX, BY), vmem(784, BY), vmem(784, BY), vmem(6 * NZ, BY)),
        (source, to_low, to_high, from_low, from_high),
        name="join_x",
    )
    from_left, from_right = both_ways("gy", to_left, to_right)
    fd0_red, fd0_black, black0, sent, own1, up1, down1, fix_cols = call(
        fine_down_kernel,
        (
            vmem(2, 16, 32, BY),
            vmem(2, 16, 32, BY),
            vmem(2, 16, 32, BY),
            vmem(16, BY),
            vmem(256, BY),
            vmem(128, BY),
            vmem(128, BY),
            vmem(2, BX, BY),
        ),
        (wide, to_left, from_left, from_right),
        [(2, 16, WX, BY)] * 2
        + [(2, 16, WX + 16, BY)] * 2
        + [(512, 256), (512, BY)]
        + [(1, 8, 16, BY)] * 2
        + [(1, 8, 32, BY)] * 2
        + [(64, BY)],
        name="fine_down",
    )
    gathered = lax.all_to_all(jnp.broadcast_to(sent, (nx, 16, BY)), "gx", 0, 0)
    low1, high1 = both_ways("gx", down1, up1)
    fd1_red, fd1_black, black1 = call(
        middle_kernel,
        (vmem(1, 8, 32, BY), vmem(1, 8, 32, BY), vmem(8, 32, BY)),
        (own1, low1, high1),
        [(1, 8, 48, BY)] * 2,
        name="middle",
    )
    pred = call(predictor_kernel, vmem(block, BY), (pred, fix_rows, fix_cols), name="predictor")
    g_left, g_right = both_ways("gy", gathered, gathered)
    x2 = 4 * nx
    corrected, pressure = call(
        functools.partial(up_kernel, nx),
        (vmem(block, BY), vmem(NZ * BX, BY)),
        (gathered, g_left, g_right, fd1_red, fd1_black, black1, fd0_red, fd0_black, black0, pred, obst),
        [(1, 4, x2, BY)] * 2
        + [(1, 4, x2 + 16, BY)] * 2
        + [(4 * x2, BY), (2 * x2, BY)]
        + [(1, 8, 48, BY)] * 2
        + [(256, BY)]
        + [(2, 16, 48, BY)] * 2
        + [(2, 512, BY), (12, x2, BY), (block, BY), (NZ * BX, BY), pltpu.SemaphoreType.DMA((4, 4))],
        out_specs=(pl.BlockSpec(memory_space=pl.ANY),) * 2,
        name="up",
    )
    return corrected.reshape(3, NZ, BX, BY), pressure.reshape(NZ, BX, BY)


def solution(mesh):
    placed = (P(None, None, "gx", "gy"), P(None, None, "gx", "gy"), P(None, "gx", "gy"))
    return jax.shard_map(
        body,
        mesh=mesh,
        in_specs=placed,
        out_specs=(P(None, None, "gx", "gy"), P(None, "gx", "gy")),
        check_vma=False,
    )
```

```python
import functools

import jax
import jax.numpy as jnp
from jax import lax
from jax.experimental import pallas as pl
from jax.experimental.pallas import tpu as pltpu
from jax.sharding import PartitionSpec as P

TIME_STEP = 0.25
VISCOSITY = 0.1
WEIGHT_NEW = 15.0 / 16.0
WEIGHT_OLD = -25.0 / 48.0
HELMHOLTZ = 1.0e-4
SCALE = -0.5 / TIME_STEP
INTERPRET = False
F32 = jnp.float32
NZ = 32
BX = 16
BY = 128
WX = 40
CHUNKS = 8


def vmem(*shape):
    return jax.ShapeDtypeStruct(shape, F32)


def call(kernel, outs, args, scratch=(), in_specs=None, out_specs=None, flags=None, name=None):
    everywhere = pl.BlockSpec(memory_space=pltpu.VMEM)
    return pl.pallas_call(
        kernel,
        out_shape=outs,
        out_specs=out_specs or jax.tree.map(lambda _: everywhere, outs),
        in_specs=in_specs or [everywhere] * len(args),
        scratch_shapes=[pltpu.VMEM(s, F32) if isinstance(s, tuple) else s for s in scratch],
        compiler_params=pltpu.CompilerParams(vmem_limit_bytes=16 << 20, flags=flags),
        interpret=INTERPRET,
        name=name,
    )(*args)


def turn(a, shift, axis):
    return pltpu.roll(a, shift % a.shape[axis], axis)


def lanes(rows, cols=128):
    return lax.broadcasted_iota(jnp.int32, (rows, cols), 1)


def rows_of(rows, cols=128):
    return lax.broadcasted_iota(jnp.int32, (rows, cols), 0)


def odd_cells(rows, cols):
    return (rows_of(rows, cols) + lanes(rows, cols)) % 2 == 1


def diag(level, m):
    return HELMHOLTZ + (4.0 + m) / float(4**level)


def at_end(colour, k, count, odd, inner, end):
    if k == 0:
        return jnp.where(odd, inner, end) if colour == 0 else jnp.where(odd, end, inner)
    if k == count - 1:
        return jnp.where(odd, end, inner) if colour == 0 else jnp.where(odd, inner, end)
    return inner


def pack(low, high, odd):
    return jnp.where(odd, high, low), jnp.where(odd, low, high)


def scaled(value, level, colour, k, count, odd):
    return value * at_end(colour, k, count, odd, 1.0 / diag(level, 2), 1.0 / diag(level, 1))


def put(dst, k, tiles):
    n = tiles[0].shape[0]
    for t, v in enumerate(tiles):
        dst[t, k, 8 : 8 + n, :] = v
        dst[t, k, 7:8, :] = v[n - 1 : n]
        dst[t, k, 8 + n : 9 + n, :] = v[0:1]


def get(src, k, shift=0):
    tiles, _, rows, _ = src.shape
    return [src[t, k, 8 + shift : rows - 8 + shift, :] for t in range(tiles)]


def beside(tiles):
    if len(tiles) == 1:
        return [turn(tiles[0], 1, 1) + turn(tiles[0], -1, 1)]
    lane = lanes(tiles[0].shape[0])
    out = []
    for own, other in (tiles, tiles[::-1]):
        last = jnp.where(lane == BY - 1, other, own)
        first = jnp.where(lane == 0, other, own)
        out.append(turn(last, 1, 1) + turn(first, -1, 1))
    return out


def vertical(above, below, colour, odd):
    return jnp.where(odd, above, below) if colour == 0 else jnp.where(odd, below, above)


def weight_of(level, colour, k, count, odd):
    s = float(4**level)
    return at_end(colour, k, count, odd, 1.0 / s / diag(level, 2), 1.0 / s / diag(level, 1))


def relaxed(src, fd, level, colour, k, count, odd):
    b = get(src, k)
    zero = [jnp.zeros_like(v) for v in b]
    above = get(src, k + 1) if k < count - 1 else zero
    below = get(src, k - 1) if k > 0 else zero
    c = weight_of(level, colour, k, count, odd)
    out = []
    for t, (y, low, high) in enumerate(zip(beside(b), get(src, k, -1), get(src, k, 1))):
        z = vertical(above[t], below[t], colour, odd)
        out.append(fd[t, k] + c * ((y + (low + high)) + (b[t] + z)))
    return out


def half_sweep(dst, src, fd, level, colour, count, odd):
    for k in range(count):
        put(dst, k, relaxed(src, fd, level, colour, k, count, odd))


def first_sweeps(red, black, fd_red, fd_black, level, count, odd):
    for k in range(count):
        put(red, k, [fd_red[t, k] for t in range(red.shape[0])])
    half_sweep(black, red, fd_black, level, 1, count, odd)
    half_sweep(red, black, fd_red, level, 0, count, odd)
    half_sweep(black, red, fd_black, level, 1, count, odd)


def last_sweeps(red, black, fd_red, fd_black, level, count, odd):
    for _ in range(2):
        half_sweep(red, black, fd_red, level, 0, count, odd)
        half_sweep(black, red, fd_black, level, 1, count, odd)


def residual(red, black, fd, level, k, count, odd):
    d = at_end(0, k, count, odd, diag(level, 2), diag(level, 1))
    return [d * (new - old) for new, old in zip(relaxed(black, fd, level, 0, k, count, odd), get(red, k))]


def shifted(slots, reach):
    return {s: [turn(v, s, 1) if s else v for v in slots] for s in range(-reach, reach + 1)}


def relaxed_shifted(src, fd, reach, level, colour, parity):
    out = {}
    for s in range(-reach, reach + 1):
        odd = parity[s % 2]
        slots = src[s]
        count = len(slots)
        new = []
        for k in range(count):
            b = slots[k]
            zero = jnp.zeros_like(b)
            z = vertical(slots[k + 1] if k < count - 1 else zero, slots[k - 1] if k > 0 else zero, colour, odd)
            y = src[s - 1][k] + src[s + 1][k]
            x = turn(b, 1, 0) + turn(b, -1, 0)
            new.append(fd[s][k] + weight_of(level, colour, k, count, odd) * ((y + x) + (b + z)))
        out[s] = new
    return out


def halving(n, m, target):
    i = lax.broadcasted_iota(jnp.int32, (n, m), 0)
    return (i // 2 == target).astype(F32)


def doubling(n, m, target):
    i = lax.broadcasted_iota(jnp.int32, (n, m), 0)
    return (i == target).astype(F32)


def matmul(a, b):
    b = b.astype(jnp.bfloat16)
    out = None
    for part in range(3):
        piece = a.astype(jnp.bfloat16)
        term = jnp.dot(piece, b, preferred_element_type=F32)
        out = term if part == 0 else out + term
        if part < 2:
            a = a - piece.astype(F32)
    return out


def local_kernel(vel_hbm, old_hbm, obst_hbm, pred, source, to_low, to_high, vel, old, obst, edge_x, sems):
    lane = lanes(BX)
    row = rows_of(BX)
    depth = NZ // CHUNKS
    copies = []
    for c in range(CHUNKS):
        group = []
        for i, (src, dst, q) in enumerate(
            [(vel_hbm, vel, q) for q in range(3)] + [(old_hbm, old, q) for q in range(3)] + [(obst_hbm, obst, 0)]
        ):
            at = pl.ds((q * NZ + c * depth) * BX, depth * BX)
            group.append(pltpu.make_async_copy(src.at[at, :], dst.at[at, :], sems.at[c, i]))
        copies.append(group)
    for c in range(CHUNKS):
        for copy in copies[c]:
            copy.start()

    def cut(ref, j):
        return ref[BX * j : BX * (j + 1), :]

    packs = [jnp.zeros((BX, BY), F32) for _ in range(3)]

    def put_pair(pack, value, at):
        return jnp.where((lane == at) | (lane == at + 1), turn(value, at + 1, 1), pack)

    for copy in copies[0]:
        copy.wait()
    for z in range(NZ):
        if z % depth == depth - 1 and z < NZ - 1:
            for copy in copies[z // depth + 1]:
                copy.wait()
        fluid = (1 - cut(obst, z)).astype(F32)
        now = [cut(vel, q * NZ + z) for q in range(3)]
        spread = (TIME_STEP * WEIGHT_NEW * VISCOSITY) * fluid
        carry = (TIME_STEP * WEIGHT_NEW * 0.5) * fluid
        flow = [carry * v for v in now]
        plus = [spread - v for v in flow]
        minus = [spread + v for v in flow]
        across_x = jnp.where(row == 0, minus[0], jnp.where(row == BX - 1, plus[0], 0.0))
        across_y = jnp.where(lane == 0, minus[1], plus[1])
        plus_x = jnp.where(row == BX - 1, 0.0, plus[0])
        minus_x = jnp.where(row == 0, 0.0, minus[0])
        plus_y = jnp.where(lane == BY - 1, 0.0, plus[1])
        minus_y = jnp.where(lane == 0, 0.0, minus[1])
        keep = (1.0 - 6.0 * TIME_STEP * WEIGHT_NEW * VISCOSITY) * fluid
        past = (TIME_STEP * WEIGHT_OLD) * fluid
        for q in range(3):
            j = q * NZ + z
            v = now[q]
            p = keep * v + past * cut(old, j)
            p = p + (plus_x * turn(v, -1, 0) + minus_x * turn(v, 1, 0))
            p = p + (plus_y * turn(v, -1, 1) + minus_y * turn(v, 1, 1))
            if z < NZ - 1:
                p = p + plus[2] * cut(vel, j + 1)
            if z > 0:
                p = p + minus[2] * cut(vel, j - 1)
            pred[BX * j : BX * (j + 1), :] = p
            if q == 1:
                pv = p
        edge_x[BX * z : BX * (z + 1), :] = across_x
        for t, pair in enumerate(((now[0], now[1]), (now[2], across_y), (pv, across_x))):
            for i in range(2):
                packs[t] = put_pair(packs[t], pair[i], 64 * i + 2 * z)
    for z in range(NZ):
        u = cut(pred, z)
        v = cut(pred, NZ + z)
        zero = jnp.zeros_like(u)
        upper = cut(pred, 2 * NZ + z + 1) if z < NZ - 1 else zero
        lower = cut(pred, 2 * NZ + z - 1) if z > 0 else zero
        east = jnp.where(row == BX - 1, 0.0, turn(u, -1, 0))
        west = jnp.where(row == 0, 0.0, turn(u, 1, 0))
        north = jnp.where(lane == BY - 1, 0.0, turn(v, -1, 1))
        south = jnp.where(lane == 0, 0.0, turn(v, 1, 1))
        s = SCALE * ((east - west) + (north - south) + (upper - lower))
        source[BX * z : BX * (z + 1), :] = s
        to_low[8 * z : 8 * z + 8, :] = s[:8]
        to_high[8 * z : 8 * z + 8, :] = s[8:]
    half = NZ // 2
    sub = rows_of(8)
    for h in range(half):
        at = 8 * (NZ + h)
        a = source[BX * h : BX * (h + 1), :]
        b = source[BX * (h + half) : BX * (h + half + 1), :]
        to_low[at : at + 8, :] = jnp.where(sub < 4, a[8:], turn(b[8:], 4, 0))
        to_high[at : at + 8, :] = jnp.where(sub < 4, turn(b[:8], 4, 0), a[:8])
    for ref, r in ((to_low, 0), (to_high, BX - 1)):
        at = 12 * NZ
        ref[at : at + NZ, :] = edge_x[pl.ds(r, NZ, stride=BX), :]
        ref[at + NZ : at + 4 * NZ, :] = vel[pl.ds(r, 3 * NZ, stride=BX), :]
        ref[at + 4 * NZ : at + 5 * NZ, :] = pred[pl.ds(r, NZ, stride=BX), :]
        for t in range(3):
            ref[at + 5 * NZ + BX * t : at + 5 * NZ + BX * (t + 1), :] = packs[t]


def join_x_kernel(source, to_low, to_high, from_low, from_high, wide, to_left, to_right, fix_rows):
    lane = lanes(NZ)
    layer = rows_of(NZ)
    sub = rows_of(8)
    half = NZ // 2

    def line(ref, i):
        at = 12 * NZ + NZ * i
        return ref[at : at + NZ, :]

    def slope_y(f):
        return jnp.where(lane == BY - 1, 0.0, turn(f, -1, 1)) - jnp.where(lane == 0, 0.0, turn(f, 1, 1))

    def slope_z(f):
        return jnp.where(layer == NZ - 1, 0.0, turn(f, -1, 0)) - jnp.where(layer == 0, 0.0, turn(f, 1, 0))

    for z in range(NZ):
        w = WX * z
        wide[w : w + 16, :] = source[BX * z : BX * (z + 1), :]
        wide[w + 16 : w + 24, :] = from_high[8 * z : 8 * z + 8, :]
        at = 8 * (NZ + z % half)
        high = from_high[at : at + 8, :]
        low = from_low[at : at + 8, :]
        if z < half:
            wide[w + 24 : w + 32, :] = jnp.where(sub < 4, high, low)
        else:
            wide[w + 24 : w + 32, :] = turn(jnp.where(sub < 4, low, high), 4, 0)
        wide[w + 32 : w + 40, :] = from_low[8 * z : 8 * z + 8, :]

    def add(row, value):
        at = pl.ds(row % WX, NZ, stride=WX)
        wide[at, :] = wide[at, :] + SCALE * value

    for near, far, row, step, sign in ((to_low, from_low, 0, -1, 1.0), (to_high, from_high, 15, 1, -1.0)):
        inner = [line(near, 0) * line(far, 1 + q) for q in range(3)]
        outer = [line(far, 0) * line(near, 1 + q) for q in range(3)]
        add(row - step, -sign * inner[0])
        add(row, -sign * (line(far, 4) + outer[0]) + slope_y(inner[1]) + slope_z(inner[2]))
        add(row + step, sign * (line(near, 4) + inner[0]) + slope_y(outer[1]) + slope_z(outer[2]))
        add(row + 2 * step, sign * outer[0])
        for q in range(3):
            at = NZ * (3 * (step > 0) + q)
            fix_rows[at : at + NZ, :] = inner[q]

    stack = []
    for t in range(3):
        at = 17 * NZ + BX * t
        stack.append(jnp.concatenate([ref[at : at + BX, :] for ref in (to_low, from_high, from_low)], axis=0))
    first = rows_of(48) % BX == 0
    other = jnp.where(first, turn(stack[0], 1, 0), turn(stack[0], -1, 0))
    stack[2] = stack[2] + turn(stack[2] * other, 64, 1)
    lane = lanes(WX)
    for h in range(half):
        a = wide[WX * h : WX * (h + 1), :]
        b = turn(wide[WX * (h + half) : WX * (h + half + 1), :], 64, 1)
        to_left[WX * h : WX * (h + 1), :] = jnp.where(lane < 64, a, b)
        to_right[WX * h : WX * (h + 1), :] = jnp.where(lane < 64, b, a)
    for t in range(3):
        at = WX * half + 48 * t
        to_left[at : at + 48, :] = stack[t]
        to_right[at : at + 48, :] = stack[t]


def trimmed(a):
    return jnp.concatenate([a[0:24], a[32:40]], axis=0)


def fine_down_kernel(
    wide, sent_left, from_left, from_right,
    fd0_red, fd0_black, black0, sent_hbm, own1, up1, down1, fix_cols,
    fd_red, fd_black, red, black, res, thin, fd1_red, fd1_black, red1, black1, res1, sent, sems,
):
    lane = lanes(WX)
    odd = odd_cells(WX, 128)
    half = NZ // 2
    slots = NZ // 2

    lane48 = lanes(48)
    even = lane48 % 2 == 0
    low_half = lane48 < 64

    def pack_of(ref, t):
        at = WX * half + 48 * t
        return ref[at : at + 48, :]

    def swap(f):
        return turn(f, 64, 1)

    def both(f):
        return jnp.where(low_half, swap(f), f)

    def facing(left, right):
        return jnp.where(even, turn(right, -1, 1), turn(left, 1, 1))

    def slope_x(f):
        return turn(f, -1, 0) - turn(f, 1, 0)

    def slope_z(f):
        above = jnp.where(lane48 >= 2 * NZ - 2, 0.0, turn(f, -2, 1))
        below = jnp.where(lane48 < 2, 0.0, turn(f, 2, 1))
        return above - below

    def signed(f):
        return jnp.where(even, f, -f)

    own = [pack_of(sent_left, t) for t in range(3)]
    left = [pack_of(from_left, t) for t in range(3)]
    right = [pack_of(from_right, t) for t in range(3)]
    near = both(own[1])
    inner_uv = near * facing(left[0], right[0])
    inner_w = near * facing(left[1], right[1])
    far = both(jnp.where(even, left[1], right[1]))
    outer_uv = far * facing(own[0], own[0])
    outer_w = far * facing(own[1], own[1])
    inner_v = swap(inner_uv)
    outer_v = swap(outer_uv)
    pv_far = jnp.where(even, left[2], right[2]) + outer_v
    pv_own = own[2] + inner_v
    e0 = signed(facing(pv_far, pv_far)) + slope_x(inner_uv) + slope_z(inner_w)
    e1 = signed(facing(pv_own, pv_own)) + slope_x(outer_uv) + slope_z(outer_w)
    i = lax.broadcasted_iota(jnp.int32, (128, 128), 0)
    j = lax.broadcasted_iota(jnp.int32, (128, 128), 1)
    side = i % 2
    to = 4 * ((i % 64) // 2) + jnp.where(i < 64, 1 + side, 3 * side)
    order = SCALE * (to == j).astype(F32)
    mixed = []
    for e, v in ((e0, inner_v), (e1, outer_v)):
        m = jnp.where(low_half, e, swap(signed(v)))
        m = jnp.concatenate([m[0:24], jnp.where(rows_of(8) < 4, m[24:32], m[32:40]), m[40:48]], axis=0)
        mixed.append(matmul(m, order))
    edge = (lane < 2) | (lane >= BY - 2)

    def layer(z):
        t0 = wide[WX * z : WX * (z + 1), :]
        h = z % half
        a = from_right[WX * h : WX * (h + 1), :]
        b = from_left[WX * h : WX * (h + 1), :]
        if z < half:
            t1 = jnp.where(lane < 64, a, b)
        else:
            t1 = turn(jnp.where(lane < 64, b, a), 64, 1)
        t0 = t0 + jnp.where(edge, turn(mixed[0], 126 - 4 * z, 1), 0.0)
        t1 = t1 + jnp.where(edge, turn(mixed[1], 126 - 4 * z, 1), 0.0)
        return t0, t1

    for k in range(slots):
        for t, (low, high) in enumerate(zip(layer(2 * k), layer(2 * k + 1))):
            r, b = pack(low, high, odd)
            r = scaled(r, 0, 0, k, slots, odd)
            b = scaled(b, 0, 1, k, slots, odd)
            fd_red[t, k] = r
            fd_black[t, k] = b
    first_sweeps(red, black, fd_red, fd_black, 0, slots, odd)
    for k in range(slots):
        for t, r in enumerate(residual(red, black, fd_red, 0, k, slots, odd)):
            res[t, 32 * k : 32 * (k + 1), :] = trimmed(r)
    matrix = 0.125 * halving(256, 128, lax.broadcasted_iota(jnp.int32, (256, 128), 1))
    n = BX * slots
    for t in range(2):
        part = res.at[t]
        thin[:, 128 * t : 128 * t + 128] = part[pl.ds(0, n, stride=2), :] + part[pl.ds(1, n, stride=2), :]
    own1[...] = matmul(thin[...], matrix)

    odd1 = odd_cells(16, 128)
    slots1 = slots // 2
    sub = rows_of(8)

    def plane(z):
        return own1[16 * z : 16 * (z + 1), :]

    for k in range(slots1):
        r, b = pack(plane(2 * k), plane(2 * k + 1), odd1)
        fd1_red[0, k] = scaled(r, 1, 0, k, slots1, odd1)
        fd1_black[0, k] = scaled(b, 1, 1, k, slots1, odd1)
    first_sweeps(red1, black1, fd1_red, fd1_black, 1, slots1, odd1)
    for k in range(slots1):
        res1[8 * k : 8 * k + 8, :] = residual(red1, black1, fd1_red, 1, k, slots1, odd1)[0][:8]
    res1[...] = matmul(res1[...], 0.125 * halving(128, 128, j % 64))
    v = res1[pl.ds(0, 32, stride=2), :] + res1[pl.ds(1, 32, stride=2), :]
    sent[...] = jnp.where(lanes(16) < 64, v[:16], v[16:])
    copies = [pltpu.make_async_copy(sent, sent_hbm.at[d], sems.at[d]) for d in range(sent_hbm.shape[0])]
    for copy in copies:
        copy.start()
    for k in range(slots):
        for t, v in enumerate(get(black, k)):
            black0[t, k] = trimmed(v)
            fd0_red[t, k] = trimmed(fd_red[t, k])
            fd0_black[t, k] = trimmed(fd_black[t, k])
    for z in range(slots):
        a, b = plane(z)[:8], plane(z)[8:]
        up1[8 * z : 8 * z + 8, :] = jnp.where(sub < 4, a, b)
        down1[8 * z : 8 * z + 8, :] = jnp.where(sub < 4, b, a)
    fix_cols[0] = inner_uv[0:16]
    fix_cols[1] = inner_w[0:16]
    for copy in copies:
        copy.wait()


def predictor_kernel(pred, fix_rows, fix_cols, done):
    lane = lanes(BX)
    row = rows_of(BX)
    edge = (lane == 0) | (lane == BY - 1)
    for j in range(3 * NZ):
        q, z = divmod(j, NZ)
        low = jnp.broadcast_to(fix_rows[j : j + 1, :], (BX, BY))
        high = jnp.broadcast_to(fix_rows[3 * NZ + j : 3 * NZ + j + 1, :], (BX, BY))
        rim = jnp.where(row == 0, low, jnp.where(row == BX - 1, high, 0.0))
        column = turn(fix_cols[q // 2], -(64 * (q % 2) + 2 * z + 1), 1)
        rim = rim + jnp.where(edge, column, 0.0)
        done[BX * j : BX * (j + 1), :] = pred[BX * j : BX * (j + 1), :] + rim


def middle_kernel(own1, from_low, from_high, fd_red, fd_black, done, red, black):
    slots = 8
    odd = odd_cells(32, 128)
    sub = rows_of(8)

    def plane(z):
        a = own1[16 * z : 16 * z + 8, :]
        b = own1[16 * z + 8 : 16 * z + 16, :]
        low = from_low[8 * z : 8 * z + 8, :]
        high = from_high[8 * z : 8 * z + 8, :]
        tiles = [a] + [jnp.where(sub < 4, p, q) for p, q in ((b, high), (high, low), (low, b))]
        return jnp.concatenate(tiles, axis=0)

    for k in range(slots):
        r, b = pack(plane(2 * k), plane(2 * k + 1), odd)
        fd_red[0, k] = scaled(r, 1, 0, k, slots, odd)
        fd_black[0, k] = scaled(b, 1, 1, k, slots, odd)
    first_sweeps(red, black, fd_red, fd_black, 1, slots, odd)
    for k in range(slots):
        done[k] = get(black, k)[0]


def up_kernel(
    nx, g_own, g_left, g_right, fd1_red, fd1_black, black1_in, fd0_red, fd0_black, black0_in, pred, obst,
    corrected_hbm, pressure_hbm, fd2_red, fd2_black, red2, black2, res2, fd3, red1, black1, big1, red0, black0, big0, ring, corrected, pressure, sems,
):
    x2 = 4 * nx
    lane = lanes(x2)
    odd2 = odd_cells(x2, 128)
    slots2 = 4

    for i, g in enumerate((g_own, g_right, g_left)):
        for j in range(nx):
            d = lax.rem(lax.axis_index("gx") + j, nx)
            for z in range(4):
                ring[4 * i + z, 4 * j : 4 * j + 4, :] = g[d, 4 * z : 4 * z + 4, :]

    def rhs2(z):
        lift = 64 * (z // 4)
        own, right, left = (ring[4 * i + z % 4] for i in range(3))
        own = turn(own, -lift, 1) if lift else own
        right = turn(right, 32 - lift, 1)
        left = jnp.where(lane < 96, turn(left, 32 - lift, 1), turn(left, 96 - lift, 1))
        return jnp.where(lane < 32, own, jnp.where(lane < 80, right, left))

    for k in range(slots2):
        r, b = pack(rhs2(2 * k), rhs2(2 * k + 1), odd2)
        fd2_red[0, k] = scaled(r, 2, 0, k, slots2, odd2)
        fd2_black[0, k] = scaled(b, 2, 1, k, slots2, odd2)
    first_sweeps(red2, black2, fd2_red, fd2_black, 2, slots2, odd2)
    for k in range(slots2):
        res2[x2 * k : x2 * (k + 1), :] = residual(red2, black2, fd2_red, 2, k, slots2, odd2)[0]
    col = lax.broadcasted_iota(jnp.int32, (128, 128), 1)
    res2[...] = matmul(res2[...], 0.125 * halving(128, 128, col % 64))
    n = slots2 * x2 // 2
    x3 = x2 // 2
    fd3[...] = res2[pl.ds(0, n, stride=2), :] + res2[pl.ds(1, n, stride=2), :]

    odd3 = odd_cells(x3, 128)
    fr, fb = [], []
    for k in range(2):
        r, b = pack(fd3[x3 * 2 * k : x3 * (2 * k + 1), :], fd3[x3 * (2 * k + 1) : x3 * (2 * k + 2), :], odd3)
        fr.append(scaled(r, 3, 0, k, 2, odd3))
        fb.append(scaled(b, 3, 1, k, 2, odd3))
    parity = (odd3, jnp.logical_not(odd3))
    fr, fb = shifted(fr, 3), shifted(fb, 2)
    b = relaxed_shifted(fr, fb, 2, 3, 1, parity)
    r = relaxed_shifted(b, fr, 1, 3, 0, parity)
    b = relaxed_shifted(r, fb, 0, 3, 1, parity)
    for _ in range(3):
        b = shifted(b[0], 4)
        for reach in (3, 1):
            r = relaxed_shifted(b, fr, reach, 3, 0, parity)
            b = relaxed_shifted(r, fb, reach - 1, 3, 1, parity)
    r, b = r[0], b[0]

    def layers(red, black, odd):
        return jnp.where(odd, black, red), jnp.where(odd, red, black)

    parts = []
    for k in range(2):
        parts += layers(r[k], b[k], odd3)
    e = matmul(jnp.concatenate(parts, axis=0), doubling(128, 128, col // 2))
    res2[pl.ds(0, n, stride=2), :] = e
    res2[pl.ds(1, n, stride=2), :] = e
    for k in range(slots2):
        put(black2, k, [get(black2, k)[0] + res2[x2 * k : x2 * (k + 1), :]])
    last_sweeps(red2, black2, fd2_red, fd2_black, 2, slots2, odd2)

    odd1 = odd_cells(32, 128)
    slots1 = 8
    sub = rows_of(8)
    for k in range(slots2):
        for i, v in enumerate(layers(get(red2, k)[0], get(black2, k)[0], odd2)):
            at = 16 * (2 * k + i)
            big1[at : at + 8, :] = v[0:8]
            big1[at + 8 : at + 16, :] = jnp.where(sub < 2, v[8:16] if nx > 2 else v[0:8], v[x2 - 8 : x2])
    e = matmul(big1[0 : 16 * slots1, :], doubling(128, 128, jnp.where(col < 96, col // 2, col // 2 + 64)))
    big1[pl.ds(0, 16 * slots1, stride=2), :] = e
    big1[pl.ds(1, 16 * slots1, stride=2), :] = e
    for k in range(slots1):
        put(black1, k, [black1_in[k] + big1[32 * k : 32 * (k + 1), :]])
    last_sweeps(red1, black1, fd1_red, fd1_black, 1, slots1, odd1)

    slots0 = NZ // 2
    for k in range(slots1):
        low, high = layers(get(red1, k)[0], get(black1, k)[0], odd1)
        for i, v in enumerate((low, high)):
            at = 16 * (2 * k + i)
            big1[at : at + 8, :] = v[0:8]
            big1[at + 8 : at + 16, :] = jnp.where(sub < 4, v[8:16], v[24:32])
    wide_col = lax.broadcasted_iota(jnp.int32, (128, 256), 1)
    e = matmul(big1[0 : 16 * slots0, :], doubling(128, 256, wide_col // 2))
    for t in range(2):
        part = e[:, 128 * t : 128 * t + 128]
        big0[t, pl.ds(0, 16 * slots0, stride=2), :] = part
        big0[t, pl.ds(1, 16 * slots0, stride=2), :] = part
    odd0 = odd_cells(32, 128)
    for k in range(slots0):
        put(black0, k, [black0_in[t, k] + big0[t, 32 * k : 32 * (k + 1), :] for t in range(2)])
    last_sweeps(red0, black0, fd0_red, fd0_black, 0, slots0, odd0)
    for k in range(slots0):
        pairs = [layers(r, b, odd0) for r, b in zip(get(red0, k), get(black0, k))]
        for i, dst in enumerate((red0, black0)):
            put(dst, k, [pair[i] for pair in pairs])

    depth = 8
    copies = []

    lane = lanes(BX)

    def at(z, t, shift=0):
        return (black0 if z % 2 else red0)[t, z // 2, 8 + shift : 24 + shift, :]

    for z in range(NZ):
        own = at(z, 0)
        pressure[BX * z : BX * (z + 1), :] = own
        zero = jnp.zeros_like(own)
        upper = at(z + 1, 0) if z < NZ - 1 else zero
        lower = at(z - 1, 0) if z > 0 else zero
        gx = at(z, 0, 1) - at(z, 0, -1)
        margin = at(z, 1)
        gy = turn(jnp.where(lane == 0, margin, own), -1, 1) - turn(jnp.where(lane == BY - 1, margin, own), 1, 1)
        fluid = (1 - obst[BX * z : BX * (z + 1), :]).astype(F32)
        for q, g in enumerate((gx, gy, upper - lower)):
            j = q * NZ + z
            v = pred[BX * j : BX * (j + 1), :]
            corrected[BX * j : BX * (j + 1), :] = fluid * (v - (0.5 * TIME_STEP) * g)
        if z % depth == depth - 1:
            c = z // depth
            for i in range(4):
                src, dst = (corrected, corrected_hbm) if i < 3 else (pressure, pressure_hbm)
                part = pl.ds(((i % 3) * NZ + c * depth) * BX, depth * BX)
                copies.append(pltpu.make_async_copy(src.at[part, :], dst.at[part, :], sems.at[c, i]))
                copies[-1].start()
    for copy in copies:
        copy.wait()


def both_ways(axis, to_low, to_high):
    n = lax.axis_size(axis)
    up = [(i, (i + 1) % n) for i in range(n)]
    down = [((i + 1) % n, i) for i in range(n)]
    return lax.ppermute(to_high, axis, up), lax.ppermute(to_low, axis, down)


def body(velocity, old_tendency, obstacle):
    nx = lax.axis_size("gx")
    vel = velocity.reshape(3 * NZ * BX, BY)
    old = old_tendency.reshape(3 * NZ * BX, BY)
    obst = obstacle.reshape(NZ * BX, BY)

    block = 3 * NZ * BX
    within = pl.BlockSpec(memory_space=pltpu.VMEM)
    anywhere = [pl.BlockSpec(memory_space=pltpu.HBM)] * 3
    pred, source, to_low, to_high = call(
        local_kernel,
        (vmem(block, BY), vmem(NZ * BX, BY), vmem(592, BY), vmem(592, BY)),
        tuple(pltpu.with_memory_space_constraint(a, pltpu.HBM) for a in (vel, old, obst)),
        [
            pltpu.VMEM((block, BY), F32),
            pltpu.VMEM((block, BY), F32),
            pltpu.VMEM((NZ * BX, BY), jnp.int32),
            pltpu.VMEM((NZ * BX, BY), F32),
            pltpu.SemaphoreType.DMA((CHUNKS, 7)),
        ],
        in_specs=anywhere,
        name="local",
    )
    from_low, from_high = both_ways("gx", to_low, to_high)
    wide, to_left, to_right, fix_rows = call(
        join_x_kernel,
        (vmem(NZ * WX, BY), vmem(784, BY), vmem(784, BY), vmem(6 * NZ, BY)),
        (source, to_low, to_high, from_low, from_high),
        name="join_x",
    )
    from_left, from_right = both_ways("gy", to_left, to_right)
    fd0_red, fd0_black, black0, sent, own1, up1, down1, fix_cols = call(
        fine_down_kernel,
        (
            vmem(2, 16, 32, BY),
            vmem(2, 16, 32, BY),
            vmem(2, 16, 32, BY),
            vmem(nx, 16, BY),
            vmem(256, BY),
            vmem(128, BY),
            vmem(128, BY),
            vmem(2, BX, BY),
        ),
        (wide, to_left, from_left, from_right),
        [(2, 16, WX, BY)] * 2
        + [(2, 16, WX + 16, BY)] * 2
        + [(2, 512, BY), (256, 256)]
        + [(1, 8, 16, BY)] * 2
        + [(1, 8, 32, BY)] * 2
        + [(64, BY), (16, BY), pltpu.SemaphoreType.DMA((nx,))],
        out_specs=(within,) * 3 + (pl.BlockSpec(memory_space=pl.ANY),) + (within,) * 4,
        name="fine_down",
    )
    gathered = lax.all_to_all(sent, "gx", 0, 0)
    low1, high1 = both_ways("gx", down1, up1)
    fd1_red, fd1_black, black1 = call(
        middle_kernel,
        (vmem(1, 8, 32, BY), vmem(1, 8, 32, BY), vmem(8, 32, BY)),
        (own1, low1, high1),
        [(1, 8, 48, BY)] * 2,
        name="middle",
    )
    pred = call(predictor_kernel, vmem(block, BY), (pred, fix_rows, fix_cols), name="predictor")
    g_left, g_right = both_ways("gy", gathered, gathered)
    x2 = 4 * nx
    corrected, pressure = call(
        functools.partial(up_kernel, nx),
        (vmem(block, BY), vmem(NZ * BX, BY)),
        (gathered, g_left, g_right, fd1_red, fd1_black, black1, fd0_red, fd0_black, black0, pred, obst),
        [(1, 4, x2, BY)] * 2
        + [(1, 4, x2 + 16, BY)] * 2
        + [(4 * x2, BY), (2 * x2, BY)]
        + [(1, 8, 48, BY)] * 2
        + [(256, BY)]
        + [(2, 16, 48, BY)] * 2
        + [(2, 512, BY), (12, x2, BY), (block, BY), (NZ * BX, BY), pltpu.SemaphoreType.DMA((4, 4))],
        out_specs=(pl.BlockSpec(memory_space=pl.ANY),) * 2,
        name="up",
    )
    return corrected.reshape(3, NZ, BX, BY), pressure.reshape(NZ, BX, BY)


def solution(mesh):
    placed = (P(None, None, "gx", "gy"), P(None, None, "gx", "gy"), P(None, "gx", "gy"))
    return jax.shard_map(
        body,
        mesh=mesh,
        in_specs=placed,
        out_specs=(P(None, None, "gx", "gy"), P(None, "gx", "gy")),
        check_vma=False,
    )
```

```python
import functools

import jax
import jax.numpy as jnp
from jax import lax
from jax.experimental import pallas as pl
from jax.experimental.pallas import tpu as pltpu
from jax.sharding import PartitionSpec as P

TIME_STEP = 0.25
VISCOSITY = 0.1
WEIGHT_NEW = 15.0 / 16.0
WEIGHT_OLD = -25.0 / 48.0
HELMHOLTZ = 1.0e-4
SCALE = -0.5 / TIME_STEP
INTERPRET = False
F32 = jnp.float32
NZ = 32
BX = 16
BY = 128
WX = 40
CHUNKS = 8


def vmem(*shape):
    return jax.ShapeDtypeStruct(shape, F32)


def call(kernel, outs, args, scratch=(), in_specs=None, out_specs=None, name=None):
    everywhere = pl.BlockSpec(memory_space=pltpu.VMEM)
    return pl.pallas_call(
        kernel,
        out_shape=outs,
        out_specs=out_specs or jax.tree.map(lambda _: everywhere, outs),
        in_specs=in_specs or [everywhere] * len(args),
        scratch_shapes=[pltpu.VMEM(s, F32) if isinstance(s, tuple) else s for s in scratch],
        compiler_params=pltpu.CompilerParams(vmem_limit_bytes=16 << 20),
        interpret=INTERPRET,
        name=name,
    )(*args)


def turn(a, shift, axis):
    return pltpu.roll(a, shift % a.shape[axis], axis)


def lanes(rows, cols=128):
    return lax.broadcasted_iota(jnp.int32, (rows, cols), 1)


def rows_of(rows, cols=128):
    return lax.broadcasted_iota(jnp.int32, (rows, cols), 0)


def odd_cells(rows, cols):
    return (rows_of(rows, cols) + lanes(rows, cols)) % 2 == 1


def diag(level, m):
    return HELMHOLTZ + (4.0 + m) / float(4**level)


def at_end(colour, k, count, odd, inner, end):
    if k == 0:
        return jnp.where(odd, inner, end) if colour == 0 else jnp.where(odd, end, inner)
    if k == count - 1:
        return jnp.where(odd, end, inner) if colour == 0 else jnp.where(odd, inner, end)
    return inner


def pack(low, high, odd):
    return jnp.where(odd, high, low), jnp.where(odd, low, high)


def scaled(value, level, colour, k, count, odd):
    return value * at_end(colour, k, count, odd, 1.0 / diag(level, 2), 1.0 / diag(level, 1))


def put(dst, k, tiles):
    n = tiles[0].shape[0]
    for t, v in enumerate(tiles):
        dst[t, k, 8 : 8 + n, :] = v
        dst[t, k, 7:8, :] = v[n - 1 : n]
        dst[t, k, 8 + n : 9 + n, :] = v[0:1]


def get(src, k, shift=0):
    tiles, _, rows, _ = src.shape
    return [src[t, k, 8 + shift : rows - 8 + shift, :] for t in range(tiles)]


def beside(tiles):
    if len(tiles) == 1:
        return [turn(tiles[0], 1, 1) + turn(tiles[0], -1, 1)]
    lane = lanes(tiles[0].shape[0])
    out = []
    for own, other in (tiles, tiles[::-1]):
        last = jnp.where(lane == BY - 1, other, own)
        first = jnp.where(lane == 0, other, own)
        out.append(turn(last, 1, 1) + turn(first, -1, 1))
    return out


def vertical(above, below, colour, odd):
    return jnp.where(odd, above, below) if colour == 0 else jnp.where(odd, below, above)


def weight_of(level, colour, k, count, odd):
    s = float(4**level)
    return at_end(colour, k, count, odd, 1.0 / s / diag(level, 2), 1.0 / s / diag(level, 1))


def relaxed(src, fd, level, colour, k, count, odd):
    b = get(src, k)
    zero = [jnp.zeros_like(v) for v in b]
    above = get(src, k + 1) if k < count - 1 else zero
    below = get(src, k - 1) if k > 0 else zero
    c = weight_of(level, colour, k, count, odd)
    out = []
    for t, (y, low, high) in enumerate(zip(beside(b), get(src, k, -1), get(src, k, 1))):
        z = vertical(above[t], below[t], colour, odd)
        out.append(fd[t, k] + c * ((y + (low + high)) + (b[t] + z)))
    return out


def half_sweep(dst, src, fd, level, colour, count, odd):
    for k in range(count):
        put(dst, k, relaxed(src, fd, level, colour, k, count, odd))


def first_sweeps(red, black, fd_red, fd_black, level, count, odd):
    for k in range(count):
        put(red, k, [fd_red[t, k] for t in range(red.shape[0])])
    half_sweep(black, red, fd_black, level, 1, count, odd)
    half_sweep(red, black, fd_red, level, 0, count, odd)
    half_sweep(black, red, fd_black, level, 1, count, odd)


def last_sweeps(red, black, fd_red, fd_black, level, count, odd):
    for _ in range(2):
        half_sweep(red, black, fd_red, level, 0, count, odd)
        half_sweep(black, red, fd_black, level, 1, count, odd)


def residual(red, black, fd, level, k, count, odd):
    d = at_end(0, k, count, odd, diag(level, 2), diag(level, 1))
    return [d * (new - old) for new, old in zip(relaxed(black, fd, level, 0, k, count, odd), get(red, k))]


def shifted(slots, reach):
    return {s: [turn(v, s, 1) if s else v for v in slots] for s in range(-reach, reach + 1)}


def relaxed_shifted(src, fd, reach, level, colour, parity):
    out = {}
    for s in range(-reach, reach + 1):
        odd = parity[s % 2]
        slots = src[s]
        count = len(slots)
        new = []
        for k in range(count):
            b = slots[k]
            zero = jnp.zeros_like(b)
            z = vertical(slots[k + 1] if k < count - 1 else zero, slots[k - 1] if k > 0 else zero, colour, odd)
            y = src[s - 1][k] + src[s + 1][k]
            x = turn(b, 1, 0) + turn(b, -1, 0)
            new.append(fd[s][k] + weight_of(level, colour, k, count, odd) * ((y + x) + (b + z)))
        out[s] = new
    return out


def halving(n, m, target):
    i = lax.broadcasted_iota(jnp.int32, (n, m), 0)
    return (i // 2 == target).astype(F32)


def doubling(n, m, target):
    i = lax.broadcasted_iota(jnp.int32, (n, m), 0)
    return (i == target).astype(F32)


def matmul(a, b):
    b = b.astype(jnp.bfloat16)
    out = None
    for part in range(3):
        piece = a.astype(jnp.bfloat16)
        term = jnp.dot(piece, b, preferred_element_type=F32)
        out = term if part == 0 else out + term
        if part < 2:
            a = a - piece.astype(F32)
    return out


def local_kernel(vel_hbm, old_hbm, obst_hbm, pred, source, to_low, to_high, vel, old, obst, edge_x, sems):
    lane = lanes(BX)
    row = rows_of(BX)
    depth = NZ // CHUNKS
    copies = []
    for c in range(CHUNKS):
        group = []
        for i, (src, dst, q) in enumerate(
            [(vel_hbm, vel, q) for q in range(3)] + [(old_hbm, old, q) for q in range(3)] + [(obst_hbm, obst, 0)]
        ):
            at = pl.ds((q * NZ + c * depth) * BX, depth * BX)
            group.append(pltpu.make_async_copy(src.at[at, :], dst.at[at, :], sems.at[c, i]))
        copies.append(group)
    for c in range(CHUNKS):
        for copy in copies[c]:
            copy.start()

    def cut(ref, j):
        return ref[BX * j : BX * (j + 1), :]

    packs = [jnp.zeros((BX, BY), F32) for _ in range(3)]

    def put_pair(pack, value, at):
        return jnp.where((lane == at) | (lane == at + 1), turn(value, at + 1, 1), pack)

    for copy in copies[0]:
        copy.wait()
    for z in range(NZ):
        if z % depth == depth - 1 and z < NZ - 1:
            for copy in copies[z // depth + 1]:
                copy.wait()
        fluid = (1 - cut(obst, z)).astype(F32)
        now = [cut(vel, q * NZ + z) for q in range(3)]
        spread = (TIME_STEP * WEIGHT_NEW * VISCOSITY) * fluid
        carry = (TIME_STEP * WEIGHT_NEW * 0.5) * fluid
        flow = [carry * v for v in now]
        plus = [spread - v for v in flow]
        minus = [spread + v for v in flow]
        across_x = jnp.where(row == 0, minus[0], jnp.where(row == BX - 1, plus[0], 0.0))
        across_y = jnp.where(lane == 0, minus[1], plus[1])
        plus_x = jnp.where(row == BX - 1, 0.0, plus[0])
        minus_x = jnp.where(row == 0, 0.0, minus[0])
        plus_y = jnp.where(lane == BY - 1, 0.0, plus[1])
        minus_y = jnp.where(lane == 0, 0.0, minus[1])
        keep = (1.0 - 6.0 * TIME_STEP * WEIGHT_NEW * VISCOSITY) * fluid
        past = (TIME_STEP * WEIGHT_OLD) * fluid
        for q in range(3):
            j = q * NZ + z
            v = now[q]
            p = keep * v + past * cut(old, j)
            p = p + (plus_x * turn(v, -1, 0) + minus_x * turn(v, 1, 0))
            p = p + (plus_y * turn(v, -1, 1) + minus_y * turn(v, 1, 1))
            if z < NZ - 1:
                p = p + plus[2] * cut(vel, j + 1)
            if z > 0:
                p = p + minus[2] * cut(vel, j - 1)
            pred[BX * j : BX * (j + 1), :] = p
            if q == 1:
                pv = p
        edge_x[BX * z : BX * (z + 1), :] = across_x
        for t, pair in enumerate(((now[0], now[1]), (now[2], across_y), (pv, across_x))):
            for i in range(2):
                packs[t] = put_pair(packs[t], pair[i], 64 * i + 2 * z)
    for z in range(NZ):
        u = cut(pred, z)
        v = cut(pred, NZ + z)
        zero = jnp.zeros_like(u)
        upper = cut(pred, 2 * NZ + z + 1) if z < NZ - 1 else zero
        lower = cut(pred, 2 * NZ + z - 1) if z > 0 else zero
        east = jnp.where(row == BX - 1, 0.0, turn(u, -1, 0))
        west = jnp.where(row == 0, 0.0, turn(u, 1, 0))
        north = jnp.where(lane == BY - 1, 0.0, turn(v, -1, 1))
        south = jnp.where(lane == 0, 0.0, turn(v, 1, 1))
        s = SCALE * ((east - west) + (north - south) + (upper - lower))
        source[BX * z : BX * (z + 1), :] = s
        to_low[8 * z : 8 * z + 8, :] = s[:8]
        to_high[8 * z : 8 * z + 8, :] = s[8:]
    half = NZ // 2
    sub = rows_of(8)
    for h in range(half):
        at = 8 * (NZ + h)
        a = source[BX * h : BX * (h + 1), :]
        b = source[BX * (h + half) : BX * (h + half + 1), :]
        to_low[at : at + 8, :] = jnp.where(sub < 4, a[8:], turn(b[8:], 4, 0))
        to_high[at : at + 8, :] = jnp.where(sub < 4, turn(b[:8], 4, 0), a[:8])
    for ref, r in ((to_low, 0), (to_high, BX - 1)):
        at = 12 * NZ
        ref[at : at + NZ, :] = edge_x[pl.ds(r, NZ, stride=BX), :]
        ref[at + NZ : at + 4 * NZ, :] = vel[pl.ds(r, 3 * NZ, stride=BX), :]
        ref[at + 4 * NZ : at + 5 * NZ, :] = pred[pl.ds(r, NZ, stride=BX), :]
        for t in range(3):
            ref[at + 5 * NZ + BX * t : at + 5 * NZ + BX * (t + 1), :] = packs[t]


def join_x_kernel(source, to_low, to_high, from_low, from_high, wide, to_left, to_right, fix_rows):
    lane = lanes(NZ)
    layer = rows_of(NZ)
    sub = rows_of(8)
    half = NZ // 2

    def line(ref, i):
        at = 12 * NZ + NZ * i
        return ref[at : at + NZ, :]

    def slope_y(f):
        return jnp.where(lane == BY - 1, 0.0, turn(f, -1, 1)) - jnp.where(lane == 0, 0.0, turn(f, 1, 1))

    def slope_z(f):
        return jnp.where(layer == NZ - 1, 0.0, turn(f, -1, 0)) - jnp.where(layer == 0, 0.0, turn(f, 1, 0))

    for z in range(NZ):
        w = WX * z
        wide[w : w + 16, :] = source[BX * z : BX * (z + 1), :]
        wide[w + 16 : w + 24, :] = from_high[8 * z : 8 * z + 8, :]
        at = 8 * (NZ + z % half)
        high = from_high[at : at + 8, :]
        low = from_low[at : at + 8, :]
        if z < half:
            wide[w + 24 : w + 32, :] = jnp.where(sub < 4, high, low)
        else:
            wide[w + 24 : w + 32, :] = turn(jnp.where(sub < 4, low, high), 4, 0)
        wide[w + 32 : w + 40, :] = from_low[8 * z : 8 * z + 8, :]

    def add(row, value):
        at = pl.ds(row % WX, NZ, stride=WX)
        wide[at, :] = wide[at, :] + SCALE * value

    for near, far, row, step, sign in ((to_low, from_low, 0, -1, 1.0), (to_high, from_high, 15, 1, -1.0)):
        inner = [line(near, 0) * line(far, 1 + q) for q in range(3)]
        outer = [line(far, 0) * line(near, 1 + q) for q in range(3)]
        add(row - step, -sign * inner[0])
        add(row, -sign * (line(far, 4) + outer[0]) + slope_y(inner[1]) + slope_z(inner[2]))
        add(row + step, sign * (line(near, 4) + inner[0]) + slope_y(outer[1]) + slope_z(outer[2]))
        add(row + 2 * step, sign * outer[0])
        for q in range(3):
            at = NZ * (3 * (step > 0) + q)
            fix_rows[at : at + NZ, :] = inner[q]

    stack = []
    for t in range(3):
        at = 17 * NZ + BX * t
        stack.append(jnp.concatenate([ref[at : at + BX, :] for ref in (to_low, from_high, from_low)], axis=0))
    first = rows_of(48) % BX == 0
    other = jnp.where(first, turn(stack[0], 1, 0), turn(stack[0], -1, 0))
    stack[2] = stack[2] + turn(stack[2] * other, 64, 1)
    lane = lanes(WX)
    for h in range(half):
        a = wide[WX * h : WX * (h + 1), :]
        b = turn(wide[WX * (h + half) : WX * (h + half + 1), :], 64, 1)
        to_left[WX * h : WX * (h + 1), :] = jnp.where(lane < 64, a, b)
        to_right[WX * h : WX * (h + 1), :] = jnp.where(lane < 64, b, a)
    for t in range(3):
        at = WX * half + 48 * t
        to_left[at : at + 48, :] = stack[t]
        to_right[at : at + 48, :] = stack[t]


def trimmed(a):
    return jnp.concatenate([a[0:24], a[32:40]], axis=0)


def fine_down_kernel(
    wide, sent_left, from_left, from_right,
    fd0_red, fd0_black, black0, sent_hbm, own1, up1, down1, fix_cols,
    fd_red, fd_black, red, black, res, thin, fd1_red, fd1_black, red1, black1, res1, sent, sems,
):
    lane = lanes(WX)
    odd = odd_cells(WX, 128)
    half = NZ // 2
    slots = NZ // 2

    lane48 = lanes(48)
    even = lane48 % 2 == 0
    low_half = lane48 < 64

    def pack_of(ref, t):
        at = WX * half + 48 * t
        return ref[at : at + 48, :]

    def swap(f):
        return turn(f, 64, 1)

    def both(f):
        return jnp.where(low_half, swap(f), f)

    def facing(left, right):
        return jnp.where(even, turn(right, -1, 1), turn(left, 1, 1))

    def slope_x(f):
        return turn(f, -1, 0) - turn(f, 1, 0)

    def slope_z(f):
        above = jnp.where(lane48 >= 2 * NZ - 2, 0.0, turn(f, -2, 1))
        below = jnp.where(lane48 < 2, 0.0, turn(f, 2, 1))
        return above - below

    def signed(f):
        return jnp.where(even, f, -f)

    own = [pack_of(sent_left, t) for t in range(3)]
    left = [pack_of(from_left, t) for t in range(3)]
    right = [pack_of(from_right, t) for t in range(3)]
    near = both(own[1])
    inner_uv = near * facing(left[0], right[0])
    inner_w = near * facing(left[1], right[1])
    far = both(jnp.where(even, left[1], right[1]))
    outer_uv = far * facing(own[0], own[0])
    outer_w = far * facing(own[1], own[1])
    inner_v = swap(inner_uv)
    outer_v = swap(outer_uv)
    pv_far = jnp.where(even, left[2], right[2]) + outer_v
    pv_own = own[2] + inner_v
    e0 = signed(facing(pv_far, pv_far)) + slope_x(inner_uv) + slope_z(inner_w)
    e1 = signed(facing(pv_own, pv_own)) + slope_x(outer_uv) + slope_z(outer_w)
    i = lax.broadcasted_iota(jnp.int32, (128, 128), 0)
    j = lax.broadcasted_iota(jnp.int32, (128, 128), 1)
    side = i % 2
    to = 4 * ((i % 64) // 2) + jnp.where(i < 64, 1 + side, 3 * side)
    order = SCALE * (to == j).astype(F32)
    mixed = []
    for e, v in ((e0, inner_v), (e1, outer_v)):
        m = jnp.where(low_half, e, swap(signed(v)))
        m = jnp.concatenate([m[0:24], jnp.where(rows_of(8) < 4, m[24:32], m[32:40]), m[40:48]], axis=0)
        mixed.append(matmul(m, order))
    edge = (lane < 2) | (lane >= BY - 2)

    def layer(z):
        t0 = wide[WX * z : WX * (z + 1), :]
        h = z % half
        a = from_right[WX * h : WX * (h + 1), :]
        b = from_left[WX * h : WX * (h + 1), :]
        if z < half:
            t1 = jnp.where(lane < 64, a, b)
        else:
            t1 = turn(jnp.where(lane < 64, b, a), 64, 1)
        t0 = t0 + jnp.where(edge, turn(mixed[0], 126 - 4 * z, 1), 0.0)
        t1 = t1 + jnp.where(edge, turn(mixed[1], 126 - 4 * z, 1), 0.0)
        return t0, t1

    for k in range(slots):
        for t, (low, high) in enumerate(zip(layer(2 * k), layer(2 * k + 1))):
            r, b = pack(low, high, odd)
            r = scaled(r, 0, 0, k, slots, odd)
            b = scaled(b, 0, 1, k, slots, odd)
            fd_red[t, k] = r
            fd_black[t, k] = b
    first_sweeps(red, black, fd_red, fd_black, 0, slots, odd)
    for k in range(slots):
        for t, r in enumerate(residual(red, black, fd_red, 0, k, slots, odd)):
            res[t, 32 * k : 32 * (k + 1), :] = trimmed(r)
    matrix = 0.125 * halving(256, 128, lax.broadcasted_iota(jnp.int32, (256, 128), 1))
    n = BX * slots
    for t in range(2):
        part = res.at[t]
        thin[:, 128 * t : 128 * t + 128] = part[pl.ds(0, n, stride=2), :] + part[pl.ds(1, n, stride=2), :]
    own1[...] = matmul(thin[...], matrix)

    odd1 = odd_cells(16, 128)
    slots1 = slots // 2
    sub = rows_of(8)

    def plane(z):
        return own1[16 * z : 16 * (z + 1), :]

    for k in range(slots1):
        r, b = pack(plane(2 * k), plane(2 * k + 1), odd1)
        fd1_red[0, k] = scaled(r, 1, 0, k, slots1, odd1)
        fd1_black[0, k] = scaled(b, 1, 1, k, slots1, odd1)
    first_sweeps(red1, black1, fd1_red, fd1_black, 1, slots1, odd1)
    for k in range(slots1):
        res1[8 * k : 8 * k + 8, :] = residual(red1, black1, fd1_red, 1, k, slots1, odd1)[0][:8]
    res1[...] = matmul(res1[...], 0.125 * halving(128, 128, j % 64))
    v = res1[pl.ds(0, 32, stride=2), :] + res1[pl.ds(1, 32, stride=2), :]
    sent[...] = jnp.where(lanes(16) < 64, v[:16], v[16:])
    copies = [pltpu.make_async_copy(sent, sent_hbm.at[d], sems.at[d]) for d in range(sent_hbm.shape[0])]
    for copy in copies:
        copy.start()
    for k in range(slots):
        for t, v in enumerate(get(black, k)):
            black0[t, k] = trimmed(v)
            fd0_red[t, k] = trimmed(fd_red[t, k])
            fd0_black[t, k] = trimmed(fd_black[t, k])
    for z in range(slots):
        a, b = plane(z)[:8], plane(z)[8:]
        up1[8 * z : 8 * z + 8, :] = jnp.where(sub < 4, a, b)
        down1[8 * z : 8 * z + 8, :] = jnp.where(sub < 4, b, a)
    fix_cols[0] = inner_uv[0:16]
    fix_cols[1] = inner_w[0:16]
    for copy in copies:
        copy.wait()


def predictor_kernel(pred, fix_rows, fix_cols, done):
    lane = lanes(BX)
    row = rows_of(BX)
    edge = (lane == 0) | (lane == BY - 1)
    for j in range(3 * NZ):
        q, z = divmod(j, NZ)
        low = jnp.broadcast_to(fix_rows[j : j + 1, :], (BX, BY))
        high = jnp.broadcast_to(fix_rows[3 * NZ + j : 3 * NZ + j + 1, :], (BX, BY))
        rim = jnp.where(row == 0, low, jnp.where(row == BX - 1, high, 0.0))
        column = turn(fix_cols[q // 2], -(64 * (q % 2) + 2 * z + 1), 1)
        rim = rim + jnp.where(edge, column, 0.0)
        done[BX * j : BX * (j + 1), :] = pred[BX * j : BX * (j + 1), :] + rim


def middle_kernel(own1, from_low, from_high, fd_red, fd_black, done, red, black):
    slots = 8
    odd = odd_cells(32, 128)
    sub = rows_of(8)

    def plane(z):
        a = own1[16 * z : 16 * z + 8, :]
        b = own1[16 * z + 8 : 16 * z + 16, :]
        low = from_low[8 * z : 8 * z + 8, :]
        high = from_high[8 * z : 8 * z + 8, :]
        tiles = [a] + [jnp.where(sub < 4, p, q) for p, q in ((b, high), (high, low), (low, b))]
        return jnp.concatenate(tiles, axis=0)

    for k in range(slots):
        r, b = pack(plane(2 * k), plane(2 * k + 1), odd)
        fd_red[0, k] = scaled(r, 1, 0, k, slots, odd)
        fd_black[0, k] = scaled(b, 1, 1, k, slots, odd)
    first_sweeps(red, black, fd_red, fd_black, 1, slots, odd)
    for k in range(slots):
        done[k] = get(black, k)[0]


def up_kernel(
    nx, g_own, g_left, g_right, fd1_red, fd1_black, black1_in, fd0_red, fd0_black, black0_in, pred, obst,
    corrected_hbm, pressure_hbm, fd2_red, fd2_black, red2, black2, res2, fd3, red1, black1, big1, red0, black0, big0, ring, corrected, pressure, sems,
):
    x2 = 4 * nx
    lane = lanes(x2)
    odd2 = odd_cells(x2, 128)
    slots2 = 4

    for i, g in enumerate((g_own, g_right, g_left)):
        for j in range(nx):
            d = lax.rem(lax.axis_index("gx") + j, nx)
            for z in range(4):
                ring[4 * i + z, 4 * j : 4 * j + 4, :] = g[d, 4 * z : 4 * z + 4, :]

    def rhs2(z):
        lift = 64 * (z // 4)
        own, right, left = (ring[4 * i + z % 4] for i in range(3))
        own = turn(own, -lift, 1) if lift else own
        right = turn(right, 32 - lift, 1)
        left = jnp.where(lane < 96, turn(left, 32 - lift, 1), turn(left, 96 - lift, 1))
        return jnp.where(lane < 32, own, jnp.where(lane < 80, right, left))

    for k in range(slots2):
        r, b = pack(rhs2(2 * k), rhs2(2 * k + 1), odd2)
        fd2_red[0, k] = scaled(r, 2, 0, k, slots2, odd2)
        fd2_black[0, k] = scaled(b, 2, 1, k, slots2, odd2)
    first_sweeps(red2, black2, fd2_red, fd2_black, 2, slots2, odd2)
    for k in range(slots2):
        res2[x2 * k : x2 * (k + 1), :] = residual(red2, black2, fd2_red, 2, k, slots2, odd2)[0]
    col = lax.broadcasted_iota(jnp.int32, (128, 128), 1)
    res2[...] = matmul(res2[...], 0.125 * halving(128, 128, col % 64))
    n = slots2 * x2 // 2
    x3 = x2 // 2
    fd3[...] = res2[pl.ds(0, n, stride=2), :] + res2[pl.ds(1, n, stride=2), :]

    odd3 = odd_cells(x3, 128)
    fr, fb = [], []
    for k in range(2):
        r, b = pack(fd3[x3 * 2 * k : x3 * (2 * k + 1), :], fd3[x3 * (2 * k + 1) : x3 * (2 * k + 2), :], odd3)
        fr.append(scaled(r, 3, 0, k, 2, odd3))
        fb.append(scaled(b, 3, 1, k, 2, odd3))
    parity = (odd3, jnp.logical_not(odd3))
    fr, fb = shifted(fr, 3), shifted(fb, 2)
    b = relaxed_shifted(fr, fb, 2, 3, 1, parity)
    r = relaxed_shifted(b, fr, 1, 3, 0, parity)
    b = relaxed_shifted(r, fb, 0, 3, 1, parity)
    for _ in range(3):
        b = shifted(b[0], 4)
        for reach in (3, 1):
            r = relaxed_shifted(b, fr, reach, 3, 0, parity)
            b = relaxed_shifted(r, fb, reach - 1, 3, 1, parity)
    r, b = r[0], b[0]

    def layers(red, black, odd):
        return jnp.where(odd, black, red), jnp.where(odd, red, black)

    parts = []
    for k in range(2):
        parts += layers(r[k], b[k], odd3)
    e = matmul(jnp.concatenate(parts, axis=0), doubling(128, 128, col // 2))
    res2[pl.ds(0, n, stride=2), :] = e
    res2[pl.ds(1, n, stride=2), :] = e
    for k in range(slots2):
        put(black2, k, [get(black2, k)[0] + res2[x2 * k : x2 * (k + 1), :]])
    last_sweeps(red2, black2, fd2_red, fd2_black, 2, slots2, odd2)

    odd1 = odd_cells(32, 128)
    slots1 = 8
    sub = rows_of(8)
    for k in range(slots2):
        for i, v in enumerate(layers(get(red2, k)[0], get(black2, k)[0], odd2)):
            at = 16 * (2 * k + i)
            big1[at : at + 8, :] = v[0:8]
            big1[at + 8 : at + 16, :] = jnp.where(sub < 2, v[8:16] if nx > 2 else v[0:8], v[x2 - 8 : x2])
    e = matmul(big1[0 : 16 * slots1, :], doubling(128, 128, jnp.where(col < 96, col // 2, col // 2 + 64)))
    big1[pl.ds(0, 16 * slots1, stride=2), :] = e
    big1[pl.ds(1, 16 * slots1, stride=2), :] = e
    for k in range(slots1):
        put(black1, k, [black1_in[k] + big1[32 * k : 32 * (k + 1), :]])
    last_sweeps(red1, black1, fd1_red, fd1_black, 1, slots1, odd1)

    slots0 = NZ // 2
    for k in range(slots1):
        low, high = layers(get(red1, k)[0], get(black1, k)[0], odd1)
        for i, v in enumerate((low, high)):
            at = 16 * (2 * k + i)
            big1[at : at + 8, :] = v[0:8]
            big1[at + 8 : at + 16, :] = jnp.where(sub < 4, v[8:16], v[24:32])
    wide_col = lax.broadcasted_iota(jnp.int32, (128, 256), 1)
    e = matmul(big1[0 : 16 * slots0, :], doubling(128, 256, wide_col // 2))
    for t in range(2):
        part = e[:, 128 * t : 128 * t + 128]
        big0[t, pl.ds(0, 16 * slots0, stride=2), :] = part
        big0[t, pl.ds(1, 16 * slots0, stride=2), :] = part
    odd0 = odd_cells(32, 128)
    for k in range(slots0):
        put(black0, k, [black0_in[t, k] + big0[t, 32 * k : 32 * (k + 1), :] for t in range(2)])
    last_sweeps(red0, black0, fd0_red, fd0_black, 0, slots0, odd0)
    for k in range(slots0):
        pairs = [layers(r, b, odd0) for r, b in zip(get(red0, k), get(black0, k))]
        for i, dst in enumerate((red0, black0)):
            put(dst, k, [pair[i] for pair in pairs])

    depth = 8
    copies = []

    lane = lanes(BX)

    def at(z, t, shift=0):
        return (black0 if z % 2 else red0)[t, z // 2, 8 + shift : 24 + shift, :]

    for z in range(NZ):
        own = at(z, 0)
        pressure[BX * z : BX * (z + 1), :] = own
        zero = jnp.zeros_like(own)
        upper = at(z + 1, 0) if z < NZ - 1 else zero
        lower = at(z - 1, 0) if z > 0 else zero
        gx = at(z, 0, 1) - at(z, 0, -1)
        margin = at(z, 1)
        gy = turn(jnp.where(lane == 0, margin, own), -1, 1) - turn(jnp.where(lane == BY - 1, margin, own), 1, 1)
        fluid = (1 - obst[BX * z : BX * (z + 1), :]).astype(F32)
        for q, g in enumerate((gx, gy, upper - lower)):
            j = q * NZ + z
            v = pred[BX * j : BX * (j + 1), :]
            corrected[BX * j : BX * (j + 1), :] = fluid * (v - (0.5 * TIME_STEP) * g)
        if z % depth == depth - 1:
            c = z // depth
            for i in range(4):
                src, dst = (corrected, corrected_hbm) if i < 3 else (pressure, pressure_hbm)
                part = pl.ds(((i % 3) * NZ + c * depth) * BX, depth * BX)
                copies.append(pltpu.make_async_copy(src.at[part, :], dst.at[part, :], sems.at[c, i]))
                copies[-1].start()
    for copy in copies:
        copy.wait()


def both_ways(axis, to_low, to_high):
    n = lax.axis_size(axis)
    up = [(i, (i + 1) % n) for i in range(n)]
    down = [((i + 1) % n, i) for i in range(n)]
    return lax.ppermute(to_high, axis, up), lax.ppermute(to_low, axis, down)


def body(velocity, old_tendency, obstacle):
    nx = lax.axis_size("gx")
    vel = velocity.reshape(3 * NZ * BX, BY)
    old = old_tendency.reshape(3 * NZ * BX, BY)
    obst = obstacle.reshape(NZ * BX, BY)

    block = 3 * NZ * BX
    within = pl.BlockSpec(memory_space=pltpu.VMEM)
    anywhere = [pl.BlockSpec(memory_space=pltpu.HBM)] * 3
    pred, source, to_low, to_high = call(
        local_kernel,
        (vmem(block, BY), vmem(NZ * BX, BY), vmem(592, BY), vmem(592, BY)),
        tuple(pltpu.with_memory_space_constraint(a, pltpu.HBM) for a in (vel, old, obst)),
        [
            pltpu.VMEM((block, BY), F32),
            pltpu.VMEM((block, BY), F32),
            pltpu.VMEM((NZ * BX, BY), jnp.int32),
            pltpu.VMEM((NZ * BX, BY), F32),
            pltpu.SemaphoreType.DMA((CHUNKS, 7)),
        ],
        in_specs=anywhere,
        name="local",
    )
    from_low, from_high = both_ways("gx", to_low, to_high)
    wide, to_left, to_right, fix_rows = call(
        join_x_kernel,
        (vmem(NZ * WX, BY), vmem(784, BY), vmem(784, BY), vmem(6 * NZ, BY)),
        (source, to_low, to_high, from_low, from_high),
        name="join_x",
    )
    from_left, from_right = both_ways("gy", to_left, to_right)
    fd0_red, fd0_black, black0, sent, own1, up1, down1, fix_cols = call(
        fine_down_kernel,
        (
            vmem(2, 16, 32, BY),
            vmem(2, 16, 32, BY),
            vmem(2, 16, 32, BY),
            vmem(nx, 16, BY),
            vmem(256, BY),
            vmem(128, BY),
            vmem(128, BY),
            vmem(2, BX, BY),
        ),
        (wide, to_left, from_left, from_right),
        [(2, 16, WX, BY)] * 2
        + [(2, 16, WX + 16, BY)] * 2
        + [(2, 512, BY), (256, 256)]
        + [(1, 8, 16, BY)] * 2
        + [(1, 8, 32, BY)] * 2
        + [(64, BY), (16, BY), pltpu.SemaphoreType.DMA((nx,))],
        out_specs=(within,) * 3 + (pl.BlockSpec(memory_space=pl.ANY),) + (within,) * 4,
        name="fine_down",
    )
    gathered = lax.all_to_all(sent, "gx", 0, 0)
    low1, high1 = both_ways("gx", down1, up1)
    fd1_red, fd1_black, black1 = call(
        middle_kernel,
        (vmem(1, 8, 32, BY), vmem(1, 8, 32, BY), vmem(8, 32, BY)),
        (own1, low1, high1),
        [(1, 8, 48, BY)] * 2,
        name="middle",
    )
    pred = call(predictor_kernel, vmem(block, BY), (pred, fix_rows, fix_cols), name="predictor")
    g_left, g_right = both_ways("gy", gathered, gathered)
    x2 = 4 * nx
    corrected, pressure = call(
        functools.partial(up_kernel, nx),
        (vmem(block, BY), vmem(NZ * BX, BY)),
        (gathered, g_left, g_right, fd1_red, fd1_black, black1, fd0_red, fd0_black, black0, pred, obst),
        [(1, 4, x2, BY)] * 2
        + [(1, 4, x2 + 16, BY)] * 2
        + [(4 * x2, BY), (2 * x2, BY)]
        + [(1, 8, 48, BY)] * 2
        + [(256, BY)]
        + [(2, 16, 48, BY)] * 2
        + [(2, 512, BY), (12, x2, BY), (block, BY), (NZ * BX, BY), pltpu.SemaphoreType.DMA((4, 4))],
        out_specs=(pl.BlockSpec(memory_space=pl.ANY),) * 2,
        name="up",
    )
    return corrected.reshape(3, NZ, BX, BY), pressure.reshape(NZ, BX, BY)


def solution(mesh):
    placed = (P(None, None, "gx", "gy"), P(None, None, "gx", "gy"), P(None, "gx", "gy"))
    return jax.shard_map(
        body,
        mesh=mesh,
        in_specs=placed,
        out_specs=(P(None, None, "gx", "gy"), P(None, "gx", "gy")),
        check_vma=False,
    )
```
